32 devices in a mesh: gx: 4 (over z), gy: 2 (over x), gz: 4 (over y, core).
Axes of the slice: x: 2, y: 2, z: 4, core: 2. Of those that a mesh axis runs over, the one named last changes fastest.
Arguments:
- volume: bfloat16 [32, 8, 32, 512], P(None, 'gx', 'gy', 'gz'), may hold values from -6 to 6
- w_first: bfloat16 [3, 3, 3, 32, 32], replicated, may hold values from -0.21875 to 0.21875
- w_second: bfloat16 [3, 3, 3, 32, 32], replicated, may hold values from -0.21875 to 0.21875
- v_first: bfloat16 [3, 3, 3, 32, 32], replicated, may hold values from -0.21875 to 0.21875
- v_second: bfloat16 [3, 3, 3, 32, 32], replicated, may hold values from -0.21875 to 0.21875
Outputs:
- jv: bfloat16 [32, 8, 32, 512], P(None, 'gx', 'gy', 'gz')
- gv_first: float32 [3, 3, 3, 32, 32], replicated
- gv_second: float32 [3, 3, 3, 32, 32], replicated
The draws below stay inside these ranges and needn't reach their ends.
All inputs are finite; a program needn't handle non-finite values.
Results may differ from the reference program's by a relative error of at most 0.005.
Values may be sent and summed in bfloat16 or wider, within the bound.
A program may use at most 64 MiB of HBM per device.

```python
import jax
import jax.numpy as jnp
from jax import lax

CHANNELS = 32
NX = 8
NY = 32
NZ = 512
CELLS = 131072
FILT = 864


def shard_levels(key, extent, split, least, high):
    factor_of, own = 1.0, jax.random.fold_in(key, 6)
    for dim, parts in split:
        heights = jnp.exp(jax.random.uniform(jax.random.fold_in(own, dim), (parts,), jnp.float32, least / len(split), high / len(split)))
        factor_of = factor_of * jnp.repeat(heights, extent[dim] // parts).reshape([-1 if axis == dim else 1 for axis in range(len(extent))])
    return factor_of


def bell_draw(key, dims, deviation, bound, shards=(), held_as=jnp.bfloat16):
    gain = shard_levels(key, dims, shards, -0.22, 0.18) if shards else 1.0
    drawn = jax.random.normal(key, dims, jnp.float32) * deviation * gain
    return jnp.minimum(jnp.maximum(drawn, -bound), bound).astype(held_as)


def setup_inputs(seed: int = 0) -> dict:
    key_of = jax.random.split(jax.random.key(seed), 6)
    return {
        "volume": bell_draw(key_of[0], (CHANNELS, NX, NY, NZ), 1.0, 6.0, ((1, 4), (2, 2), (3, 4))),
        "w_first": bell_draw(key_of[1], (3, 3, 3, CHANNELS, CHANNELS), FILT ** -0.5, 0.21875),
        "w_second": bell_draw(key_of[2], (3, 3, 3, CHANNELS, CHANNELS), FILT ** -0.5, 0.21875),
        "v_first": bell_draw(key_of[3], (3, 3, 3, CHANNELS, CHANNELS), FILT ** -0.5, 0.21875),
        "v_second": bell_draw(key_of[4], (3, 3, 3, CHANNELS, CHANNELS), FILT ** -0.5, 0.21875),
    }


def gelu_pair(pre):
    inner = 0.7978845608 * (pre + 0.044715 * pre * pre * pre)
    hyper = jnp.tanh(inner)
    hidden = 0.5 * pre * (1.0 + hyper)
    slope = 0.5 * (1.0 + hyper) + 0.5 * pre * (1.0 - hyper * hyper) * 0.7978845608 * (1.0 + 0.134145 * pre * pre)
    return hidden, slope


def convolve(field, weight):
    result = lax.conv_general_dilated(field.astype(jnp.float32)[None], weight.astype(jnp.float32), (1, 1, 1), "SAME", dimension_numbers=("NCDHW", "DHWIO", "NCDHW"), precision=lax.Precision.HIGHEST)
    return result[0]


def correlate(field, target):
    padded = jnp.pad(field.astype(jnp.float32), ((0, 0), (1, 1), (1, 1), (1, 1)))
    target32 = target.astype(jnp.float32)
    sizes = field.shape
    planes = []
    for shift_x in range(3):
        rows_y = []
        for shift_y in range(3):
            rows_z = []
            for shift_z in range(3):
                window = padded[:, shift_x:shift_x + sizes[1], shift_y:shift_y + sizes[2], shift_z:shift_z + sizes[3]]
                rows_z.append(jnp.einsum("cxyz,oxyz->co", window, target32, precision=lax.Precision.HIGHEST))
            rows_y.append(jnp.stack(rows_z))
        planes.append(jnp.stack(rows_y))
    return jnp.stack(planes)


def reference(volume, w_first, w_second, v_first, v_second):
    pre = convolve(volume, w_first)
    hidden_f, slope = gelu_pair(pre)
    hidden = hidden_f.astype(jnp.bfloat16)
    tangent = (slope * convolve(volume, v_first)).astype(jnp.bfloat16)
    jv = (convolve(tangent, w_second) + convolve(hidden, v_second)).astype(jnp.bfloat16)
    flipped = jnp.transpose(jnp.flip(w_second, (0, 1, 2)), (0, 1, 2, 4, 3))
    back = (slope * convolve(jv, flipped)).astype(jnp.bfloat16)
    count_all = jnp.float32(CELLS)
    factor = jnp.float32(FILT) ** 0.5
    gv_second = factor * (correlate(hidden, jv) / count_all + 0.1 * v_second.astype(jnp.float32))
    gv_first = factor * (correlate(volume, back) / count_all + 0.1 * v_first.astype(jnp.float32))
    return jv, gv_first, gv_second
```

```python
import functools
import itertools
import math

import jax
import jax.numpy as jnp
from jax import lax
from jax.experimental import pallas as pl
from jax.experimental.pallas import tpu as pltpu
from jax.sharding import PartitionSpec as P

MESH = pl.DeviceIdType.MESH
AXES = ("gx", "gy", "gz")
STEPS = [d for d in itertools.product((-1, 0, 1), repeat=3) if d != (0, 0, 0)]
STEPS.sort(key=lambda d: (d[2] != 0, d[0] == 0, abs(d[0]) + abs(d[1])))
NT = (((1,), (1,)), ((), ()))


def gelu_pair(pre):
    inner = 0.7978845608 * (pre + 0.044715 * pre * pre * pre)
    hyper = jnp.tanh(inner)
    hidden = 0.5 * pre * (1.0 + hyper)
    slope = 0.5 * (1.0 + hyper) + 0.5 * pre * (1.0 - hyper * hyper) * 0.7978845608 * (
        1.0 + 0.134145 * pre * pre
    )
    return hidden, slope


def code(step):
    return (step[0] + 1) * 9 + (step[1] + 1) * 3 + step[2] + 1


def kernel(
    sizes,
    volume,
    w1,
    w2,
    w3,
    d1,
    d2,
    jv_out,
    gv1,
    gv2,
    *scratch,
):
    (rv, rp, rj, zv, zp, zj, ev, ep, ej, sv, sp, sj, slope_ref, back_ref,
     t1, t2, t3, shift, keep, acc, pack, land, part, full,
     hsend, hrecv, asend, arecv, bsend, brecv) = scratch
    depth, height, chan, width = volume.shape
    me = tuple(lax.axis_index(a) for a in AXES)
    total = sizes[0] * sizes[1] * sizes[2]
    line = (me[0] * sizes[1] + me[1]) * sizes[2] + me[2]

    def place(index):
        return (
            index // (sizes[1] * sizes[2]),
            index // sizes[2] % sizes[1],
            index % sizes[2],
        )

    def there(step):
        ok = None
        for pos, size, delta in zip(me, sizes, step):
            if delta == -1:
                term = pos > 0
            elif delta == 1:
                term = pos < size - 1
            else:
                continue
            ok = term if ok is None else jnp.logical_and(ok, term)
        return ok

    barrier = pltpu.get_barrier_semaphore()
    near_only = max(sizes) <= 4

    if near_only:
        greeted = 0
        for step in STEPS:
            ok = there(step)
            greeted = greeted + jnp.where(ok, 1, 0)

            @pl.when(ok)
            def _():
                pl.semaphore_signal(
                    barrier,
                    inc=1,
                    device_id=tuple(p + d for p, d in zip(me, step)),
                    device_id_type=MESH,
                )
    else:
        greeted = total - 1

        @pl.loop(1, total)
        def _(i):
            pl.semaphore_signal(
                barrier, inc=1, device_id=place(lax.rem(line + i, total)), device_id_type=MESH
            )

    def source(delta, extent):
        return {-1: pl.ds(1, 1), 1: pl.ds(extent, 1), 0: pl.ds(1, extent)}[delta]

    def target(delta, extent):
        return {-1: pl.ds(extent + 1, 1), 1: pl.ds(0, 1), 0: pl.ds(1, extent)}[delta]

    def landing(step, rows, zbuf):
        if step[2] == 0:
            return rows.at[target(step[0], depth), target(step[1], height)]
        return zbuf.at[0 if step[2] == 1 else 1, 1 - step[0], 1 - step[1]]

    def message(step, rows, zbuf, edge, slot):
        if step[2] == 0:
            src = rows.at[source(step[0], depth), source(step[1], height)]
        else:
            src = edge
        return pltpu.make_async_remote_copy(
            src_ref=src,
            dst_ref=landing(step, rows, zbuf),
            send_sem=hsend.at[slot, code(step)],
            recv_sem=hrecv.at[slot, code(step)],
            device_id=tuple(p + d for p, d in zip(me, step)),
            device_id_type=MESH,
        )

    def send(rows, zbuf, edge, slot, cross):
        for step in STEPS:
            if (step[2] != 0) == cross:

                @pl.when(there(step))
                def _():
                    message(step, rows, zbuf, edge, slot).start()

    def clear(rows, zbuf):
        for step in STEPS:
            back = tuple(-d for d in step)

            @pl.when(jnp.logical_not(there(back)))
            def _():
                ref = landing(step, rows, zbuf)
                ref[...] = jnp.zeros(ref.shape, ref.dtype)

    def receive(rows, zbuf, edge, slot, kind):
        for step in STEPS:
            if (step[0] != 0) != (kind == 1):
                continue
            back = tuple(-d for d in step)

            @pl.when(there(back))
            def _():
                message(step, rows, zbuf, edge, slot).wait_recv()

    def stage(rows, zbuf, edge, slot, out, table, group, finish):
        for kind in range(2):
            receive(rows, zbuf, edge, slot, kind)
            spread(rows, zbuf, out, (near, far)[kind])
            convolve(table, out, group, kind, finish)

    def sent(rows, zbuf, edge, slot):
        for step in STEPS:

            @pl.when(there(step))
            def _():
                message(step, rows, zbuf, edge, slot).wait_send()

    def edges(rows, edge):
        count = rows.shape[2]
        lane = lax.broadcasted_iota(jnp.int32, (count, width), 1)
        cells = depth * height
        built = jnp.zeros((count, width), jnp.float32)
        for x in range(depth):

            def step(y, built, x=x):
                row = rows[x + 1, y + 1].astype(jnp.float32)
                at = x * height + y
                built = jnp.where(lane == at, pltpu.roll(row, at, 1), built)
                return jnp.where(lane == cells + at, pltpu.roll(row, cells + at + 1, 1), built)

            built = lax.fori_loop(0, height, step, built, unroll=4)
        edge[...] = built.astype(edge.dtype)

    def shifter():
        src = lax.broadcasted_iota(jnp.int32, (2 * width, 2 * width), 0)
        dst = lax.broadcasted_iota(jnp.int32, (2 * width, 2 * width), 1)
        cells = depth * height
        low = jnp.logical_or(
            jnp.logical_and(src == dst - 1, src < width - 1),
            jnp.logical_and(
                dst == 0, jnp.logical_and(src >= width + cells, src < width + 2 * cells)
            ),
        )
        high = jnp.logical_or(
            jnp.logical_and(src == dst - width + 1, src < width),
            jnp.logical_and(
                dst == 2 * width - 1, jnp.logical_and(src >= width, src < width + cells)
            ),
        )
        pick = jnp.logical_or(
            jnp.logical_and(dst < width, low), jnp.logical_and(dst >= width, high)
        )
        shift[...] = jnp.where(pick, 1.0, 0.0).astype(shift.dtype)

    near = tuple(range(1, depth + 1))
    far = (0, depth + 1)

    def spread(rows, zbuf, out, planes):
        count = rows.shape[2]
        groups = count // chan
        lane = lax.broadcasted_iota(jnp.int32, (count, width), 1)
        cells = depth * height

        for xp in planes:
            dx = 0 if xp == 0 else (2 if xp == depth + 1 else 1)
            halo = []
            for yp in range(height + 2):
                dy = 0 if yp == 0 else (2 if yp == height + 1 else 1)
                left = zbuf[0, dx, dy].astype(jnp.float32)
                right = zbuf[1, dx, dy].astype(jnp.float32)
                at = (xp - 1) % depth * height + (yp - 1) % height
                both = jnp.where(lane == at, right, jnp.where(lane == cells + at, left, 0.0))
                halo.append(both.astype(rows.dtype))
            wide = rows[xp].reshape((height + 2) * count, width)
            lhs = jnp.concatenate([wide, jnp.concatenate(halo, axis=0)], axis=1)
            moved = jnp.dot(lhs, shift[...], preferred_element_type=jnp.float32)
            moved = moved.astype(rows.dtype).reshape(height + 2, count, 2 * width)
            kept = wide.reshape(height + 2, count, width)
            for g in range(groups):
                at = slice(g * chan, (g + 1) * chan)
                base = g * 3 * chan
                out[xp, :, base : base + chan] = moved[:, at, :width]
                out[xp, :, base + chan : base + 2 * chan] = kept[:, at]
                out[xp, :, base + 2 * chan : base + 3 * chan] = moved[:, at, width:]

    def band(weights, table, group):
        outs = weights.shape[0]
        third = weights.shape[1] // 3
        step = third // 3
        table[...] = jnp.zeros_like(table)
        for kx in range(3):
            piece = weights[:, kx * third : (kx + 1) * third]
            for ox in range(depth):
                xp = ox + kx
                kind, pos = (0, near.index(xp)) if xp in near else (1, far.index(xp))
                for oy in range(group):
                    row = (ox * group + oy) * outs
                    at = (pos * (group + 2) + oy) * step
                    table[kind, row : row + outs, at : at + third] = piece

    def convolve(table, ref, group, kind, finish):
        outs = table.shape[1] // (depth * group)
        planes = (near, far)[kind]

        @pl.loop(0, height // (2 * group))
        def _(j):
            halves = []
            for half in range(2):
                y = (2 * j + half) * group
                halves.append(
                    jnp.concatenate(
                        [
                            ref[xp, pl.ds(y, group + 2)].reshape(
                                (group + 2) * ref.shape[2], width
                            )
                            for xp in planes
                        ],
                        axis=0,
                    )
                )
            rhs = jnp.concatenate(halves, axis=1)
            out = jnp.dot(
                table[kind, :, : rhs.shape[0]], rhs, preferred_element_type=jnp.float32
            )
            if kind == 0:
                keep[j] = out
                return
            out = out + keep[j]
            for half in range(2):
                for ox in range(depth):
                    for oy in range(group):
                        row = (ox * group + oy) * outs
                        finish(
                            ox,
                            (2 * j + half) * group + oy,
                            out[row : row + outs, half * width : (half + 1) * width],
                        )

    def correlate(ref, rows, offset):
        acc[...] = jnp.zeros_like(acc)
        for x in range(depth):

            @pl.loop(0, height // 4)
            def _(j, x=x):
                y = 4 * j
                rhs = jnp.concatenate(
                    [rows[x + offset, y + i + offset] for i in range(4)], axis=1
                )
                for kx in range(3):
                    lhs = jnp.concatenate(
                        [
                            ref[x + kx, pl.ds(y + i, 3), : 3 * chan].reshape(9 * chan, width)
                            for i in range(4)
                        ],
                        axis=1,
                    )
                    acc[kx] += lax.dot_general(lhs, rhs, NT, preferred_element_type=jnp.float32)

    tiles = pack.shape[1]
    cells_all = float(depth * height * width * total)
    factor = math.sqrt(27.0 * chan)

    def owner(t):
        return t * total // tiles

    span = 8 * tiles
    lanes = width // chan

    def scatter(slot):
        for j in range(lanes):
            flat = acc[...].reshape(27 * chan, chan)
            pack[slot, :, :, j * chan : (j + 1) * chan] = flat[
                j * span : (j + 1) * span
            ].reshape(tiles, 8, chan)
        for t in range(tiles):
            at = owner(t)

            @pl.when(line != at)
            def _():
                pltpu.make_async_remote_copy(
                    src_ref=pack.at[slot, t],
                    dst_ref=land.at[slot, lax.rem(line - at + total, total) - 1],
                    send_sem=asend.at[slot],
                    recv_sem=arecv.at[slot],
                    device_id=place(at),
                    device_id_type=MESH,
                ).start()

    def gather(slot):
        for t in range(tiles):

            @pl.when(line == owner(t))
            def _():
                pltpu.make_async_copy(
                    land.at[slot], land.at[slot], arecv.at[slot]
                ).wait()
                summed = pack[slot, t] + jnp.sum(land[slot], axis=0)
                part[slot] = summed
                full[slot, t] = summed

                @pl.loop(1, total)
                def _(i):
                    pltpu.make_async_remote_copy(
                        src_ref=part.at[slot],
                        dst_ref=full.at[slot, t],
                        send_sem=bsend.at[slot],
                        recv_sem=brecv.at[slot],
                        device_id=place(lax.rem(line + i, total)),
                        device_id_type=MESH,
                    ).start()

    def owning():
        held = line == owner(0)
        for t in range(1, tiles):
            held = jnp.logical_or(held, line == owner(t))
        return held

    def drain(slot, out, direction):
        held = owning()
        for flag, count in ((held, tiles - 1), (jnp.logical_not(held), tiles)):

            @pl.when(flag)
            def _():
                some = full.at[slot, pl.ds(0, count)]
                pltpu.make_async_copy(some, some, brecv.at[slot]).wait()
                mine = pack.at[slot, pl.ds(0, count)]
                pltpu.make_async_copy(mine, mine, asend.at[slot]).wait()

        @pl.when(held)
        def _():
            pltpu.make_async_copy(land.at[slot], land.at[slot], bsend.at[slot]).wait()

        whole = full[slot].reshape(span, width)
        for j in range(lanes):
            at = slice(j * span, (j + 1) * span)
            damp = 0.1 * direction[at].astype(jnp.float32)
            out[at] = factor * (whole[:, j * chan : (j + 1) * chan] / cells_all + damp)

    inner = (slice(1, depth + 1), slice(1, height + 1))
    rv[inner] = volume[...]
    pl.semaphore_wait(barrier, greeted)
    send(rv, zv, ev, 0, False)
    edges(rv, ev)
    send(rv, zv, ev, 0, True)
    for rows, zbuf in ((rv, zv), (rp, zp), (rj, zj)):
        clear(rows, zbuf)
    shifter()
    band(w1, t1, 2)
    band(w2, t2, 4)
    band(w3, t3, 4)

    def first(x, y, out):
        hidden, slope = gelu_pair(out[:chan])
        slope_ref[x, y] = slope
        rp[x + 1, y + 1, :chan] = hidden.astype(jnp.bfloat16)
        rp[x + 1, y + 1, chan:] = (slope * out[chan:]).astype(jnp.bfloat16)

    stage(rv, zv, ev, 0, sv, t1, 2, first)
    send(rp, zp, ep, 1, False)
    edges(rp, ep)
    send(rp, zp, ep, 1, True)

    def second(x, y, out):
        rj[x + 1, y + 1] = out.astype(jnp.bfloat16)

    stage(rp, zp, ep, 1, sp, t2, 4, second)
    send(rj, zj, ej, 2, False)
    edges(rj, ej)
    send(rj, zj, ej, 2, True)
    jv_out[...] = rj[inner]
    correlate(sp, rj, 1)
    scatter(0)

    def third(x, y, out):
        back_ref[x, y] = (slope_ref[x, y] * out).astype(jnp.bfloat16)

    stage(rj, zj, ej, 2, sj, t3, 4, third)
    correlate(sv, back_ref, 0)
    scatter(1)
    gather(0)
    gather(1)
    drain(0, gv2, d2)
    drain(1, gv1, d1)
    sent(rv, zv, ev, 0)
    sent(rp, zp, ep, 1)
    sent(rj, zj, ej, 2)


def body(volume, w_first, w_second, v_first, v_second):
    chan, depth, height, width = volume.shape
    sizes = tuple(lax.axis_size(a) for a in AXES)
    total = sizes[0] * sizes[1] * sizes[2]
    filt = 27 * chan
    tiles = filt * chan // (8 * width)
    w1 = jnp.concatenate([w_first, v_first], axis=-1).reshape(filt, 2 * chan).T
    w2 = jnp.stack([v_second, w_second], axis=2).reshape(2 * filt, chan).T
    w3 = jnp.transpose(jnp.flip(w_second, (0, 1, 2)), (3, 0, 1, 2, 4)).reshape(chan, filt)
    cells = jnp.transpose(volume, (1, 2, 0, 3))
    bf, f32 = jnp.bfloat16, jnp.float32
    pads = (depth + 2, height + 2)
    vmem = pl.BlockSpec(memory_space=pltpu.VMEM)
    jv, corr1, corr2 = pl.pallas_call(
        functools.partial(kernel, sizes),
        out_shape=(
            jax.ShapeDtypeStruct((depth, height, chan, width), bf),
            jax.ShapeDtypeStruct((filt, chan), f32),
            jax.ShapeDtypeStruct((filt, chan), f32),
        ),
        in_specs=[vmem] * 6,
        out_specs=(vmem,) * 3,
        scratch_shapes=[
            pltpu.VMEM(pads + (chan, width), bf),
            pltpu.VMEM(pads + (2 * chan, width), bf),
            pltpu.VMEM(pads + (chan, width), bf),
            pltpu.VMEM((2, 3, 3, chan, width), bf),
            pltpu.VMEM((2, 3, 3, 2 * chan, width), bf),
            pltpu.VMEM((2, 3, 3, chan, width), bf),
            pltpu.VMEM((chan, width), bf),
            pltpu.VMEM((2 * chan, width), bf),
            pltpu.VMEM((chan, width), bf),
            pltpu.VMEM(pads + (3 * chan, width), bf),
            pltpu.VMEM(pads + (6 * chan, width), bf),
            pltpu.VMEM(pads + (3 * chan, width), bf),
            pltpu.VMEM((depth, height, chan, width), f32),
            pltpu.VMEM((depth, height, chan, width), bf),
            pltpu.VMEM((2, depth * 2 * 2 * chan, depth * 4 * 3 * chan), bf),
            pltpu.VMEM((2, depth * 4 * chan, depth * 6 * 6 * chan), bf),
            pltpu.VMEM((2, depth * 4 * chan, depth * 6 * 3 * chan), bf),
            pltpu.VMEM((2 * width, 2 * width), bf),
            pltpu.VMEM((height // 4, depth * 4 * chan, 2 * width), f32),
            pltpu.VMEM((3, 9 * chan, chan), f32),
            pltpu.VMEM((2, tiles, 8, width), f32),
            pltpu.VMEM((2, total - 1, 8, width), f32),
            pltpu.VMEM((2, 8, width), f32),
            pltpu.VMEM((2, tiles, 8, width), f32),
            pltpu.SemaphoreType.DMA((3, 27)),
            pltpu.SemaphoreType.DMA((3, 27)),
            pltpu.SemaphoreType.DMA((2,)),
            pltpu.SemaphoreType.DMA((2,)),
            pltpu.SemaphoreType.DMA((2,)),
            pltpu.SemaphoreType.DMA((2,)),
        ],
        compiler_params=pltpu.CompilerParams(
            collective_id=0, has_side_effects=True, vmem_limit_bytes=48 * 1024 * 1024
        ),
    )(cells, w1, w2, w3, v_first.reshape(filt, chan), v_second.reshape(filt, chan))
    return (
        jnp.transpose(jv, (2, 0, 1, 3)),
        corr1.reshape(v_first.shape),
        corr2.reshape(v_second.shape),
    )


def solution(mesh):
    in_specs = (P(None, "gx", "gy", "gz"), P(), P(), P(), P())
    out_specs = (P(None, "gx", "gy", "gz"), P(), P())
    return jax.shard_map(body, mesh=mesh, in_specs=in_specs, out_specs=out_specs, check_vma=False)
```

```python
import functools
import itertools
import math

import jax
import jax.numpy as jnp
from jax import lax
from jax.experimental import pallas as pl
from jax.experimental.pallas import tpu as pltpu
from jax.sharding import PartitionSpec as P

MESH = pl.DeviceIdType.MESH
AXES = ("gx", "gy", "gz")
STEPS = [d for d in itertools.product((-1, 0, 1), repeat=3) if d != (0, 0, 0)]
STEPS.sort(key=lambda d: (d[2] != 0, d[0] == 0, abs(d[0]) + abs(d[1])))
NT = (((1,), (1,)), ((), ()))


def gelu_pair(pre):
    inner = 0.7978845608 * (pre + 0.044715 * pre * pre * pre)
    hyper = jnp.tanh(inner)
    hidden = 0.5 * pre * (1.0 + hyper)
    slope = 0.5 * (1.0 + hyper) + 0.5 * pre * (1.0 - hyper * hyper) * 0.7978845608 * (
        1.0 + 0.134145 * pre * pre
    )
    return hidden, slope


def code(step):
    return (step[0] + 1) * 9 + (step[1] + 1) * 3 + step[2] + 1


def kernel(
    sizes,
    volume_hbm,
    wf_hbm,
    ws_hbm,
    vf_hbm,
    vs_hbm,
    jv_out,
    gv1,
    gv2,
    *scratch,
):
    (rv, rp, rj, zv, zp, zj, ev, ep, ej, sv, sp, sj, slope_ref, back_ref,
     t1, t2, t3, shift, keep, acc, pack, land, part, full,
     hsend, hrecv, asend, arecv, bsend, brecv,
     volume, wf, ws, vf, vs, w1, w2, w3, isem) = scratch
    chan, depth, height, width = volume.shape
    loads = [
        pltpu.make_async_copy(src, dst, isem.at[i])
        for i, (src, dst) in enumerate(
            (
                (volume_hbm, volume),
                (wf_hbm, wf),
                (ws_hbm, ws),
                (vf_hbm, vf),
                (vs_hbm, vs),
            )
        )
    ]
    for load in loads:
        load.start()
    me = tuple(lax.axis_index(a) for a in AXES)
    total = sizes[0] * sizes[1] * sizes[2]
    line = (me[0] * sizes[1] + me[1]) * sizes[2] + me[2]

    def place(index):
        return (
            index // (sizes[1] * sizes[2]),
            index // sizes[2] % sizes[1],
            index % sizes[2],
        )

    def there(step):
        ok = None
        for pos, size, delta in zip(me, sizes, step):
            if delta == -1:
                term = pos > 0
            elif delta == 1:
                term = pos < size - 1
            else:
                continue
            ok = term if ok is None else jnp.logical_and(ok, term)
        return ok

    barrier = pltpu.get_barrier_semaphore()
    near_only = max(sizes) <= 4

    if near_only:
        greeted = 0
        for step in STEPS:
            ok = there(step)
            greeted = greeted + jnp.where(ok, 1, 0)

            @pl.when(ok)
            def _():
                pl.semaphore_signal(
                    barrier,
                    inc=1,
                    device_id=tuple(p + d for p, d in zip(me, step)),
                    device_id_type=MESH,
                )
    else:
        greeted = total - 1

        @pl.loop(1, total)
        def _(i):
            pl.semaphore_signal(
                barrier, inc=1, device_id=place(lax.rem(line + i, total)), device_id_type=MESH
            )

    def source(delta, extent):
        return {-1: pl.ds(1, 1), 1: pl.ds(extent, 1), 0: pl.ds(1, extent)}[delta]

    def target(delta, extent):
        return {-1: pl.ds(extent + 1, 1), 1: pl.ds(0, 1), 0: pl.ds(1, extent)}[delta]

    def landing(step, rows, zbuf):
        if step[2] == 0:
            return rows.at[target(step[0], depth), target(step[1], height)]
        return zbuf.at[0 if step[2] == 1 else 1, 1 - step[0], 1 - step[1]]

    def message(step, rows, zbuf, edge, slot):
        if step[2] == 0:
            src = rows.at[source(step[0], depth), source(step[1], height)]
        else:
            src = edge
        return pltpu.make_async_remote_copy(
            src_ref=src,
            dst_ref=landing(step, rows, zbuf),
            send_sem=hsend.at[slot, code(step)],
            recv_sem=hrecv.at[slot, code(step)],
            device_id=tuple(p + d for p, d in zip(me, step)),
            device_id_type=MESH,
        )

    def send(rows, zbuf, edge, slot, cross):
        for step in STEPS:
            if (step[2] != 0) == cross:

                @pl.when(there(step))
                def _():
                    message(step, rows, zbuf, edge, slot).start()

    def clear(rows, zbuf):
        for step in STEPS:
            back = tuple(-d for d in step)

            @pl.when(jnp.logical_not(there(back)))
            def _():
                ref = landing(step, rows, zbuf)
                ref[...] = jnp.zeros(ref.shape, ref.dtype)

    def receive(rows, zbuf, edge, slot, kind):
        for step in STEPS:
            if (step[0] != 0) != (kind == 1):
                continue
            back = tuple(-d for d in step)

            @pl.when(there(back))
            def _():
                message(step, rows, zbuf, edge, slot).wait_recv()

    def stage(rows, zbuf, edge, slot, out, table, group, finish):
        for kind in range(2):
            receive(rows, zbuf, edge, slot, kind)
            spread(rows, zbuf, out, (near, far)[kind])
            convolve(table, out, group, kind, finish)

    def sent(rows, zbuf, edge, slot):
        for step in STEPS:

            @pl.when(there(step))
            def _():
                message(step, rows, zbuf, edge, slot).wait_send()

    def edges(rows, edge):
        count = rows.shape[2]
        lane = lax.broadcasted_iota(jnp.int32, (count, width), 1)
        cells = depth * height
        built = jnp.zeros((count, width), jnp.float32)
        for x in range(depth):

            def step(y, built, x=x):
                row = rows[x + 1, y + 1].astype(jnp.float32)
                at = x * height + y
                built = jnp.where(lane == at, pltpu.roll(row, at, 1), built)
                return jnp.where(lane == cells + at, pltpu.roll(row, cells + at + 1, 1), built)

            built = lax.fori_loop(0, height, step, built, unroll=4)
        edge[...] = built.astype(edge.dtype)

    def shifter():
        src = lax.broadcasted_iota(jnp.int32, (2 * width, 2 * width), 0)
        dst = lax.broadcasted_iota(jnp.int32, (2 * width, 2 * width), 1)
        cells = depth * height
        low = jnp.logical_or(
            jnp.logical_and(src == dst - 1, src < width - 1),
            jnp.logical_and(
                dst == 0, jnp.logical_and(src >= width + cells, src < width + 2 * cells)
            ),
        )
        high = jnp.logical_or(
            jnp.logical_and(src == dst - width + 1, src < width),
            jnp.logical_and(
                dst == 2 * width - 1, jnp.logical_and(src >= width, src < width + cells)
            ),
        )
        pick = jnp.logical_or(
            jnp.logical_and(dst < width, low), jnp.logical_and(dst >= width, high)
        )
        shift[...] = jnp.where(pick, 1.0, 0.0).astype(shift.dtype)

    near = tuple(range(1, depth + 1))
    far = (0, depth + 1)

    def spread(rows, zbuf, out, planes):
        count = rows.shape[2]
        groups = count // chan
        lane = lax.broadcasted_iota(jnp.int32, (count, width), 1)
        cells = depth * height

        for xp in planes:
            dx = 0 if xp == 0 else (2 if xp == depth + 1 else 1)
            halo = []
            for yp in range(height + 2):
                dy = 0 if yp == 0 else (2 if yp == height + 1 else 1)
                left = zbuf[0, dx, dy].astype(jnp.float32)
                right = zbuf[1, dx, dy].astype(jnp.float32)
                at = (xp - 1) % depth * height + (yp - 1) % height
                both = jnp.where(lane == at, right, jnp.where(lane == cells + at, left, 0.0))
                halo.append(both.astype(rows.dtype))
            wide = rows[xp].reshape((height + 2) * count, width)
            lhs = jnp.concatenate([wide, jnp.concatenate(halo, axis=0)], axis=1)
            moved = jnp.dot(lhs, shift[...], preferred_element_type=jnp.float32)
            moved = moved.astype(rows.dtype).reshape(height + 2, count, 2 * width)
            kept = wide.reshape(height + 2, count, width)
            for g in range(groups):
                at = slice(g * chan, (g + 1) * chan)
                base = g * 3 * chan
                out[xp, :, base : base + chan] = moved[:, at, :width]
                out[xp, :, base + chan : base + 2 * chan] = kept[:, at]
                out[xp, :, base + 2 * chan : base + 3 * chan] = moved[:, at, width:]

    def band(weights, table, group):
        outs = weights.shape[0]
        third = weights.shape[1] // 3
        step = third // 3
        table[...] = jnp.zeros_like(table)
        for kx in range(3):
            piece = weights[:, kx * third : (kx + 1) * third]
            for ox in range(depth):
                xp = ox + kx
                kind, pos = (0, near.index(xp)) if xp in near else (1, far.index(xp))
                for oy in range(group):
                    row = (ox * group + oy) * outs
                    at = (pos * (group + 2) + oy) * step
                    table[kind, row : row + outs, at : at + third] = piece

    def convolve(table, ref, group, kind, finish):
        outs = table.shape[1] // (depth * group)
        planes = (near, far)[kind]

        @pl.loop(0, height // (2 * group))
        def _(j):
            halves = []
            for half in range(2):
                y = (2 * j + half) * group
                halves.append(
                    jnp.concatenate(
                        [
                            ref[xp, pl.ds(y, group + 2)].reshape(
                                (group + 2) * ref.shape[2], width
                            )
                            for xp in planes
                        ],
                        axis=0,
                    )
                )
            rhs = jnp.concatenate(halves, axis=1)
            out = jnp.dot(
                table[kind, :, : rhs.shape[0]], rhs, preferred_element_type=jnp.float32
            )
            if kind == 0:
                keep[j] = out
                return
            out = out + keep[j]
            for half in range(2):
                for ox in range(depth):
                    for oy in range(group):
                        row = (ox * group + oy) * outs
                        finish(
                            ox,
                            (2 * j + half) * group + oy,
                            out[row : row + outs, half * width : (half + 1) * width],
                        )

    def correlate(ref, rows, offset):
        acc[...] = jnp.zeros_like(acc)
        for x in range(depth):

            @pl.loop(0, height // 4)
            def _(j, x=x):
                y = 4 * j
                rhs = jnp.concatenate(
                    [rows[x + offset, y + i + offset] for i in range(4)], axis=1
                )
                for kx in range(3):
                    lhs = jnp.concatenate(
                        [
                            ref[x + kx, pl.ds(y + i, 3), : 3 * chan].reshape(9 * chan, width)
                            for i in range(4)
                        ],
                        axis=1,
                    )
                    acc[kx] += lax.dot_general(lhs, rhs, NT, preferred_element_type=jnp.float32)

    tiles = pack.shape[1]
    cells_all = float(depth * height * width * total)
    factor = math.sqrt(27.0 * chan)

    def owner(t):
        return t * total // tiles

    span = 8 * tiles
    lanes = width // chan

    def scatter(slot):
        for j in range(lanes):
            flat = acc[...].reshape(27 * chan, chan)
            pack[slot, :, :, j * chan : (j + 1) * chan] = flat[
                j * span : (j + 1) * span
            ].reshape(tiles, 8, chan)
        for t in range(tiles):
            at = owner(t)

            @pl.when(line != at)
            def _():
                pltpu.make_async_remote_copy(
                    src_ref=pack.at[slot, t],
                    dst_ref=land.at[slot, lax.rem(line - at + total, total) - 1],
                    send_sem=asend.at[slot],
                    recv_sem=arecv.at[slot],
                    device_id=place(at),
                    device_id_type=MESH,
                ).start()

    def gather(slot):
        for t in range(tiles):

            @pl.when(line == owner(t))
            def _():
                pltpu.make_async_copy(
                    land.at[slot], land.at[slot], arecv.at[slot]
                ).wait()
                summed = pack[slot, t] + jnp.sum(land[slot], axis=0)
                part[slot] = summed
                full[slot, t] = summed

                @pl.loop(1, total)
                def _(i):
                    pltpu.make_async_remote_copy(
                        src_ref=part.at[slot],
                        dst_ref=full.at[slot, t],
                        send_sem=bsend.at[slot],
                        recv_sem=brecv.at[slot],
                        device_id=place(lax.rem(line + i, total)),
                        device_id_type=MESH,
                    ).start()

    def owning():
        held = line == owner(0)
        for t in range(1, tiles):
            held = jnp.logical_or(held, line == owner(t))
        return held

    def drain(slot, out, direction):
        held = owning()
        for flag, count in ((held, tiles - 1), (jnp.logical_not(held), tiles)):

            @pl.when(flag)
            def _():
                some = full.at[slot, pl.ds(0, count)]
                pltpu.make_async_copy(some, some, brecv.at[slot]).wait()
                mine = pack.at[slot, pl.ds(0, count)]
                pltpu.make_async_copy(mine, mine, asend.at[slot]).wait()

        @pl.when(held)
        def _():
            pltpu.make_async_copy(land.at[slot], land.at[slot], bsend.at[slot]).wait()

        whole = full[slot].reshape(span, width)
        for j in range(lanes):
            at = slice(j * span, (j + 1) * span)
            damp = 0.1 * direction[at].astype(jnp.float32)
            out[at] = factor * (whole[:, j * chan : (j + 1) * chan] / cells_all + damp)

    def arrange():
        filt = 27 * chan
        for load in loads[1:]:
            load.wait()
        four = jnp.concatenate([wf[...], vf[...], vs[...], ws[...]], axis=1)
        rows = lax.broadcasted_iota(jnp.int32, (4 * chan, 4 * chan), 0)
        cols = lax.broadcasted_iota(jnp.int32, (4 * chan, 4 * chan), 1)
        eye = jnp.where(rows == cols, 1.0, 0.0).astype(four.dtype)
        turned = lax.dot_general(eye, four, NT, preferred_element_type=jnp.float32)
        turned = turned.astype(w1.dtype)
        w1[...] = turned[: 2 * chan]
        third = 3 * chan
        for k in range(9):
            part = slice(k * third, (k + 1) * third)
            w2[:, 2 * k * third : (2 * k + 1) * third] = turned[2 * chan : 3 * chan, part]
            w2[:, (2 * k + 1) * third : (2 * k + 2) * third] = turned[3 * chan :, part]
        for k in range(27):
            at = filt - (k + 1) * chan
            w3[:, k * chan : (k + 1) * chan] = ws[at : at + chan]

    inner = (slice(1, depth + 1), slice(1, height + 1))
    loads[0].wait()
    for x in range(depth):
        rv[x + 1, 1 : height + 1] = jnp.swapaxes(volume[:, x], 0, 1)
    pl.semaphore_wait(barrier, greeted)
    send(rv, zv, ev, 0, False)
    edges(rv, ev)
    send(rv, zv, ev, 0, True)
    for rows, zbuf in ((rv, zv), (rp, zp), (rj, zj)):
        clear(rows, zbuf)
    shifter()
    arrange()
    band(w1, t1, 2)
    band(w2, t2, 4)
    band(w3, t3, 4)

    def first(x, y, out):
        hidden, slope = gelu_pair(out[:chan])
        slope_ref[x, y] = slope
        rp[x + 1, y + 1, :chan] = hidden.astype(jnp.bfloat16)
        rp[x + 1, y + 1, chan:] = (slope * out[chan:]).astype(jnp.bfloat16)

    stage(rv, zv, ev, 0, sv, t1, 2, first)
    send(rp, zp, ep, 1, False)
    edges(rp, ep)
    send(rp, zp, ep, 1, True)

    def second(x, y, out):
        rj[x + 1, y + 1] = out.astype(jnp.bfloat16)

    stage(rp, zp, ep, 1, sp, t2, 4, second)
    send(rj, zj, ej, 2, False)
    edges(rj, ej)
    send(rj, zj, ej, 2, True)
    for x in range(depth):
        jv_out[:, x] = jnp.swapaxes(rj[x + 1, 1 : height + 1], 0, 1)
    correlate(sp, rj, 1)
    scatter(0)

    def third(x, y, out):
        back_ref[x, y] = (slope_ref[x, y] * out).astype(jnp.bfloat16)

    stage(rj, zj, ej, 2, sj, t3, 4, third)
    correlate(sv, back_ref, 0)
    scatter(1)
    gather(0)
    gather(1)
    drain(0, gv2, vs)
    drain(1, gv1, vf)
    sent(rv, zv, ev, 0)
    sent(rp, zp, ep, 1)
    sent(rj, zj, ej, 2)


def place_out(*refs):
    count = len(refs) // 2
    sems = refs[-1]
    copies = [
        pltpu.make_async_copy(refs[i], refs[count + i], sems.at[i]) for i in range(count)
    ]
    for copy in copies:
        copy.start()
    for copy in copies:
        copy.wait()


def body(volume, w_first, w_second, v_first, v_second):
    chan, depth, height, width = volume.shape
    sizes = tuple(lax.axis_size(a) for a in AXES)
    total = sizes[0] * sizes[1] * sizes[2]
    filt = 27 * chan
    tiles = filt * chan // (8 * width)
    bf, f32 = jnp.bfloat16, jnp.float32
    pads = (depth + 2, height + 2)
    vmem = pl.BlockSpec(memory_space=pltpu.VMEM)
    jv, corr1, corr2 = pl.pallas_call(
        functools.partial(kernel, sizes),
        out_shape=(
            jax.ShapeDtypeStruct(volume.shape, bf),
            jax.ShapeDtypeStruct((filt, chan), f32),
            jax.ShapeDtypeStruct((filt, chan), f32),
        ),
        in_specs=[pl.BlockSpec(memory_space=pltpu.HBM)] * 5,
        out_specs=(vmem,) * 3,
        scratch_shapes=[
            pltpu.VMEM(pads + (chan, width), bf),
            pltpu.VMEM(pads + (2 * chan, width), bf),
            pltpu.VMEM(pads + (chan, width), bf),
            pltpu.VMEM((2, 3, 3, chan, width), bf),
            pltpu.VMEM((2, 3, 3, 2 * chan, width), bf),
            pltpu.VMEM((2, 3, 3, chan, width), bf),
            pltpu.VMEM((chan, width), bf),
            pltpu.VMEM((2 * chan, width), bf),
            pltpu.VMEM((chan, width), bf),
            pltpu.VMEM(pads + (3 * chan, width), bf),
            pltpu.VMEM(pads + (6 * chan, width), bf),
            pltpu.VMEM(pads + (3 * chan, width), bf),
            pltpu.VMEM((depth, height, chan, width), f32),
            pltpu.VMEM((depth, height, chan, width), bf),
            pltpu.VMEM((2, depth * 2 * 2 * chan, depth * 4 * 3 * chan), bf),
            pltpu.VMEM((2, depth * 4 * chan, depth * 6 * 6 * chan), bf),
            pltpu.VMEM((2, depth * 4 * chan, depth * 6 * 3 * chan), bf),
            pltpu.VMEM((2 * width, 2 * width), bf),
            pltpu.VMEM((height // 4, depth * 4 * chan, 2 * width), f32),
            pltpu.VMEM((3, 9 * chan, chan), f32),
            pltpu.VMEM((2, tiles, 8, width), f32),
            pltpu.VMEM((2, total - 1, 8, width), f32),
            pltpu.VMEM((2, 8, width), f32),
            pltpu.VMEM((2, tiles, 8, width), f32),
            pltpu.SemaphoreType.DMA((3, 27)),
            pltpu.SemaphoreType.DMA((3, 27)),
            pltpu.SemaphoreType.DMA((2,)),
            pltpu.SemaphoreType.DMA((2,)),
            pltpu.SemaphoreType.DMA((2,)),
            pltpu.SemaphoreType.DMA((2,)),
            pltpu.VMEM(volume.shape, bf),
            pltpu.VMEM((filt, chan), bf),
            pltpu.VMEM((filt, chan), bf),
            pltpu.VMEM((filt, chan), bf),
            pltpu.VMEM((filt, chan), bf),
            pltpu.VMEM((2 * chan, filt), bf),
            pltpu.VMEM((chan, 2 * filt), bf),
            pltpu.VMEM((chan, filt), bf),
            pltpu.SemaphoreType.DMA((5,)),
        ],
        compiler_params=pltpu.CompilerParams(
            collective_id=0, has_side_effects=True, vmem_limit_bytes=48 * 1024 * 1024
        ),
    )(*(pltpu.with_memory_space_constraint(w, pltpu.HBM) for w in (volume, *(w.reshape(filt, chan) for w in (w_first, w_second, v_first, v_second)))))
    jv, corr1, corr2 = pl.pallas_call(
        place_out,
        out_shape=(
            jax.ShapeDtypeStruct(volume.shape, bf),
            jax.ShapeDtypeStruct((filt, chan), f32),
            jax.ShapeDtypeStruct((filt, chan), f32),
        ),
        in_specs=[vmem] * 3,
        out_specs=(pl.BlockSpec(memory_space=pltpu.HBM),) * 3,
        scratch_shapes=[pltpu.SemaphoreType.DMA((3,))],
        compiler_params=pltpu.CompilerParams(vmem_limit_bytes=4 * 1024 * 1024),
    )(jv, corr1, corr2)
    return jv, corr1.reshape(v_first.shape), corr2.reshape(v_second.shape)


def solution(mesh):
    in_specs = (P(None, "gx", "gy", "gz"), P(), P(), P(), P())
    out_specs = (P(None, "gx", "gy", "gz"), P(), P())
    return jax.shard_map(body, mesh=mesh, in_specs=in_specs, out_specs=out_specs, check_vma=False)
```

```python
import functools
import itertools
import math

import jax
import jax.numpy as jnp
from jax import lax
from jax.experimental import pallas as pl
from jax.experimental.pallas import tpu as pltpu
from jax.sharding import PartitionSpec as P

MESH = pl.DeviceIdType.MESH
AXES = ("gx", "gy", "gz")
STEPS = [d for d in itertools.product((-1, 0, 1), repeat=3) if d != (0, 0, 0)]
STEPS.sort(key=lambda d: (d[2] != 0, d[0] == 0, abs(d[0]) + abs(d[1])))
NT = (((1,), (1,)), ((), ()))


def gelu_pair(pre):
    inner = 0.7978845608 * (pre + 0.044715 * pre * pre * pre)
    hyper = jnp.tanh(inner)
    hidden = 0.5 * pre * (1.0 + hyper)
    slope = 0.5 * (1.0 + hyper) + 0.5 * pre * (1.0 - hyper * hyper) * 0.7978845608 * (
        1.0 + 0.134145 * pre * pre
    )
    return hidden, slope


def codes(sizes):
    spans = [3 if size > 2 else 2 for size in sizes]

    def code(step):
        total = 0
        for delta, span in zip(step, spans):
            total = total * span + (delta + 1 if span == 3 else abs(delta))
        return total

    return code, math.prod(spans)


def kernel(
    sizes,
    volume_hbm,
    wf_hbm,
    ws_hbm,
    vf_hbm,
    vs_hbm,
    jv_out,
    gv1,
    gv2,
    *scratch,
):
    (rv, rp, rj, zv, zp, zj, ev, ep, ej, sv, sp, sj, slope_ref, back_ref,
     t1, t2, t3, shift, keep, prod, diag, pack, land, part, full,
     hsend, hrecv, asend, arecv, bsend, brecv,
     volume, wf, ws, vf, vs, w1, w2, w3, isem) = scratch
    chan, depth, height, width = volume.shape
    code, _ = codes(sizes)
    loads = [
        pltpu.make_async_copy(src, dst, isem.at[i])
        for i, (src, dst) in enumerate(
            (
                (volume_hbm, volume),
                (wf_hbm, wf),
                (ws_hbm, ws),
                (vf_hbm, vf),
                (vs_hbm, vs),
            )
        )
    ]
    for load in loads:
        load.start()
    me = tuple(lax.axis_index(a) for a in AXES)
    total = sizes[0] * sizes[1] * sizes[2]
    line = (me[0] * sizes[1] + me[1]) * sizes[2] + me[2]

    def place(index):
        return (
            index // (sizes[1] * sizes[2]),
            index // sizes[2] % sizes[1],
            index % sizes[2],
        )

    def there(step):
        ok = None
        for pos, size, delta in zip(me, sizes, step):
            if delta == -1:
                term = pos > 0
            elif delta == 1:
                term = pos < size - 1
            else:
                continue
            ok = term if ok is None else jnp.logical_and(ok, term)
        return ok

    barrier = pltpu.get_barrier_semaphore()
    near_only = max(sizes) <= 4

    if near_only:
        greeted = 0
        for step in STEPS:
            ok = there(step)
            greeted = greeted + jnp.where(ok, 1, 0)

            @pl.when(ok)
            def _():
                pl.semaphore_signal(
                    barrier,
                    inc=1,
                    device_id=tuple(p + d for p, d in zip(me, step)),
                    device_id_type=MESH,
                )
    else:
        greeted = total - 1

        @pl.loop(1, total)
        def _(i):
            pl.semaphore_signal(
                barrier, inc=1, device_id=place(lax.rem(line + i, total)), device_id_type=MESH
            )

    def source(delta, extent):
        return {-1: pl.ds(1, 1), 1: pl.ds(extent, 1), 0: pl.ds(1, extent)}[delta]

    def target(delta, extent):
        return {-1: pl.ds(extent + 1, 1), 1: pl.ds(0, 1), 0: pl.ds(1, extent)}[delta]

    def landing(step, rows, zbuf):
        if step[2] == 0:
            return rows.at[target(step[0], depth), target(step[1], height)]
        return zbuf.at[0 if step[2] == 1 else 1, 1 - step[0], 1 - step[1]]

    def message(step, rows, zbuf, edge, slot):
        if step[2] == 0:
            src = rows.at[source(step[0], depth), source(step[1], height)]
        else:
            src = edge
        return pltpu.make_async_remote_copy(
            src_ref=src,
            dst_ref=landing(step, rows, zbuf),
            send_sem=hsend.at[code(step)],
            recv_sem=hrecv.at[slot % 2, code(step)],
            device_id=tuple(p + d for p, d in zip(me, step)),
            device_id_type=MESH,
        )

    def send(rows, zbuf, edge, slot, cross):
        for step in STEPS:
            if (step[2] != 0) == cross:

                @pl.when(there(step))
                def _():
                    message(step, rows, zbuf, edge, slot).start()

    def clear(rows, zbuf):
        for step in STEPS:
            back = tuple(-d for d in step)

            @pl.when(jnp.logical_not(there(back)))
            def _():
                ref = landing(step, rows, zbuf)
                ref[...] = jnp.zeros(ref.shape, ref.dtype)

    def receive(rows, zbuf, edge, slot, kind):
        for step in STEPS:
            if (step[0] != 0) != (kind == 1):
                continue
            back = tuple(-d for d in step)

            @pl.when(there(back))
            def _():
                message(step, rows, zbuf, edge, slot).wait_recv()

    def stage(rows, zbuf, edge, slot, out, table, group, finish):
        for kind in range(2):
            receive(rows, zbuf, edge, slot, kind)
            spread(rows, zbuf, out, (near, far)[kind])
            convolve(table, out, group, kind, finish)

    def sent(rows, zbuf, edge, slot):
        for step in STEPS:

            @pl.when(there(step))
            def _():
                message(step, rows, zbuf, edge, slot).wait_send()

    def edges(rows, edge):
        count = rows.shape[2]
        lane = lax.broadcasted_iota(jnp.int32, (count, width), 1)
        cells = depth * height
        built = jnp.zeros((count, width), jnp.float32)
        for x in range(depth):

            def step(y, built, x=x):
                row = rows[x + 1, y + 1].astype(jnp.float32)
                at = x * height + y
                built = jnp.where(lane == at, pltpu.roll(row, at, 1), built)
                return jnp.where(lane == cells + at, pltpu.roll(row, cells + at + 1, 1), built)

            built = lax.fori_loop(0, height, step, built, unroll=4)
        edge[...] = built.astype(edge.dtype)

    def shifter():
        src = lax.broadcasted_iota(jnp.int32, (2 * width, 2 * width), 0)
        dst = lax.broadcasted_iota(jnp.int32, (2 * width, 2 * width), 1)
        cells = depth * height
        low = jnp.logical_or(
            jnp.logical_and(src == dst - 1, src < width - 1),
            jnp.logical_and(
                dst == 0, jnp.logical_and(src >= width + cells, src < width + 2 * cells)
            ),
        )
        high = jnp.logical_or(
            jnp.logical_and(src == dst - width + 1, src < width),
            jnp.logical_and(
                dst == 2 * width - 1, jnp.logical_and(src >= width, src < width + cells)
            ),
        )
        pick = jnp.logical_or(
            jnp.logical_and(dst < width, low), jnp.logical_and(dst >= width, high)
        )
        shift[...] = jnp.where(pick, 1.0, 0.0).astype(shift.dtype)

    near = tuple(range(1, depth + 1))
    far = (0, depth + 1)

    def spread(rows, zbuf, out, planes):
        count = rows.shape[2]
        groups = count // chan
        lane = lax.broadcasted_iota(jnp.int32, (count, width), 1)
        cells = depth * height

        for xp in planes:
            dx = 0 if xp == 0 else (2 if xp == depth + 1 else 1)
            halo = []
            for yp in range(height + 2):
                dy = 0 if yp == 0 else (2 if yp == height + 1 else 1)
                left = zbuf[0, dx, dy].astype(jnp.float32)
                right = zbuf[1, dx, dy].astype(jnp.float32)
                at = (xp - 1) % depth * height + (yp - 1) % height
                both = jnp.where(lane == at, right, jnp.where(lane == cells + at, left, 0.0))
                halo.append(both.astype(rows.dtype))
            wide = rows[xp].reshape((height + 2) * count, width)
            lhs = jnp.concatenate([wide, jnp.concatenate(halo, axis=0)], axis=1)
            moved = jnp.dot(lhs, shift[...], preferred_element_type=jnp.float32)
            moved = moved.astype(rows.dtype).reshape(height + 2, count, 2 * width)
            kept = wide.reshape(height + 2, count, width)
            for g in range(groups):
                at = slice(g * chan, (g + 1) * chan)
                base = g * 3 * chan
                out[xp, :, base : base + chan] = moved[:, at, :width]
                out[xp, :, base + chan : base + 2 * chan] = kept[:, at]
                out[xp, :, base + 2 * chan : base + 3 * chan] = moved[:, at, width:]

    def band(weights, table, group):
        outs = weights.shape[0]
        third = weights.shape[1] // 3
        step = third // 3
        table[...] = jnp.zeros_like(table)
        for kx in range(3):
            piece = weights[:, kx * third : (kx + 1) * third]
            for ox in range(depth):
                xp = ox + kx
                kind, pos = (0, near.index(xp)) if xp in near else (1, far.index(xp))
                for oy in range(group):
                    row = (ox * group + oy) * outs
                    at = (pos * (group + 2) + oy) * step
                    table[kind, row : row + outs, at : at + third] = piece

    def convolve(table, ref, group, kind, finish):
        outs = table.shape[1] // (depth * group)
        planes = (near, far)[kind]

        @pl.loop(0, height // (2 * group))
        def _(j):
            halves = []
            for half in range(2):
                y = (2 * j + half) * group
                halves.append(
                    jnp.concatenate(
                        [
                            ref[xp, pl.ds(y, group + 2)].reshape(
                                (group + 2) * ref.shape[2], width
                            )
                            for xp in planes
                        ],
                        axis=0,
                    )
                )
            rhs = jnp.concatenate(halves, axis=1)
            out = jnp.dot(
                table[kind, :, : rhs.shape[0]], rhs, preferred_element_type=jnp.float32
            )
            if kind == 0:
                keep[j] = out
                return
            out = out + keep[j]
            for half in range(2):
                for ox in range(depth):
                    for oy in range(group):
                        row = (ox * group + oy) * outs
                        finish(
                            ox,
                            (2 * j + half) * group + oy,
                            out[row : row + outs, half * width : (half + 1) * width],
                        )

    tiles = pack.shape[1]
    cells_all = float(depth * height * width * total)
    factor = math.sqrt(27.0 * chan)
    span = 8 * tiles
    lanes = width // chan
    trio = 3 * chan

    def correlate(ref, rows, offset, slot):
        bands = range(0, height, 4)
        lhs = jnp.concatenate(
            [
                ref[:, y : y + 6, :trio].reshape((depth + 2) * 6 * trio, width)
                for y in bands
            ],
            axis=1,
        )
        inner = slice(offset, offset + depth)
        rhs = jnp.concatenate(
            [
                rows[inner, y + offset : y + offset + 4].reshape(depth * 4 * chan, width)
                for y in bands
            ],
            axis=1,
        )
        prod[...] = lax.dot_general(
            lhs, rhs, NT, preferred_element_type=jnp.float32
        ).reshape(prod.shape)

    def fold(slot):
        group = lax.broadcasted_iota(jnp.int32, (8, width), 1) // chan
        for kx in range(3):
            for r in range(0, trio, 8):
                sums = []
                for y in range(6):
                    part = prod[kx, y, r : r + 8, :width]
                    for x in range(1, depth):
                        part = part + prod[kx + x, y, r : r + 8, x * width : (x + 1) * width]
                    sums.append(part)
                for ky in range(3):
                    at = (3 * kx + ky) * trio + r
                    keep_y = sums[ky + 3]
                    for y in (2, 1, 0):
                        keep_y = jnp.where(group == y, sums[ky + y], keep_y)
                    diag[at : at + 8] = keep_y
        low = group < 2
        even = group % 2 == 0
        for t in range(tiles):
            rows = [diag[j * span + 8 * t : j * span + 8 * t + 8] for j in range(4)]
            pairs = []
            for j in range(2):
                one, two = rows[j], rows[j + 2]
                pairs.append(
                    jnp.where(low, one, two)
                    + pltpu.roll(jnp.where(low, two, one), 2 * chan, 1)
                )
            one, two = pairs
            cross = jnp.where(even, two, one)
            pack[slot, t] = jnp.where(even, one, two) + jnp.where(
                even, pltpu.roll(cross, width - chan, 1), pltpu.roll(cross, chan, 1)
            )

    mids = min(2, sizes[0])
    first_mid = (sizes[0] - mids) // 2
    owners = mids * sizes[1] * sizes[2]
    rounds = -(-tiles // owners)
    is_mid = jnp.logical_and(me[0] >= first_mid, me[0] < first_mid + mids)
    mine = (me[1] * sizes[2] + me[2]) * mids + me[0] - first_mid

    def owner(t):
        w = t % owners
        return (first_mid + w % mids, w // mids // sizes[2], w // mids % sizes[2])

    def owns(count):
        if count == 0:
            none = jnp.logical_or(jnp.logical_not(is_mid), mine >= tiles)
            return none
        more = mine + (count - 1) * owners < tiles
        last = mine + count * owners >= tiles
        return jnp.logical_and(is_mid, jnp.logical_and(more, last))

    def scatter(slot):
        for t in range(tiles):
            spot = owner(t)
            at = (spot[0] * sizes[1] + spot[1]) * sizes[2] + spot[2]

            @pl.when(line != at)
            def _():
                pltpu.make_async_remote_copy(
                    src_ref=pack.at[slot, t],
                    dst_ref=land.at[slot, t // owners, lax.rem(line - at + total, total) - 1],
                    send_sem=asend.at[slot],
                    recv_sem=arecv.at[slot, t // owners],
                    device_id=spot,
                    device_id_type=MESH,
                ).start()

    def others():
        axes = [
            [me[i] if d == 0 else lax.rem(me[i] + d, sizes[i]) for d in range(sizes[i])]
            for i in range(3)
        ]
        return list(itertools.product(*axes))[1:]

    def gather(slot):
        for r in range(rounds):

            @pl.when(jnp.logical_and(is_mid, mine + r * owners < tiles))
            def _():
                t = mine + r * owners
                landed = land.at[slot, r]
                pltpu.make_async_copy(landed, landed, arecv.at[slot, r]).wait()
                summed = pack[slot, t] + jnp.sum(land[slot, r], axis=0)
                part[slot, r] = summed
                full[slot, t] = summed

                def tell(spot):
                    pltpu.make_async_remote_copy(
                        src_ref=part.at[slot, r],
                        dst_ref=full.at[slot, t],
                        send_sem=bsend.at[slot],
                        recv_sem=brecv.at[slot],
                        device_id=spot,
                        device_id_type=MESH,
                    ).start()

                if total <= 64:
                    for spot in others():
                        tell(spot)
                else:

                    @pl.loop(1, total)
                    def _(i):
                        tell(place(lax.rem(line + i, total)))

    def drain(slot, out, direction):
        for count in range(rounds + 1):

            @pl.when(owns(count))
            def _():
                some = full.at[slot, pl.ds(0, tiles - count)]
                pltpu.make_async_copy(some, some, brecv.at[slot]).wait()
                sent_all = pack.at[slot, pl.ds(0, tiles - count)]
                pltpu.make_async_copy(sent_all, sent_all, asend.at[slot]).wait()
                if count:
                    told = land.at[slot, pl.ds(0, count)]
                    pltpu.make_async_copy(told, told, bsend.at[slot]).wait()

        whole = full[slot].reshape(span, width)
        for j in range(lanes):
            at = slice(j * span, (j + 1) * span)
            damp = 0.1 * direction[at].astype(jnp.float32)
            out[at] = factor * (whole[:, j * chan : (j + 1) * chan] / cells_all + damp)

    def arrange():
        filt = 27 * chan
        for load in loads[1:]:
            load.wait()
        four = jnp.concatenate([wf[...], vf[...], vs[...], ws[...]], axis=1)
        rows = lax.broadcasted_iota(jnp.int32, (4 * chan, 4 * chan), 0)
        cols = lax.broadcasted_iota(jnp.int32, (4 * chan, 4 * chan), 1)
        eye = jnp.where(rows == cols, 1.0, 0.0).astype(four.dtype)
        turned = lax.dot_general(eye, four, NT, preferred_element_type=jnp.float32)
        turned = turned.astype(w1.dtype)
        w1[...] = turned[: 2 * chan]
        third = 3 * chan
        for k in range(9):
            part = slice(k * third, (k + 1) * third)
            w2[:, 2 * k * third : (2 * k + 1) * third] = turned[2 * chan : 3 * chan, part]
            w2[:, (2 * k + 1) * third : (2 * k + 2) * third] = turned[3 * chan :, part]
        for k in range(27):
            at = filt - (k + 1) * chan
            w3[:, k * chan : (k + 1) * chan] = ws[at : at + chan]

    inner = (slice(1, depth + 1), slice(1, height + 1))
    loads[0].wait()
    for x in range(depth):
        rv[x + 1, 1 : height + 1] = jnp.swapaxes(volume[:, x], 0, 1)
    pl.semaphore_wait(barrier, greeted)
    send(rv, zv, ev, 0, False)
    edges(rv, ev)
    send(rv, zv, ev, 0, True)
    for rows, zbuf in ((rv, zv), (rp, zp), (rj, zj)):
        clear(rows, zbuf)
    shifter()
    arrange()
    band(w1, t1, 2)
    band(w2, t2, 4)
    band(w3, t3, 4)

    def first(x, y, out):
        hidden, slope = gelu_pair(out[:chan])
        slope_ref[x, y] = slope
        rp[x + 1, y + 1, :chan] = hidden.astype(jnp.bfloat16)
        rp[x + 1, y + 1, chan:] = (slope * out[chan:]).astype(jnp.bfloat16)

    stage(rv, zv, ev, 0, sv, t1, 2, first)
    sent(rv, zv, ev, 0)
    send(rp, zp, ep, 1, False)
    edges(rp, ep)
    send(rp, zp, ep, 1, True)

    def second(x, y, out):
        rj[x + 1, y + 1] = out.astype(jnp.bfloat16)

    stage(rp, zp, ep, 1, sp, t2, 4, second)
    sent(rp, zp, ep, 1)
    send(rj, zj, ej, 2, False)
    edges(rj, ej)
    send(rj, zj, ej, 2, True)
    for x in range(depth):
        jv_out[:, x] = jnp.swapaxes(rj[x + 1, 1 : height + 1], 0, 1)
    correlate(sp, rj, 1, 0)
    fold(0)
    scatter(0)

    def third(x, y, out):
        back_ref[x, y] = (slope_ref[x, y] * out).astype(jnp.bfloat16)

    stage(rj, zj, ej, 2, sj, t3, 4, third)
    correlate(sv, back_ref, 0, 1)
    fold(1)
    scatter(1)
    gather(0)
    gather(1)
    drain(0, gv2, vs)
    drain(1, gv1, vf)
    sent(rj, zj, ej, 2)


def place_out(*refs):
    count = len(refs) // 2
    sems = refs[-1]
    copies = [
        pltpu.make_async_copy(refs[i], refs[count + i], sems.at[i]) for i in range(count)
    ]
    for copy in copies:
        copy.start()
    for copy in copies:
        copy.wait()


def body(volume, w_first, w_second, v_first, v_second):
    chan, depth, height, width = volume.shape
    sizes = tuple(lax.axis_size(a) for a in AXES)
    total = sizes[0] * sizes[1] * sizes[2]
    filt = 27 * chan
    tiles = filt * chan // (8 * width)
    rounds = -(-tiles // (min(2, sizes[0]) * sizes[1] * sizes[2]))
    _, ways = codes(sizes)
    bf, f32 = jnp.bfloat16, jnp.float32
    pads = (depth + 2, height + 2)
    vmem = pl.BlockSpec(memory_space=pltpu.VMEM)
    jv, corr1, corr2 = pl.pallas_call(
        functools.partial(kernel, sizes),
        out_shape=(
            jax.ShapeDtypeStruct(volume.shape, bf),
            jax.ShapeDtypeStruct((filt, chan), f32),
            jax.ShapeDtypeStruct((filt, chan), f32),
        ),
        in_specs=[pl.BlockSpec(memory_space=pltpu.HBM)] * 5,
        out_specs=(vmem,) * 3,
        scratch_shapes=[
            pltpu.VMEM(pads + (chan, width), bf),
            pltpu.VMEM(pads + (2 * chan, width), bf),
            pltpu.VMEM(pads + (chan, width), bf),
            pltpu.VMEM((2, 3, 3, chan, width), bf),
            pltpu.VMEM((2, 3, 3, 2 * chan, width), bf),
            pltpu.VMEM((2, 3, 3, chan, width), bf),
            pltpu.VMEM((chan, width), bf),
            pltpu.VMEM((2 * chan, width), bf),
            pltpu.VMEM((chan, width), bf),
            pltpu.VMEM(pads + (3 * chan, width), bf),
            pltpu.VMEM(pads + (6 * chan, width), bf),
            pltpu.VMEM(pads + (3 * chan, width), bf),
            pltpu.VMEM((depth, height, chan, width), f32),
            pltpu.VMEM((depth, height, chan, width), bf),
            pltpu.VMEM((2, depth * 2 * 2 * chan, depth * 4 * 3 * chan), bf),
            pltpu.VMEM((2, depth * 4 * chan, depth * 6 * 6 * chan), bf),
            pltpu.VMEM((2, depth * 4 * chan, depth * 6 * 3 * chan), bf),
            pltpu.VMEM((2 * width, 2 * width), bf),
            pltpu.VMEM((height // 4, depth * 4 * chan, 2 * width), f32),
            pltpu.VMEM((depth + 2, 6, 3 * chan, depth * 4 * chan), f32),
            pltpu.VMEM((filt, width), f32),
            pltpu.VMEM((2, tiles, 8, width), f32),
            pltpu.VMEM((2, rounds, total - 1, 8, width), f32),
            pltpu.VMEM((2, rounds, 8, width), f32),
            pltpu.VMEM((2, tiles, 8, width), f32),
            pltpu.SemaphoreType.DMA((ways,)),
            pltpu.SemaphoreType.DMA((2, ways)),
            pltpu.SemaphoreType.DMA((2,)),
            pltpu.SemaphoreType.DMA((2, rounds)),
            pltpu.SemaphoreType.DMA((2,)),
            pltpu.SemaphoreType.DMA((2,)),
            pltpu.VMEM(volume.shape, bf),
            pltpu.VMEM((filt, chan), bf),
            pltpu.VMEM((filt, chan), bf),
            pltpu.VMEM((filt, chan), bf),
            pltpu.VMEM((filt, chan), bf),
            pltpu.VMEM((2 * chan, filt), bf),
            pltpu.VMEM((chan, 2 * filt), bf),
            pltpu.VMEM((chan, filt), bf),
            pltpu.SemaphoreType.DMA((5,)),
        ],
        compiler_params=pltpu.CompilerParams(
            collective_id=0, has_side_effects=True, vmem_limit_bytes=48 * 1024 * 1024
        ),
    )(*(pltpu.with_memory_space_constraint(w, pltpu.HBM) for w in (volume, *(w.reshape(filt, chan) for w in (w_first, w_second, v_first, v_second)))))
    jv, corr1, corr2 = pl.pallas_call(
        place_out,
        out_shape=(
            jax.ShapeDtypeStruct(volume.shape, bf),
            jax.ShapeDtypeStruct((filt, chan), f32),
            jax.ShapeDtypeStruct((filt, chan), f32),
        ),
        in_specs=[vmem] * 3,
        out_specs=(pl.BlockSpec(memory_space=pltpu.HBM),) * 3,
        scratch_shapes=[pltpu.SemaphoreType.DMA((3,))],
        compiler_params=pltpu.CompilerParams(vmem_limit_bytes=4 * 1024 * 1024),
    )(jv, corr1, corr2)
    return jv, corr1.reshape(v_first.shape), corr2.reshape(v_second.shape)


def solution(mesh):
    in_specs = (P(None, "gx", "gy", "gz"), P(), P(), P(), P())
    out_specs = (P(None, "gx", "gy", "gz"), P(), P())
    return jax.shard_map(body, mesh=mesh, in_specs=in_specs, out_specs=out_specs, check_vma=False)
```

```python
import functools
import itertools
import math

import jax
import jax.numpy as jnp
from jax import lax
from jax.experimental import pallas as pl
from jax.experimental.pallas import tpu as pltpu
from jax.sharding import PartitionSpec as P

MESH = pl.DeviceIdType.MESH
AXES = ("gx", "gy", "gz")
STEPS = [d for d in itertools.product((-1, 0, 1), repeat=3) if d != (0, 0, 0)]
STEPS.sort(key=lambda d: (d[2] != 0, d[0] == 0, abs(d[0]) + abs(d[1])))
NT = (((1,), (1,)), ((), ()))


def gelu_pair(pre):
    inner = 0.7978845608 * (pre + 0.044715 * pre * pre * pre)
    hyper = jnp.tanh(inner)
    hidden = 0.5 * pre * (1.0 + hyper)
    slope = 0.5 * (1.0 + hyper) + 0.5 * pre * (1.0 - hyper * hyper) * 0.7978845608 * (
        1.0 + 0.134145 * pre * pre
    )
    return hidden, slope


def codes(sizes):
    spans = [3 if size > 2 else 2 for size in sizes]

    def code(step):
        total = 0
        for delta, span in zip(step, spans):
            total = total * span + (delta + 1 if span == 3 else abs(delta))
        return total

    return code, math.prod(spans)


def kernel(
    sizes,
    volume_hbm,
    wf_hbm,
    ws_hbm,
    vf_hbm,
    vs_hbm,
    jv_out,
    gv1,
    gv2,
    *scratch,
):
    (rv, rp, rj, zv, zp, zj, ev, ep, ej, sv, sp, sj, slope_ref, back_ref,
     t1, t2, t3, shift, keep, prod, diag, pack, land, part, full,
     hsend, hrecv, asend, arecv, bsend, brecv,
     volume, wf, ws, vf, vs, w1, w2, w3, isem) = scratch
    chan, depth, height, width = volume.shape
    code, ways = codes(sizes)
    early = height - 4
    bands = (early - 1) // 8
    cuts = ((height,), (4, early, height), (8 * bands, height))
    loads = [
        pltpu.make_async_copy(src, dst, isem.at[i])
        for i, (src, dst) in enumerate(
            (
                (volume_hbm, volume),
                (wf_hbm, wf),
                (ws_hbm, ws),
                (vf_hbm, vf),
                (vs_hbm, vs),
            )
        )
    ]
    for load in loads:
        load.start()
    me = tuple(lax.axis_index(a) for a in AXES)
    total = sizes[0] * sizes[1] * sizes[2]
    line = (me[0] * sizes[1] + me[1]) * sizes[2] + me[2]

    def place(index):
        return (
            index // (sizes[1] * sizes[2]),
            index // sizes[2] % sizes[1],
            index % sizes[2],
        )

    def there(step):
        ok = None
        for pos, size, delta in zip(me, sizes, step):
            if delta == -1:
                term = pos > 0
            elif delta == 1:
                term = pos < size - 1
            else:
                continue
            ok = term if ok is None else jnp.logical_and(ok, term)
        return ok

    barrier = pltpu.get_barrier_semaphore()
    near_only = max(sizes) <= 4

    if near_only:
        greeted = 0
        for step in STEPS:
            ok = there(step)
            greeted = greeted + jnp.where(ok, 1, 0)

            @pl.when(ok)
            def _():
                pl.semaphore_signal(
                    barrier,
                    inc=1,
                    device_id=tuple(p + d for p, d in zip(me, step)),
                    device_id_type=MESH,
                )
    else:
        greeted = total - 1

        @pl.loop(1, total)
        def _(i):
            pl.semaphore_signal(
                barrier, inc=1, device_id=place(lax.rem(line + i, total)), device_id_type=MESH
            )

    def source(delta, extent):
        return {-1: pl.ds(1, 1), 1: pl.ds(extent, 1), 0: pl.ds(1, extent)}[delta]

    def target(delta, extent):
        return {-1: pl.ds(extent + 1, 1), 1: pl.ds(0, 1), 0: pl.ds(1, extent)}[delta]

    def pieces(step, slot):
        if step[1] or step[2]:
            return [None]
        ends = cuts[slot]
        return [(p, lo, hi) for p, (lo, hi) in enumerate(zip((0,) + ends, ends))]

    def landing(step, rows, zbuf, piece=None):
        if step[2] == 0:
            if piece is None:
                return rows.at[target(step[0], depth), target(step[1], height)]
            _, lo, hi = piece
            return rows.at[target(step[0], depth), pl.ds(1 + lo, hi - lo)]
        return zbuf.at[0 if step[2] == 1 else 1, 1 - step[0], 1 - step[1]]

    def message(step, rows, zbuf, edge, slot, piece=None):
        lane = code(step)
        if step[2] != 0:
            src = edge
        elif piece is None:
            src = rows.at[source(step[0], depth), source(step[1], height)]
        else:
            part, lo, hi = piece
            src = rows.at[source(step[0], depth), pl.ds(1 + lo, hi - lo)]
            if part:
                lane = ways + 2 * (part - 1) + (step[0] > 0)
        return pltpu.make_async_remote_copy(
            src_ref=src,
            dst_ref=landing(step, rows, zbuf, piece),
            send_sem=hsend.at[lane],
            recv_sem=hrecv.at[slot % 2, lane],
            device_id=tuple(p + d for p, d in zip(me, step)),
            device_id_type=MESH,
        )

    def send_faces(halo, part):
        for step in STEPS:
            found = pieces(step, halo[3])
            if found == [None] or part >= len(found):
                continue

            @pl.when(there(step))
            def _():
                message(step, *halo, found[part]).start()

    def send_rest(halo, cross):
        for step in STEPS:
            if (step[2] != 0) == cross and pieces(step, halo[3]) == [None]:

                @pl.when(there(step))
                def _():
                    message(step, *halo).start()

    def clear(rows, zbuf):
        for step in STEPS:
            back = tuple(-d for d in step)

            @pl.when(jnp.logical_not(there(back)))
            def _():
                ref = landing(step, rows, zbuf)
                ref[...] = jnp.zeros(ref.shape, ref.dtype)

    def receive(halo, kind, parts):
        for step in STEPS:
            if (step[0] != 0) != (kind == 1):
                continue
            found = pieces(step, halo[3])
            if found == [None]:
                found = found if 0 in parts else []
            else:
                found = [piece for piece in found if piece[0] in parts]
            if not found:
                continue
            back = tuple(-d for d in step)

            @pl.when(there(back))
            def _():
                for piece in found:
                    message(step, *halo, piece).wait_recv()

    def stage(halo, out, table, group, finish, plan):
        rows, zbuf, _, slot = halo
        receive(halo, 0, (0,))
        spread(rows, zbuf, out, near, 0, height + 2)
        convolve(table, out, group, 0, finish, 0, height // (2 * group))
        done = 0
        for parts, upto, hook in plan:
            if parts:
                receive(halo, 1, parts)
                last = cuts[slot][parts[-1]]
                end = height + 2 if last == height else last + 1
                start = 0 if parts[0] == 0 else cuts[slot][parts[0] - 1] + 1
                spread(rows, zbuf, out, far, start, end)
            convolve(table, out, group, 1, finish, done, upto)
            done = upto
            hook()

    def sent(halo):
        for step in STEPS:

            @pl.when(there(step))
            def _():
                for piece in pieces(step, halo[3]):
                    message(step, *halo, piece).wait_send()

    cells = depth * height
    folds = 2 if 4 * cells <= width else 1
    pitch = width // folds

    def edges(rows, edge):
        count = edge.shape[0]
        lane = lax.broadcasted_iota(jnp.int32, (count, width), 1)
        built = jnp.zeros((count, width), jnp.float32)
        for x in range(depth):

            def step(y, built, x=x):
                for f in range(folds):
                    row = rows[x + 1, y + 1, f * count : (f + 1) * count].astype(jnp.float32)
                    at = f * pitch + x * height + y
                    built = jnp.where(lane == at, pltpu.roll(row, at, 1), built)
                    at = at + cells
                    built = jnp.where(lane == at, pltpu.roll(row, at + 1, 1), built)
                return built

            built = lax.fori_loop(0, height, step, built, unroll=4)
        edge[...] = built.astype(edge.dtype)

    def shifter():
        src = lax.broadcasted_iota(jnp.int32, (2 * width, 2 * width), 0)
        dst = lax.broadcasted_iota(jnp.int32, (2 * width, 2 * width), 1)
        spot = src % pitch
        right = jnp.logical_and(src >= width, spot < cells)
        left = jnp.logical_and(
            src >= width, jnp.logical_and(spot >= cells, spot < 2 * cells)
        )
        low = jnp.logical_or(
            jnp.logical_and(src == dst - 1, src < width - 1),
            jnp.logical_and(dst == 0, left),
        )
        high = jnp.logical_or(
            jnp.logical_and(src == dst - width + 1, src < width),
            jnp.logical_and(dst == 2 * width - 1, right),
        )
        pick = jnp.logical_or(
            jnp.logical_and(dst < width, low), jnp.logical_and(dst >= width, high)
        )
        shift[...] = jnp.where(pick, 1.0, 0.0).astype(shift.dtype)

    near = tuple(range(1, depth + 1))
    far = (0, depth + 1)

    def spread(rows, zbuf, out, planes, start, end):
        count = rows.shape[2]
        part = zbuf.shape[3]
        groups = count // chan
        span = end - start
        lane = lax.broadcasted_iota(jnp.int32, (part, width), 1)

        for xp in planes:
            dx = 0 if xp == 0 else (2 if xp == depth + 1 else 1)
            halo = []
            for yp in range(start, end):
                dy = 0 if yp == 0 else (2 if yp == height + 1 else 1)
                left = zbuf[0, dx, dy].astype(jnp.float32)
                right = zbuf[1, dx, dy].astype(jnp.float32)
                for f in range(folds):
                    at = f * pitch + (xp - 1) % depth * height + (yp - 1) % height
                    both = jnp.where(
                        lane == at, right, jnp.where(lane == cells + at, left, 0.0)
                    )
                    halo.append(both.astype(rows.dtype))
            wide = rows[xp, start:end].reshape(span * count, width)
            lhs = jnp.concatenate([wide, jnp.concatenate(halo, axis=0)], axis=1)
            moved = jnp.dot(lhs, shift[...], preferred_element_type=jnp.float32)
            moved = moved.astype(rows.dtype).reshape(span, count, 2 * width)
            kept = wide.reshape(span, count, width)
            for g in range(groups):
                at = slice(g * chan, (g + 1) * chan)
                base = g * 3 * chan
                out[xp, start:end, base : base + chan] = moved[:, at, :width]
                out[xp, start:end, base + chan : base + 2 * chan] = kept[:, at]
                out[xp, start:end, base + 2 * chan : base + 3 * chan] = moved[:, at, width:]

    def band(weights, table, group):
        outs = weights.shape[0]
        third = weights.shape[1] // 3
        step = third // 3
        table[...] = jnp.zeros_like(table)
        for kx in range(3):
            piece = weights[:, kx * third : (kx + 1) * third]
            for ox in range(depth):
                xp = ox + kx
                kind, pos = (0, near.index(xp)) if xp in near else (1, far.index(xp))
                for oy in range(group):
                    row = (ox * group + oy) * outs
                    at = (pos * (group + 2) + oy) * step
                    table[kind, row : row + outs, at : at + third] = piece

    def convolve(table, ref, group, kind, finish, lo, hi):
        outs = table.shape[1] // (depth * group)
        planes = (near, far)[kind]

        @pl.loop(lo, hi)
        def _(j):
            halves = []
            for half in range(2):
                y = (2 * j + half) * group
                halves.append(
                    jnp.concatenate(
                        [
                            ref[xp, pl.ds(y, group + 2)].reshape(
                                (group + 2) * ref.shape[2], width
                            )
                            for xp in planes
                        ],
                        axis=0,
                    )
                )
            rhs = jnp.concatenate(halves, axis=1)
            out = jnp.dot(
                table[kind, :, : rhs.shape[0]], rhs, preferred_element_type=jnp.float32
            )
            if kind == 0:
                keep[j] = out
                return
            out = out + keep[j]
            for half in range(2):
                for ox in range(depth):
                    for oy in range(group):
                        row = (ox * group + oy) * outs
                        finish(
                            ox,
                            (2 * j + half) * group + oy,
                            out[row : row + outs, half * width : (half + 1) * width],
                        )

    tiles = pack.shape[1]
    cells_all = float(depth * height * width * total)
    factor = math.sqrt(27.0 * chan)
    span = 8 * tiles
    lanes = width // chan
    trio = 3 * chan

    def correlate(ref, rows, offset, slot):
        bands = range(0, height, 4)
        lhs = jnp.concatenate(
            [
                ref[:, y : y + 6, :trio].reshape((depth + 2) * 6 * trio, width)
                for y in bands
            ],
            axis=1,
        )
        inner = slice(offset, offset + depth)
        rhs = jnp.concatenate(
            [
                rows[inner, y + offset : y + offset + 4].reshape(depth * 4 * chan, width)
                for y in bands
            ],
            axis=1,
        )
        prod[...] = lax.dot_general(
            lhs, rhs, NT, preferred_element_type=jnp.float32
        ).reshape(prod.shape)

    def fold(slot):
        group = lax.broadcasted_iota(jnp.int32, (8, width), 1) // chan
        for kx in range(3):
            for r in range(0, trio, 8):
                sums = []
                for y in range(6):
                    part = prod[kx, y, r : r + 8, :width]
                    for x in range(1, depth):
                        part = part + prod[kx + x, y, r : r + 8, x * width : (x + 1) * width]
                    sums.append(part)
                for ky in range(3):
                    at = (3 * kx + ky) * trio + r
                    keep_y = sums[ky + 3]
                    for y in (2, 1, 0):
                        keep_y = jnp.where(group == y, sums[ky + y], keep_y)
                    diag[at : at + 8] = keep_y
        low = group < 2
        even = group % 2 == 0
        for t in range(tiles):
            rows = [diag[j * span + 8 * t : j * span + 8 * t + 8] for j in range(4)]
            pairs = []
            for j in range(2):
                one, two = rows[j], rows[j + 2]
                pairs.append(
                    jnp.where(low, one, two)
                    + pltpu.roll(jnp.where(low, two, one), 2 * chan, 1)
                )
            one, two = pairs
            cross = jnp.where(even, two, one)
            pack[slot, t] = jnp.where(even, one, two) + jnp.where(
                even, pltpu.roll(cross, width - chan, 1), pltpu.roll(cross, chan, 1)
            )

    mids = min(2, sizes[0])
    first_mid = (sizes[0] - mids) // 2
    owners = mids * sizes[1] * sizes[2]
    rounds = -(-tiles // owners)
    is_mid = jnp.logical_and(me[0] >= first_mid, me[0] < first_mid + mids)
    mine = (me[1] * sizes[2] + me[2]) * mids + me[0] - first_mid

    def owner(t):
        w = t % owners
        return (first_mid + w % mids, w // mids // sizes[2], w // mids % sizes[2])

    def owns(count):
        if count == 0:
            none = jnp.logical_or(jnp.logical_not(is_mid), mine >= tiles)
            return none
        more = mine + (count - 1) * owners < tiles
        last = mine + count * owners >= tiles
        return jnp.logical_and(is_mid, jnp.logical_and(more, last))

    def scatter(slot):
        for t in range(tiles):
            spot = owner(t)
            at = (spot[0] * sizes[1] + spot[1]) * sizes[2] + spot[2]

            @pl.when(line != at)
            def _():
                pltpu.make_async_remote_copy(
                    src_ref=pack.at[slot, t],
                    dst_ref=land.at[slot, t // owners, lax.rem(line - at + total, total) - 1],
                    send_sem=asend.at[slot],
                    recv_sem=arecv.at[slot, t // owners],
                    device_id=spot,
                    device_id_type=MESH,
                ).start()

    def others():
        axes = [
            [me[i] if d == 0 else lax.rem(me[i] + d, sizes[i]) for d in range(sizes[i])]
            for i in range(3)
        ]
        return list(itertools.product(*axes))[1:]

    def gather(slot):
        for r in range(rounds):

            @pl.when(jnp.logical_and(is_mid, mine + r * owners < tiles))
            def _():
                t = mine + r * owners
                landed = land.at[slot, r]
                pltpu.make_async_copy(landed, landed, arecv.at[slot, r]).wait()
                summed = pack[slot, t] + jnp.sum(land[slot, r], axis=0)
                part[slot, r] = summed
                full[slot, t] = summed

                def tell(spot):
                    pltpu.make_async_remote_copy(
                        src_ref=part.at[slot, r],
                        dst_ref=full.at[slot, t],
                        send_sem=bsend.at[slot],
                        recv_sem=brecv.at[slot],
                        device_id=spot,
                        device_id_type=MESH,
                    ).start()

                if total <= 64:
                    for spot in others():
                        tell(spot)
                else:

                    @pl.loop(1, total)
                    def _(i):
                        tell(place(lax.rem(line + i, total)))

    def drain(slot, out, direction):
        for count in range(rounds + 1):

            @pl.when(owns(count))
            def _():
                some = full.at[slot, pl.ds(0, tiles - count)]
                pltpu.make_async_copy(some, some, brecv.at[slot]).wait()
                sent_all = pack.at[slot, pl.ds(0, tiles - count)]
                pltpu.make_async_copy(sent_all, sent_all, asend.at[slot]).wait()
                if count:
                    told = land.at[slot, pl.ds(0, count)]
                    pltpu.make_async_copy(told, told, bsend.at[slot]).wait()

        whole = full[slot].reshape(span, width)
        for j in range(lanes):
            at = slice(j * span, (j + 1) * span)
            damp = 0.1 * direction[at].astype(jnp.float32)
            out[at] = factor * (whole[:, j * chan : (j + 1) * chan] / cells_all + damp)

    def arrange():
        filt = 27 * chan
        for load in loads[1:]:
            load.wait()
        four = jnp.concatenate([wf[...], vf[...], vs[...], ws[...]], axis=1)
        rows = lax.broadcasted_iota(jnp.int32, (4 * chan, 4 * chan), 0)
        cols = lax.broadcasted_iota(jnp.int32, (4 * chan, 4 * chan), 1)
        eye = jnp.where(rows == cols, 1.0, 0.0).astype(four.dtype)
        turned = lax.dot_general(eye, four, NT, preferred_element_type=jnp.float32)
        turned = turned.astype(w1.dtype)
        w1[...] = turned[: 2 * chan]
        third = 3 * chan
        for k in range(9):
            part = slice(k * third, (k + 1) * third)
            w2[:, 2 * k * third : (2 * k + 1) * third] = turned[2 * chan : 3 * chan, part]
            w2[:, (2 * k + 1) * third : (2 * k + 2) * third] = turned[3 * chan :, part]
        for k in range(27):
            at = filt - (k + 1) * chan
            w3[:, k * chan : (k + 1) * chan] = ws[at : at + chan]

    inner = (slice(1, depth + 1), slice(1, height + 1))
    loads[0].wait()
    for x in range(depth):
        rv[x + 1, 1 : height + 1] = jnp.swapaxes(volume[:, x], 0, 1)
    cells0, cells1, cells2 = (rv, zv, ev, 0), (rp, zp, ep, 1), (rj, zj, ej, 2)
    pl.semaphore_wait(barrier, greeted)
    send_faces(cells0, 0)
    send_rest(cells0, False)
    edges(rv, ev)
    send_rest(cells0, True)
    for rows, zbuf in ((rv, zv), (rp, zp), (rj, zj)):
        clear(rows, zbuf)
    shifter()
    arrange()
    band(w1, t1, 2)
    band(w2, t2, 4)
    band(w3, t3, 4)

    def first(x, y, out):
        hidden, slope = gelu_pair(out[:chan])
        slope_ref[x, y] = slope
        rp[x + 1, y + 1, :chan] = hidden.astype(jnp.bfloat16)
        rp[x + 1, y + 1, chan:] = (slope * out[chan:]).astype(jnp.bfloat16)

    def launch():
        sent(cells0)
        send_faces(cells1, 0)

    def launch_rest():
        edges(rp, ep)
        send_rest(cells1, False)
        send_rest(cells1, True)
        send_faces(cells1, 2)

    stage(
        cells0,
        sv,
        t1,
        2,
        first,
        (
            ((0,), 1, launch),
            ((), early // 4, lambda: send_faces(cells1, 1)),
            ((), height // 4, launch_rest),
        ),
    )

    def second(x, y, out):
        rj[x + 1, y + 1] = out.astype(jnp.bfloat16)

    def pass_on():
        sent(cells1)
        send_faces(cells2, 0)

    def pass_rest():
        send_faces(cells2, 1)
        edges(rj, ej)
        send_rest(cells2, False)
        send_rest(cells2, True)

    stage(
        cells1,
        sp,
        t2,
        4,
        second,
        (((0, 1), bands, pass_on), ((2,), height // 8, pass_rest)),
    )
    for x in range(depth):
        jv_out[:, x] = jnp.swapaxes(rj[x + 1, 1 : height + 1], 0, 1)
    correlate(sp, rj, 1, 0)
    fold(0)
    scatter(0)

    def third(x, y, out):
        back_ref[x, y] = (slope_ref[x, y] * out).astype(jnp.bfloat16)

    stage(cells2, sj, t3, 4, third, (((0, 1), height // 8, lambda: None),))
    correlate(sv, back_ref, 0, 1)
    fold(1)
    scatter(1)
    gather(0)
    gather(1)
    drain(0, gv2, vs)
    drain(1, gv1, vf)
    sent(cells2)


def place_out(*refs):
    count = len(refs) // 2
    sems = refs[-1]
    copies = [
        pltpu.make_async_copy(refs[i], refs[count + i], sems.at[i]) for i in range(count)
    ]
    for copy in copies:
        copy.start()
    for copy in copies:
        copy.wait()


def body(volume, w_first, w_second, v_first, v_second):
    chan, depth, height, width = volume.shape
    sizes = tuple(lax.axis_size(a) for a in AXES)
    total = sizes[0] * sizes[1] * sizes[2]
    filt = 27 * chan
    tiles = filt * chan // (8 * width)
    rounds = -(-tiles // (min(2, sizes[0]) * sizes[1] * sizes[2]))
    _, ways = codes(sizes)
    folds = 2 if 4 * depth * height <= width else 1
    bf, f32 = jnp.bfloat16, jnp.float32
    pads = (depth + 2, height + 2)
    vmem = pl.BlockSpec(memory_space=pltpu.VMEM)
    jv, corr1, corr2 = pl.pallas_call(
        functools.partial(kernel, sizes),
        out_shape=(
            jax.ShapeDtypeStruct(volume.shape, bf),
            jax.ShapeDtypeStruct((filt, chan), f32),
            jax.ShapeDtypeStruct((filt, chan), f32),
        ),
        in_specs=[pl.BlockSpec(memory_space=pltpu.HBM)] * 5,
        out_specs=(vmem,) * 3,
        scratch_shapes=[
            pltpu.VMEM(pads + (chan, width), bf),
            pltpu.VMEM(pads + (2 * chan, width), bf),
            pltpu.VMEM(pads + (chan, width), bf),
            pltpu.VMEM((2, 3, 3, chan // folds, width), bf),
            pltpu.VMEM((2, 3, 3, 2 * chan // folds, width), bf),
            pltpu.VMEM((2, 3, 3, chan // folds, width), bf),
            pltpu.VMEM((chan // folds, width), bf),
            pltpu.VMEM((2 * chan // folds, width), bf),
            pltpu.VMEM((chan // folds, width), bf),
            pltpu.VMEM(pads + (3 * chan, width), bf),
            pltpu.VMEM(pads + (6 * chan, width), bf),
            pltpu.VMEM(pads + (3 * chan, width), bf),
            pltpu.VMEM((depth, height, chan, width), f32),
            pltpu.VMEM((depth, height, chan, width), bf),
            pltpu.VMEM((2, depth * 2 * 2 * chan, depth * 4 * 3 * chan), bf),
            pltpu.VMEM((2, depth * 4 * chan, depth * 6 * 6 * chan), bf),
            pltpu.VMEM((2, depth * 4 * chan, depth * 6 * 3 * chan), bf),
            pltpu.VMEM((2 * width, 2 * width), bf),
            pltpu.VMEM((height // 4, depth * 4 * chan, 2 * width), f32),
            pltpu.VMEM((depth + 2, 6, 3 * chan, depth * 4 * chan), f32),
            pltpu.VMEM((filt, width), f32),
            pltpu.VMEM((2, tiles, 8, width), f32),
            pltpu.VMEM((2, rounds, total - 1, 8, width), f32),
            pltpu.VMEM((2, rounds, 8, width), f32),
            pltpu.VMEM((2, tiles, 8, width), f32),
            pltpu.SemaphoreType.DMA((ways + 4,)),
            pltpu.SemaphoreType.DMA((2, ways + 4)),
            pltpu.SemaphoreType.DMA((2,)),
            pltpu.SemaphoreType.DMA((2, rounds)),
            pltpu.SemaphoreType.DMA((2,)),
            pltpu.SemaphoreType.DMA((2,)),
            pltpu.VMEM(volume.shape, bf),
            pltpu.VMEM((filt, chan), bf),
            pltpu.VMEM((filt, chan), bf),
            pltpu.VMEM((filt, chan), bf),
            pltpu.VMEM((filt, chan), bf),
            pltpu.VMEM((2 * chan, filt), bf),
            pltpu.VMEM((chan, 2 * filt), bf),
            pltpu.VMEM((chan, filt), bf),
            pltpu.SemaphoreType.DMA((5,)),
        ],
        compiler_params=pltpu.CompilerParams(
            collective_id=0, has_side_effects=True, vmem_limit_bytes=48 * 1024 * 1024
        ),
    )(*(pltpu.with_memory_space_constraint(w, pltpu.HBM) for w in (volume, *(w.reshape(filt, chan) for w in (w_first, w_second, v_first, v_second)))))
    jv, corr1, corr2 = pl.pallas_call(
        place_out,
        out_shape=(
            jax.ShapeDtypeStruct(volume.shape, bf),
            jax.ShapeDtypeStruct((filt, chan), f32),
            jax.ShapeDtypeStruct((filt, chan), f32),
        ),
        in_specs=[vmem] * 3,
        out_specs=(pl.BlockSpec(memory_space=pltpu.HBM),) * 3,
        scratch_shapes=[pltpu.SemaphoreType.DMA((3,))],
        compiler_params=pltpu.CompilerParams(vmem_limit_bytes=4 * 1024 * 1024),
    )(jv, corr1, corr2)
    return jv, corr1.reshape(v_first.shape), corr2.reshape(v_second.shape)


def solution(mesh):
    in_specs = (P(None, "gx", "gy", "gz"), P(), P(), P(), P())
    out_specs = (P(None, "gx", "gy", "gz"), P(), P())
    return jax.shard_map(body, mesh=mesh, in_specs=in_specs, out_specs=out_specs, check_vma=False)
```

```python
import functools
import itertools
import math

import jax
import jax.numpy as jnp
from jax import lax
from jax.experimental import pallas as pl
from jax.experimental.pallas import tpu as pltpu
from jax.sharding import PartitionSpec as P

MESH = pl.DeviceIdType.MESH
AXES = ("gx", "gy", "gz")
STEPS = [d for d in itertools.product((-1, 0, 1), repeat=3) if d != (0, 0, 0)]
STEPS.sort(key=lambda d: (d[2] != 0, d[0] == 0, abs(d[0]) + abs(d[1])))
NT = (((1,), (1,)), ((), ()))


def gelu_pair(pre):
    inner = 0.7978845608 * (pre + 0.044715 * pre * pre * pre)
    hyper = jnp.tanh(inner)
    hidden = 0.5 * pre * (1.0 + hyper)
    slope = 0.5 * (1.0 + hyper) + 0.5 * pre * (1.0 - hyper * hyper) * 0.7978845608 * (
        1.0 + 0.134145 * pre * pre
    )
    return hidden, slope


def codes(sizes):
    spans = [3 if size > 2 else 2 for size in sizes]

    def code(step):
        total = 0
        for delta, span in zip(step, spans):
            total = total * span + (delta + 1 if span == 3 else abs(delta))
        return total

    return code, math.prod(spans)


def kernel(
    sizes,
    volume_hbm,
    wf_hbm,
    ws_hbm,
    vf_hbm,
    vs_hbm,
    jv_out,
    gv1,
    gv2,
    *scratch,
):
    (rv, rp, rj, zv, zp, zj, ev, ep, ej, sv, sp, sj, slope_ref, back_ref,
     t1, t2, t3, shift, keep, prod, diag, pack, land, part, full,
     hsend, hrecv, asend, arecv, bsend, brecv,
     volume, wf, ws, vf, vs, w1, w2, w3, build1, build2, isem) = scratch
    chan, depth, height, width = volume.shape
    code, ways = codes(sizes)
    early = height - 4
    bands = (early - 1) // 8
    cuts = ((5, 9, height), (4, 8 * bands + 1, height), (8 * bands, height))
    loads = [
        pltpu.make_async_copy(src, dst, isem.at[i])
        for i, (src, dst) in enumerate(
            (
                (volume_hbm, volume),
                (wf_hbm, wf),
                (ws_hbm, ws),
                (vf_hbm, vf),
                (vs_hbm, vs),
            )
        )
    ]
    for load in loads:
        load.start()
    me = tuple(lax.axis_index(a) for a in AXES)
    total = sizes[0] * sizes[1] * sizes[2]
    line = (me[0] * sizes[1] + me[1]) * sizes[2] + me[2]

    def place(index):
        return (
            index // (sizes[1] * sizes[2]),
            index // sizes[2] % sizes[1],
            index % sizes[2],
        )

    def there(step):
        ok = None
        for pos, size, delta in zip(me, sizes, step):
            if delta == -1:
                term = pos > 0
            elif delta == 1:
                term = pos < size - 1
            else:
                continue
            ok = term if ok is None else jnp.logical_and(ok, term)
        return ok

    barrier = pltpu.get_barrier_semaphore()
    near_only = max(sizes) <= 4

    if near_only:
        greeted = 0
        for step in STEPS:
            ok = there(step)
            greeted = greeted + jnp.where(ok, 1, 0)

            @pl.when(ok)
            def _():
                pl.semaphore_signal(
                    barrier,
                    inc=1,
                    device_id=tuple(p + d for p, d in zip(me, step)),
                    device_id_type=MESH,
                )
    else:
        greeted = total - 1

        @pl.loop(1, total)
        def _(i):
            pl.semaphore_signal(
                barrier, inc=1, device_id=place(lax.rem(line + i, total)), device_id_type=MESH
            )

    def source(delta, extent):
        return {-1: pl.ds(1, 1), 1: pl.ds(extent, 1), 0: pl.ds(1, extent)}[delta]

    def target(delta, extent):
        return {-1: pl.ds(extent + 1, 1), 1: pl.ds(0, 1), 0: pl.ds(1, extent)}[delta]

    def pieces(step, slot):
        if step[1] or step[2]:
            return [None]
        ends = cuts[slot]
        return [(p, lo, hi) for p, (lo, hi) in enumerate(zip((0,) + ends, ends))]

    def landing(step, rows, zbuf, piece=None):
        if step[2] == 0:
            if piece is None:
                return rows.at[target(step[0], depth), target(step[1], height)]
            _, lo, hi = piece
            return rows.at[target(step[0], depth), pl.ds(1 + lo, hi - lo)]
        return zbuf.at[0 if step[2] == 1 else 1, 1 - step[0], 1 - step[1]]

    def message(step, rows, zbuf, edge, slot, piece=None):
        lane = code(step)
        if step[2] != 0:
            src = edge
        elif piece is None:
            src = rows.at[source(step[0], depth), source(step[1], height)]
        else:
            part, lo, hi = piece
            src = rows.at[source(step[0], depth), pl.ds(1 + lo, hi - lo)]
            if part:
                lane = ways + 2 * (part - 1) + (step[0] > 0)
        return pltpu.make_async_remote_copy(
            src_ref=src,
            dst_ref=landing(step, rows, zbuf, piece),
            send_sem=hsend.at[lane],
            recv_sem=hrecv.at[slot % 2, lane],
            device_id=tuple(p + d for p, d in zip(me, step)),
            device_id_type=MESH,
        )

    def send_faces(halo, part):
        for step in STEPS:
            found = pieces(step, halo[3])
            if found == [None] or part >= len(found):
                continue

            @pl.when(there(step))
            def _():
                message(step, *halo, found[part]).start()

    def send_rest(halo, cross):
        for step in STEPS:
            if (step[2] != 0) == cross and pieces(step, halo[3]) == [None]:

                @pl.when(there(step))
                def _():
                    message(step, *halo).start()

    def clear(rows, zbuf):
        for step in STEPS:
            back = tuple(-d for d in step)

            @pl.when(jnp.logical_not(there(back)))
            def _():
                ref = landing(step, rows, zbuf)
                ref[...] = jnp.zeros(ref.shape, ref.dtype)

    def receive(halo, kind, parts):
        for step in STEPS:
            if (step[0] != 0) != (kind == 1):
                continue
            found = pieces(step, halo[3])
            if found == [None]:
                found = found if 0 in parts else []
            else:
                found = [piece for piece in found if piece[0] in parts]
            if not found:
                continue
            back = tuple(-d for d in step)

            @pl.when(there(back))
            def _():
                for piece in found:
                    message(step, *halo, piece).wait_recv()

    def stage(halo, out, table, group, finish, plan):
        rows, zbuf, _, slot = halo
        receive(halo, 0, (0,))
        spread(rows, zbuf, out, near, 0, height + 2)
        convolve(table, out, group, 0, finish, 0, height // (2 * group))
        done = 0
        for parts, upto, hook in plan:
            if parts:
                receive(halo, 1, parts)
                last = cuts[slot][parts[-1]]
                end = height + 2 if last == height else last + 1
                start = 0 if parts[0] == 0 else cuts[slot][parts[0] - 1] + 1
                spread(rows, zbuf, out, far, start, end)
            convolve(table, out, group, 1, finish, done, upto)
            done = upto
            hook()

    def sent(halo):
        for step in STEPS:

            @pl.when(there(step))
            def _():
                for piece in pieces(step, halo[3]):
                    message(step, *halo, piece).wait_send()

    cells = depth * height
    folds = 2 if 4 * cells <= width else 1
    pitch = width // folds

    def collect(build, bits, at):
        count = bits[0].shape[0]
        lane = lax.broadcasted_iota(jnp.int32, (count, width), 1)
        built = build[...]
        for f, bit in enumerate(bits):
            spot = f * pitch + at
            built = jnp.where(lane == spot, pltpu.roll(bit, spot, 1), built)
            spot = spot + cells
            built = jnp.where(lane == spot, pltpu.roll(bit, spot + 1, 1), built)
        build[...] = built

    def edges(rows, edge):
        count = edge.shape[0]
        lane = lax.broadcasted_iota(jnp.int32, (count, width), 1)
        for f in range(folds):
            part = slice(f * count, (f + 1) * count)
            built = jnp.zeros((count, width), jnp.float32)
            for x in range(depth):
                for y in range(height):
                    row = rows[x + 1, y + 1, part].astype(jnp.float32)
                    at = f * pitch + x * height + y
                    built = jnp.where(lane == at, pltpu.roll(row, at, 1), built)
                    at = at + cells
                    shift_by = (at + 1) % width
                    built = jnp.where(lane == at, pltpu.roll(row, shift_by, 1), built)
            if f == 0:
                whole = built
            else:
                whole = jnp.where(lane < f * pitch, whole, built)
        edge[...] = whole.astype(edge.dtype)

    def shifter():
        src = lax.broadcasted_iota(jnp.int32, (2 * width, 2 * width), 0)
        dst = lax.broadcasted_iota(jnp.int32, (2 * width, 2 * width), 1)
        spot = src % pitch
        right = jnp.logical_and(src >= width, spot < cells)
        left = jnp.logical_and(
            src >= width, jnp.logical_and(spot >= cells, spot < 2 * cells)
        )
        low = jnp.logical_or(
            jnp.logical_and(src == dst - 1, src < width - 1),
            jnp.logical_and(dst == 0, left),
        )
        high = jnp.logical_or(
            jnp.logical_and(src == dst - width + 1, src < width),
            jnp.logical_and(dst == 2 * width - 1, right),
        )
        pick = jnp.logical_or(
            jnp.logical_and(dst < width, low), jnp.logical_and(dst >= width, high)
        )
        shift[...] = jnp.where(pick, 1.0, 0.0).astype(shift.dtype)

    near = tuple(range(1, depth + 1))
    far = (0, depth + 1)

    def spread(rows, zbuf, out, planes, start, end):
        count = rows.shape[2]
        part = zbuf.shape[3]
        groups = count // chan
        span = end - start
        lane = lax.broadcasted_iota(jnp.int32, (part, width), 1)

        for xp in planes:
            dx = 0 if xp == 0 else (2 if xp == depth + 1 else 1)
            halo = []
            for yp in range(start, end):
                dy = 0 if yp == 0 else (2 if yp == height + 1 else 1)
                left = zbuf[0, dx, dy].astype(jnp.float32)
                right = zbuf[1, dx, dy].astype(jnp.float32)
                for f in range(folds):
                    at = f * pitch + (xp - 1) % depth * height + (yp - 1) % height
                    both = jnp.where(
                        lane == at, right, jnp.where(lane == cells + at, left, 0.0)
                    )
                    halo.append(both.astype(rows.dtype))
            wide = rows[xp, start:end].reshape(span * count, width)
            lhs = jnp.concatenate([wide, jnp.concatenate(halo, axis=0)], axis=1)
            moved = jnp.dot(lhs, shift[...], preferred_element_type=jnp.float32)
            moved = moved.astype(rows.dtype).reshape(span, count, 2 * width)
            kept = wide.reshape(span, count, width)
            for g in range(groups):
                at = slice(g * chan, (g + 1) * chan)
                base = g * 3 * chan
                out[xp, start:end, base : base + chan] = moved[:, at, :width]
                out[xp, start:end, base + chan : base + 2 * chan] = kept[:, at]
                out[xp, start:end, base + 2 * chan : base + 3 * chan] = moved[:, at, width:]

    def band(weights, table, group):
        outs = weights.shape[0]
        third = weights.shape[1] // 3
        step = third // 3
        table[...] = jnp.zeros_like(table)
        for kx in range(3):
            piece = weights[:, kx * third : (kx + 1) * third]
            for ox in range(depth):
                xp = ox + kx
                kind, pos = (0, near.index(xp)) if xp in near else (1, far.index(xp))
                for oy in range(group):
                    row = (ox * group + oy) * outs
                    at = (pos * (group + 2) + oy) * step
                    table[kind, row : row + outs, at : at + third] = piece

    def convolve(table, ref, group, kind, finish, lo, hi):
        outs = table.shape[1] // (depth * group)
        planes = (near, far)[kind]

        @pl.loop(lo, hi, unroll=hi - lo if kind == 0 and table is not t3 else 1)
        def _(j):
            halves = []
            for half in range(2):
                y = (2 * j + half) * group
                halves.append(
                    jnp.concatenate(
                        [
                            ref[xp, pl.ds(y, group + 2)].reshape(
                                (group + 2) * ref.shape[2], width
                            )
                            for xp in planes
                        ],
                        axis=0,
                    )
                )
            rhs = jnp.concatenate(halves, axis=1)
            out = jnp.dot(
                table[kind, :, : rhs.shape[0]], rhs, preferred_element_type=jnp.float32
            )
            if kind == 0:
                keep[j] = out
                return
            out = out + keep[j]
            for half in range(2):
                for ox in range(depth):
                    for oy in range(group):
                        row = (ox * group + oy) * outs
                        finish(
                            ox,
                            (2 * j + half) * group + oy,
                            out[row : row + outs, half * width : (half + 1) * width],
                        )

    tiles = pack.shape[1]
    cells_all = float(depth * height * width * total)
    factor = math.sqrt(27.0 * chan)
    span = 8 * tiles
    lanes = width // chan
    trio = 3 * chan

    def correlate(ref, rows, offset, slot):
        bands = range(0, height, 4)
        lhs = jnp.concatenate(
            [
                ref[:, y : y + 6, :trio].reshape((depth + 2) * 6 * trio, width)
                for y in bands
            ],
            axis=1,
        )
        inner = slice(offset, offset + depth)
        rhs = jnp.concatenate(
            [
                rows[inner, y + offset : y + offset + 4].reshape(depth * 4 * chan, width)
                for y in bands
            ],
            axis=1,
        )
        prod[...] = lax.dot_general(
            lhs, rhs, NT, preferred_element_type=jnp.float32
        ).reshape(prod.shape)

    def fold(slot):
        group = lax.broadcasted_iota(jnp.int32, (8, width), 1) // chan
        for kx in range(3):
            for r in range(0, trio, 8):
                sums = []
                for y in range(6):
                    part = prod[kx, y, r : r + 8, :width]
                    for x in range(1, depth):
                        part = part + prod[kx + x, y, r : r + 8, x * width : (x + 1) * width]
                    sums.append(part)
                for ky in range(3):
                    at = (3 * kx + ky) * trio + r
                    keep_y = sums[ky + 3]
                    for y in (2, 1, 0):
                        keep_y = jnp.where(group == y, sums[ky + y], keep_y)
                    diag[at : at + 8] = keep_y
        low = group < 2
        even = group % 2 == 0
        for t in range(tiles):
            rows = [diag[j * span + 8 * t : j * span + 8 * t + 8] for j in range(4)]
            pairs = []
            for j in range(2):
                one, two = rows[j], rows[j + 2]
                pairs.append(
                    jnp.where(low, one, two)
                    + pltpu.roll(jnp.where(low, two, one), 2 * chan, 1)
                )
            one, two = pairs
            cross = jnp.where(even, two, one)
            pack[slot, t] = jnp.where(even, one, two) + jnp.where(
                even, pltpu.roll(cross, width - chan, 1), pltpu.roll(cross, chan, 1)
            )

    mids = min(2, sizes[0])
    first_mid = (sizes[0] - mids) // 2
    owners = mids * sizes[1] * sizes[2]
    rounds = -(-tiles // owners)
    is_mid = jnp.logical_and(me[0] >= first_mid, me[0] < first_mid + mids)
    mine = (me[1] * sizes[2] + me[2]) * mids + me[0] - first_mid

    def owner(t):
        w = t % owners
        return (first_mid + w % mids, w // mids // sizes[2], w // mids % sizes[2])

    def owns(count):
        if count == 0:
            none = jnp.logical_or(jnp.logical_not(is_mid), mine >= tiles)
            return none
        more = mine + (count - 1) * owners < tiles
        last = mine + count * owners >= tiles
        return jnp.logical_and(is_mid, jnp.logical_and(more, last))

    def scatter(slot):
        for t in range(tiles):
            spot = owner(t)
            at = (spot[0] * sizes[1] + spot[1]) * sizes[2] + spot[2]

            @pl.when(line != at)
            def _():
                pltpu.make_async_remote_copy(
                    src_ref=pack.at[slot, t],
                    dst_ref=land.at[slot, t // owners, lax.rem(line - at + total, total) - 1],
                    send_sem=asend.at[slot],
                    recv_sem=arecv.at[slot, t // owners],
                    device_id=spot,
                    device_id_type=MESH,
                ).start()

    def others():
        axes = [
            [me[i] if d == 0 else lax.rem(me[i] + d, sizes[i]) for d in range(sizes[i])]
            for i in range(3)
        ]
        return list(itertools.product(*axes))[1:]

    def gather(slot):
        for r in range(rounds):

            @pl.when(jnp.logical_and(is_mid, mine + r * owners < tiles))
            def _():
                t = mine + r * owners
                landed = land.at[slot, r]
                pltpu.make_async_copy(landed, landed, arecv.at[slot, r]).wait()
                summed = pack[slot, t] + jnp.sum(land[slot, r], axis=0)
                part[slot, r] = summed
                full[slot, t] = summed

                def tell(spot):
                    pltpu.make_async_remote_copy(
                        src_ref=part.at[slot, r],
                        dst_ref=full.at[slot, t],
                        send_sem=bsend.at[slot],
                        recv_sem=brecv.at[slot],
                        device_id=spot,
                        device_id_type=MESH,
                    ).start()

                if total <= 64:
                    for spot in others():
                        tell(spot)
                else:

                    @pl.loop(1, total)
                    def _(i):
                        tell(place(lax.rem(line + i, total)))

    def drain(slot, out, direction):
        for count in range(rounds + 1):

            @pl.when(owns(count))
            def _():
                some = full.at[slot, pl.ds(0, tiles - count)]
                pltpu.make_async_copy(some, some, brecv.at[slot]).wait()
                sent_all = pack.at[slot, pl.ds(0, tiles - count)]
                pltpu.make_async_copy(sent_all, sent_all, asend.at[slot]).wait()
                if count:
                    told = land.at[slot, pl.ds(0, count)]
                    pltpu.make_async_copy(told, told, bsend.at[slot]).wait()

        whole = full[slot].reshape(span, width)
        for j in range(lanes):
            at = slice(j * span, (j + 1) * span)
            damp = 0.1 * direction[at].astype(jnp.float32)
            out[at] = factor * (whole[:, j * chan : (j + 1) * chan] / cells_all + damp)

    def arrange():
        filt = 27 * chan
        for load in loads[1:]:
            load.wait()
        four = jnp.concatenate([wf[...], vf[...], vs[...], ws[...]], axis=1)
        rows = lax.broadcasted_iota(jnp.int32, (4 * chan, 4 * chan), 0)
        cols = lax.broadcasted_iota(jnp.int32, (4 * chan, 4 * chan), 1)
        eye = jnp.where(rows == cols, 1.0, 0.0).astype(four.dtype)
        turned = lax.dot_general(eye, four, NT, preferred_element_type=jnp.float32)
        turned = turned.astype(w1.dtype)
        w1[...] = turned[: 2 * chan]
        third = 3 * chan
        for k in range(9):
            part = slice(k * third, (k + 1) * third)
            w2[:, 2 * k * third : (2 * k + 1) * third] = turned[2 * chan : 3 * chan, part]
            w2[:, (2 * k + 1) * third : (2 * k + 2) * third] = turned[3 * chan :, part]
        for k in range(27):
            at = filt - (k + 1) * chan
            w3[:, k * chan : (k + 1) * chan] = ws[at : at + chan]

    inner = (slice(1, depth + 1), slice(1, height + 1))
    loads[0].wait()
    for x in range(depth):
        rv[x + 1, 1 : height + 1] = jnp.swapaxes(volume[:, x], 0, 1)
    cells0, cells1, cells2 = (rv, zv, ev, 0), (rp, zp, ep, 1), (rj, zj, ej, 2)
    pl.semaphore_wait(barrier, greeted)
    send_faces(cells0, 0)
    send_rest(cells0, False)
    edges(rv, ev)
    send_rest(cells0, True)
    send_faces(cells0, 1)
    send_faces(cells0, 2)
    build1[...] = jnp.zeros_like(build1)
    build2[...] = jnp.zeros_like(build2)
    for rows, zbuf in ((rv, zv), (rp, zp), (rj, zj)):
        clear(rows, zbuf)
    shifter()
    arrange()
    band(w1, t1, 2)
    band(w2, t2, 4)
    band(w3, t3, 4)

    def first(x, y, out):
        hidden, slope = gelu_pair(out[:chan])
        slope_ref[x, y] = slope
        tangent = slope * out[chan:]
        rp[x + 1, y + 1, :chan] = hidden.astype(jnp.bfloat16)
        rp[x + 1, y + 1, chan:] = tangent.astype(jnp.bfloat16)
        if folds == 2:
            collect(build1, (hidden, tangent), x * height + y)

    def launch():
        sent(cells0)
        send_faces(cells1, 0)

    def launch_rest():
        if folds == 2:
            ep[...] = build1[...].astype(ep.dtype)
        else:
            edges(rp, ep)
        send_rest(cells1, False)
        send_rest(cells1, True)
        send_faces(cells1, 2)

    stage(
        cells0,
        sv,
        t1,
        2,
        first,
        (
            ((0,), 1, launch),
            ((1,), 2, lambda: None),
            ((2,), early // 4, lambda: send_faces(cells1, 1)),
            ((), height // 4, launch_rest),
        ),
    )

    def second(x, y, out):
        rj[x + 1, y + 1] = out.astype(jnp.bfloat16)
        if folds == 2:
            half = chan // 2
            collect(build2, (out[:half], out[half:]), x * height + y)

    def pass_on():
        sent(cells1)
        send_faces(cells2, 0)

    def pass_rest():
        if folds == 2:
            ej[...] = build2[...].astype(ej.dtype)
        else:
            edges(rj, ej)
        send_rest(cells2, False)
        send_rest(cells2, True)
        send_faces(cells2, 1)

    stage(
        cells1,
        sp,
        t2,
        4,
        second,
        (((0, 1), bands, pass_on), ((2,), height // 8, pass_rest)),
    )
    for x in range(depth):
        jv_out[:, x] = jnp.swapaxes(rj[x + 1, 1 : height + 1], 0, 1)
    correlate(sp, rj, 1, 0)
    fold(0)
    scatter(0)

    def third(x, y, out):
        back_ref[x, y] = (slope_ref[x, y] * out).astype(jnp.bfloat16)

    stage(cells2, sj, t3, 4, third, (((0, 1), height // 8, lambda: None),))
    correlate(sv, back_ref, 0, 1)
    fold(1)
    scatter(1)
    gather(0)
    gather(1)
    drain(0, gv2, vs)
    drain(1, gv1, vf)
    sent(cells2)


def place_out(*refs):
    count = len(refs) // 2
    sems = refs[-1]
    copies = [
        pltpu.make_async_copy(refs[i], refs[count + i], sems.at[i]) for i in range(count)
    ]
    for copy in copies:
        copy.start()
    for copy in copies:
        copy.wait()


def body(volume, w_first, w_second, v_first, v_second):
    chan, depth, height, width = volume.shape
    sizes = tuple(lax.axis_size(a) for a in AXES)
    total = sizes[0] * sizes[1] * sizes[2]
    filt = 27 * chan
    tiles = filt * chan // (8 * width)
    rounds = -(-tiles // (min(2, sizes[0]) * sizes[1] * sizes[2]))
    _, ways = codes(sizes)
    folds = 2 if 4 * depth * height <= width else 1
    bf, f32 = jnp.bfloat16, jnp.float32
    pads = (depth + 2, height + 2)
    vmem = pl.BlockSpec(memory_space=pltpu.VMEM)
    jv, corr1, corr2 = pl.pallas_call(
        functools.partial(kernel, sizes),
        out_shape=(
            jax.ShapeDtypeStruct(volume.shape, bf),
            jax.ShapeDtypeStruct((filt, chan), f32),
            jax.ShapeDtypeStruct((filt, chan), f32),
        ),
        in_specs=[pl.BlockSpec(memory_space=pltpu.HBM)] * 5,
        out_specs=(vmem,) * 3,
        scratch_shapes=[
            pltpu.VMEM(pads + (chan, width), bf),
            pltpu.VMEM(pads + (2 * chan, width), bf),
            pltpu.VMEM(pads + (chan, width), bf),
            pltpu.VMEM((2, 3, 3, chan // folds, width), bf),
            pltpu.VMEM((2, 3, 3, 2 * chan // folds, width), bf),
            pltpu.VMEM((2, 3, 3, chan // folds, width), bf),
            pltpu.VMEM((chan // folds, width), bf),
            pltpu.VMEM((2 * chan // folds, width), bf),
            pltpu.VMEM((chan // folds, width), bf),
            pltpu.VMEM(pads + (3 * chan, width), bf),
            pltpu.VMEM(pads + (6 * chan, width), bf),
            pltpu.VMEM(pads + (3 * chan, width), bf),
            pltpu.VMEM((depth, height, chan, width), f32),
            pltpu.VMEM((depth, height, chan, width), bf),
            pltpu.VMEM((2, depth * 2 * 2 * chan, depth * 4 * 3 * chan), bf),
            pltpu.VMEM((2, depth * 4 * chan, depth * 6 * 6 * chan), bf),
            pltpu.VMEM((2, depth * 4 * chan, depth * 6 * 3 * chan), bf),
            pltpu.VMEM((2 * width, 2 * width), bf),
            pltpu.VMEM((height // 4, depth * 4 * chan, 2 * width), f32),
            pltpu.VMEM((depth + 2, 6, 3 * chan, depth * 4 * chan), f32),
            pltpu.VMEM((filt, width), f32),
            pltpu.VMEM((2, tiles, 8, width), f32),
            pltpu.VMEM((2, rounds, total - 1, 8, width), f32),
            pltpu.VMEM((2, rounds, 8, width), f32),
            pltpu.VMEM((2, tiles, 8, width), f32),
            pltpu.SemaphoreType.DMA((ways + 4,)),
            pltpu.SemaphoreType.DMA((2, ways + 4)),
            pltpu.SemaphoreType.DMA((2,)),
            pltpu.SemaphoreType.DMA((2, rounds)),
            pltpu.SemaphoreType.DMA((2,)),
            pltpu.SemaphoreType.DMA((2,)),
            pltpu.VMEM(volume.shape, bf),
            pltpu.VMEM((filt, chan), bf),
            pltpu.VMEM((filt, chan), bf),
            pltpu.VMEM((filt, chan), bf),
            pltpu.VMEM((filt, chan), bf),
            pltpu.VMEM((2 * chan, filt), bf),
            pltpu.VMEM((chan, 2 * filt), bf),
            pltpu.VMEM((chan, filt), bf),
            pltpu.VMEM((2 * chan // folds, width), f32),
            pltpu.VMEM((chan // folds, width), f32),
            pltpu.SemaphoreType.DMA((5,)),
        ],
        compiler_params=pltpu.CompilerParams(
            collective_id=0, has_side_effects=True, vmem_limit_bytes=48 * 1024 * 1024
        ),
    )(*(pltpu.with_memory_space_constraint(w, pltpu.HBM) for w in (volume, *(w.reshape(filt, chan) for w in (w_first, w_second, v_first, v_second)))))
    jv, corr1, corr2 = pl.pallas_call(
        place_out,
        out_shape=(
            jax.ShapeDtypeStruct(volume.shape, bf),
            jax.ShapeDtypeStruct((filt, chan), f32),
            jax.ShapeDtypeStruct((filt, chan), f32),
        ),
        in_specs=[vmem] * 3,
        out_specs=(pl.BlockSpec(memory_space=pltpu.HBM),) * 3,
        scratch_shapes=[pltpu.SemaphoreType.DMA((3,))],
        compiler_params=pltpu.CompilerParams(vmem_limit_bytes=4 * 1024 * 1024),
    )(jv, corr1, corr2)
    return jv, corr1.reshape(v_first.shape), corr2.reshape(v_second.shape)


def solution(mesh):
    in_specs = (P(None, "gx", "gy", "gz"), P(), P(), P(), P())
    out_specs = (P(None, "gx", "gy", "gz"), P(), P())
    return jax.shard_map(body, mesh=mesh, in_specs=in_specs, out_specs=out_specs, check_vma=False)
```

```python
import functools
import itertools
import math

import jax
import jax.numpy as jnp
from jax import lax
from jax.experimental import pallas as pl
from jax.experimental.pallas import tpu as pltpu
from jax.sharding import PartitionSpec as P

MESH = pl.DeviceIdType.MESH
AXES = ("gx", "gy", "gz")
STEPS = [d for d in itertools.product((-1, 0, 1), repeat=3) if d != (0, 0, 0)]
STEPS.sort(key=lambda d: (d[2] != 0, d[0] == 0, abs(d[0]) + abs(d[1])))
NT = (((1,), (1,)), ((), ()))


def gelu_pair(pre):
    inner = 0.7978845608 * (pre + 0.044715 * pre * pre * pre)
    hyper = jnp.tanh(inner)
    hidden = 0.5 * pre * (1.0 + hyper)
    slope = 0.5 * (1.0 + hyper) + 0.5 * pre * (1.0 - hyper * hyper) * 0.7978845608 * (
        1.0 + 0.134145 * pre * pre
    )
    return hidden, slope


def codes(sizes):
    spans = [3 if size > 2 else 2 for size in sizes]

    def code(step):
        total = 0
        for delta, span in zip(step, spans):
            total = total * span + (delta + 1 if span == 3 else abs(delta))
        return total

    return code, math.prod(spans)


def owners(sizes):
    mids = min(2, sizes[0])
    start = (sizes[0] - mids) // 2
    spots = [
        (x, y, z)
        for z in range(sizes[2])
        for y in range(sizes[1])
        for x in range(start, start + mids)
    ]
    base = [spot for spot in spots if spot[2] % 2 == 1][:8]
    rest = [spot for spot in spots if spot not in base]
    return base, [rest[0], rest[-1], rest[len(rest) // 2 - 1]]


def kernel(
    sizes,
    volume_hbm,
    wf_hbm,
    ws_hbm,
    vf_hbm,
    vs_hbm,
    jv_out,
    gv1,
    gv2,
    *scratch,
):
    (rv, rp, rj, zv, zp, zj, ev, ep, ej, sv, sp, sj, slope_ref, back_ref,
     t1, t2, t3, shift, keep, prod, diag, pack, land, part, full, told,
     hsend, hrecv, asend, arecv, bsend, brecv,
     volume, wf, ws, vf, vs, w1, w2, w3, build1, build2, isem) = scratch
    chan, depth, height, width = volume.shape
    code, ways = codes(sizes)
    early = height - 4
    bands = (early - 1) // 8
    cuts = ((5, 9, height), (4, 8 * bands + 1, height), (8 * bands, height))
    loads = [
        pltpu.make_async_copy(src, dst, isem.at[i])
        for i, (src, dst) in enumerate(
            (
                (volume_hbm, volume),
                (wf_hbm, wf),
                (ws_hbm, ws),
                (vf_hbm, vf),
                (vs_hbm, vs),
            )
        )
    ]
    for load in loads:
        load.start()
    me = tuple(lax.axis_index(a) for a in AXES)
    total = sizes[0] * sizes[1] * sizes[2]
    line = (me[0] * sizes[1] + me[1]) * sizes[2] + me[2]

    def place(index):
        return (
            index // (sizes[1] * sizes[2]),
            index // sizes[2] % sizes[1],
            index % sizes[2],
        )

    def there(step):
        ok = None
        for pos, size, delta in zip(me, sizes, step):
            if delta == -1:
                term = pos > 0
            elif delta == 1:
                term = pos < size - 1
            else:
                continue
            ok = term if ok is None else jnp.logical_and(ok, term)
        return ok

    barrier = pltpu.get_barrier_semaphore()
    near_only = max(sizes) <= 4

    if near_only:
        greeted = 0
        for step in STEPS:
            ok = there(step)
            greeted = greeted + jnp.where(ok, 1, 0)

            @pl.when(ok)
            def _():
                pl.semaphore_signal(
                    barrier,
                    inc=1,
                    device_id=tuple(p + d for p, d in zip(me, step)),
                    device_id_type=MESH,
                )
    else:
        greeted = total - 1

        @pl.loop(1, total)
        def _(i):
            pl.semaphore_signal(
                barrier, inc=1, device_id=place(lax.rem(line + i, total)), device_id_type=MESH
            )

    def source(delta, extent):
        return {-1: pl.ds(1, 1), 1: pl.ds(extent, 1), 0: pl.ds(1, extent)}[delta]

    def target(delta, extent):
        return {-1: pl.ds(extent + 1, 1), 1: pl.ds(0, 1), 0: pl.ds(1, extent)}[delta]

    def pieces(step, slot):
        if step[1] or step[2]:
            return [None]
        ends = cuts[slot]
        return [(p, lo, hi) for p, (lo, hi) in enumerate(zip((0,) + ends, ends))]

    def landing(step, rows, zbuf, piece=None):
        if step[2] == 0:
            if piece is None:
                return rows.at[target(step[0], depth), target(step[1], height)]
            _, lo, hi = piece
            return rows.at[target(step[0], depth), pl.ds(1 + lo, hi - lo)]
        return zbuf.at[0 if step[2] == 1 else 1, 1 - step[0], 1 - step[1]]

    def message(step, rows, zbuf, edge, slot, piece=None):
        lane = code(step)
        if step[2] != 0:
            src = edge
        elif piece is None:
            src = rows.at[source(step[0], depth), source(step[1], height)]
        else:
            part, lo, hi = piece
            src = rows.at[source(step[0], depth), pl.ds(1 + lo, hi - lo)]
            if part:
                lane = ways + 2 * (part - 1) + (step[0] > 0)
        return pltpu.make_async_remote_copy(
            src_ref=src,
            dst_ref=landing(step, rows, zbuf, piece),
            send_sem=hsend.at[lane],
            recv_sem=hrecv.at[slot % 2, lane],
            device_id=tuple(p + d for p, d in zip(me, step)),
            device_id_type=MESH,
        )

    def send_faces(halo, part):
        for step in STEPS:
            found = pieces(step, halo[3])
            if found == [None] or part >= len(found):
                continue

            @pl.when(there(step))
            def _():
                message(step, *halo, found[part]).start()

    def send_rest(halo, cross):
        for step in STEPS:
            if (step[2] != 0) == cross and pieces(step, halo[3]) == [None]:

                @pl.when(there(step))
                def _():
                    message(step, *halo).start()

    def clear(rows, zbuf):
        for step in STEPS:
            back = tuple(-d for d in step)

            @pl.when(jnp.logical_not(there(back)))
            def _():
                ref = landing(step, rows, zbuf)
                ref[...] = jnp.zeros(ref.shape, ref.dtype)

    def receive(halo, kind, parts):
        for step in STEPS:
            if (step[0] != 0) != (kind == 1):
                continue
            found = pieces(step, halo[3])
            if found == [None]:
                found = found if 0 in parts else []
            else:
                found = [piece for piece in found if piece[0] in parts]
            if not found:
                continue
            back = tuple(-d for d in step)

            @pl.when(there(back))
            def _():
                for piece in found:
                    message(step, *halo, piece).wait_recv()

    def stage(halo, out, table, group, finish, plan):
        rows, zbuf, _, slot = halo
        receive(halo, 0, (0,))
        spread(rows, zbuf, out, near, 0, height + 2)
        convolve(table, out, group, 0, finish, 0, height // (2 * group))
        done = 0
        for parts, upto, hook in plan:
            if parts:
                receive(halo, 1, parts)
                last = cuts[slot][parts[-1]]
                end = height + 2 if last == height else last + 1
                start = 0 if parts[0] == 0 else cuts[slot][parts[0] - 1] + 1
                spread(rows, zbuf, out, far, start, end)
            convolve(table, out, group, 1, finish, done, upto)
            done = upto
            hook()

    def sent(halo):
        for step in STEPS:

            @pl.when(there(step))
            def _():
                for piece in pieces(step, halo[3]):
                    message(step, *halo, piece).wait_send()

    cells = depth * height
    folds = 2 if 4 * cells <= width else 1
    pitch = width // folds

    def collect(build, bits, at):
        count = bits[0].shape[0]
        lane = lax.broadcasted_iota(jnp.int32, (count, width), 1)
        built = build[...]
        for f, bit in enumerate(bits):
            spot = f * pitch + at
            built = jnp.where(lane == spot, pltpu.roll(bit, spot, 1), built)
            spot = spot + cells
            built = jnp.where(lane == spot, pltpu.roll(bit, spot + 1, 1), built)
        build[...] = built

    def edges(rows, edge):
        count = edge.shape[0]
        lane = lax.broadcasted_iota(jnp.int32, (count, width), 1)
        for f in range(folds):
            part = slice(f * count, (f + 1) * count)
            built = jnp.zeros((count, width), jnp.float32)
            for x in range(depth):
                for y in range(height):
                    row = rows[x + 1, y + 1, part].astype(jnp.float32)
                    at = f * pitch + x * height + y
                    built = jnp.where(lane == at, pltpu.roll(row, at, 1), built)
                    at = at + cells
                    shift_by = (at + 1) % width
                    built = jnp.where(lane == at, pltpu.roll(row, shift_by, 1), built)
            if f == 0:
                whole = built
            else:
                whole = jnp.where(lane < f * pitch, whole, built)
        edge[...] = whole.astype(edge.dtype)

    def shifter():
        src = lax.broadcasted_iota(jnp.int32, (2 * width, 2 * width), 0)
        dst = lax.broadcasted_iota(jnp.int32, (2 * width, 2 * width), 1)
        spot = src % pitch
        right = jnp.logical_and(src >= width, spot < cells)
        left = jnp.logical_and(
            src >= width, jnp.logical_and(spot >= cells, spot < 2 * cells)
        )
        low = jnp.logical_or(
            jnp.logical_and(src == dst - 1, src < width - 1),
            jnp.logical_and(dst == 0, left),
        )
        high = jnp.logical_or(
            jnp.logical_and(src == dst - width + 1, src < width),
            jnp.logical_and(dst == 2 * width - 1, right),
        )
        pick = jnp.logical_or(
            jnp.logical_and(dst < width, low), jnp.logical_and(dst >= width, high)
        )
        shift[...] = jnp.where(pick, 1.0, 0.0).astype(shift.dtype)

    near = tuple(range(1, depth + 1))
    far = (0, depth + 1)

    def spread(rows, zbuf, out, planes, start, end):
        count = rows.shape[2]
        part = zbuf.shape[3]
        groups = count // chan
        span = end - start
        lane = lax.broadcasted_iota(jnp.int32, (part, width), 1)

        for xp in planes:
            dx = 0 if xp == 0 else (2 if xp == depth + 1 else 1)
            halo = []
            for yp in range(start, end):
                dy = 0 if yp == 0 else (2 if yp == height + 1 else 1)
                left = zbuf[0, dx, dy].astype(jnp.float32)
                right = zbuf[1, dx, dy].astype(jnp.float32)
                for f in range(folds):
                    at = f * pitch + (xp - 1) % depth * height + (yp - 1) % height
                    both = jnp.where(
                        lane == at, right, jnp.where(lane == cells + at, left, 0.0)
                    )
                    halo.append(both.astype(rows.dtype))
            wide = rows[xp, start:end].reshape(span * count, width)
            lhs = jnp.concatenate([wide, jnp.concatenate(halo, axis=0)], axis=1)
            moved = jnp.dot(lhs, shift[...], preferred_element_type=jnp.float32)
            moved = moved.astype(rows.dtype).reshape(span, count, 2 * width)
            kept = wide.reshape(span, count, width)
            for g in range(groups):
                at = slice(g * chan, (g + 1) * chan)
                base = g * 3 * chan
                out[xp, start:end, base : base + chan] = moved[:, at, :width]
                out[xp, start:end, base + chan : base + 2 * chan] = kept[:, at]
                out[xp, start:end, base + 2 * chan : base + 3 * chan] = moved[:, at, width:]

    def band(weights, table, group):
        outs = weights.shape[0]
        third = weights.shape[1] // 3
        step = third // 3
        table[...] = jnp.zeros_like(table)
        for kx in range(3):
            piece = weights[:, kx * third : (kx + 1) * third]
            for ox in range(depth):
                xp = ox + kx
                kind, pos = (0, near.index(xp)) if xp in near else (1, far.index(xp))
                for oy in range(group):
                    row = (ox * group + oy) * outs
                    at = (pos * (group + 2) + oy) * step
                    table[kind, row : row + outs, at : at + third] = piece

    def convolve(table, ref, group, kind, finish, lo, hi):
        outs = table.shape[1] // (depth * group)
        planes = (near, far)[kind]

        @pl.loop(lo, hi, unroll=hi - lo if kind == 0 and table is not t3 else 1)
        def _(j):
            halves = []
            for half in range(2):
                y = (2 * j + half) * group
                halves.append(
                    jnp.concatenate(
                        [
                            ref[xp, pl.ds(y, group + 2)].reshape(
                                (group + 2) * ref.shape[2], width
                            )
                            for xp in planes
                        ],
                        axis=0,
                    )
                )
            rhs = jnp.concatenate(halves, axis=1)
            out = jnp.dot(
                table[kind, :, : rhs.shape[0]], rhs, preferred_element_type=jnp.float32
            )
            if kind == 0:
                keep[j] = out
                return
            out = out + keep[j]
            for half in range(2):
                for ox in range(depth):
                    for oy in range(group):
                        row = (ox * group + oy) * outs
                        finish(
                            ox,
                            (2 * j + half) * group + oy,
                            out[row : row + outs, half * width : (half + 1) * width],
                        )

    tiles = pack.shape[1]
    cells_all = float(depth * height * width * total)
    factor = math.sqrt(27.0 * chan)
    lanes = width // chan
    trio = 3 * chan

    def correlate(ref, rows, offset, slot):
        starts_y = range(0, height, 4)
        inner = slice(offset, offset + depth)
        rhs = jnp.concatenate(
            [
                rows[inner, y + offset : y + offset + 4].reshape(depth * 4 * chan, width)
                for y in starts_y
            ],
            axis=1,
        )

        def multiply(planes):
            lhs = jnp.concatenate(
                [ref[planes, y : y + 6, :trio].reshape(-1, width) for y in starts_y], axis=1
            )
            prod[planes] = lax.dot_general(
                lhs, rhs, NT, preferred_element_type=jnp.float32
            ).reshape((-1,) + prod.shape[1:])

        multiply(slice(0, depth + 2))
        for kx in range(3):
            fold(kx, slot)
            scatter(kx, slot)

    slab = 9 * chan
    step_rows = slab // lanes
    batch = step_rows // 8

    def fold(kx, slot):
        group = lax.broadcasted_iota(jnp.int32, (8, width), 1) // chan
        for r in range(0, trio, 8):
            sums = []
            for y in range(6):
                part_sum = prod[kx, y, r : r + 8, :width]
                for x in range(1, depth):
                    part_sum = part_sum + prod[
                        kx + x, y, r : r + 8, x * width : (x + 1) * width
                    ]
                sums.append(part_sum)
            for ky in range(3):
                at = ky * trio + r
                keep_y = sums[ky + 3]
                for y in (2, 1, 0):
                    keep_y = jnp.where(group == y, sums[ky + y], keep_y)
                diag[at : at + 8] = keep_y
        low = group < 2
        even = group % 2 == 0
        for i in range(batch):
            rows = [diag[j * step_rows + 8 * i : j * step_rows + 8 * i + 8] for j in range(4)]
            pairs = []
            for j in range(2):
                one, two = rows[j], rows[j + 2]
                pairs.append(
                    jnp.where(low, one, two)
                    + pltpu.roll(jnp.where(low, two, one), 2 * chan, 1)
                )
            one, two = pairs
            cross = jnp.where(even, two, one)
            pack[slot, kx * batch + i] = jnp.where(even, one, two) + jnp.where(
                even, pltpu.roll(cross, width - chan, 1), pltpu.roll(cross, chan, 1)
            )

    base, extra = owners(sizes)

    def at_spot(spot):
        return jnp.logical_and(
            me[0] == spot[0], jnp.logical_and(me[1] == spot[1], me[2] == spot[2])
        )

    def which(spots):
        found, index = False, 0
        for i, spot in enumerate(spots):
            here = at_spot(spot)
            found = jnp.logical_or(found, here)
            index = index + jnp.where(here, i, 0)
        return found, index

    is_base, base_at = which(base)
    is_extra, extra_at = which(extra)

    def give(slot, t, chunk, spot):
        at = (spot[0] * sizes[1] + spot[1]) * sizes[2] + spot[2]

        @pl.when(line != at)
        def _():
            pltpu.make_async_remote_copy(
                src_ref=pack.at[slot, t],
                dst_ref=land.at[slot, chunk, lax.rem(line - at + total, total) - 1],
                send_sem=asend.at[slot],
                recv_sem=arecv.at[slot, chunk],
                device_id=spot,
                device_id_type=MESH,
            ).start()

    def scatter(kx, slot):
        for w, spot in enumerate(base):
            give(slot, kx * batch + w, kx, spot)
        give(slot, kx * batch + len(base), 0, extra[kx])

    def others():
        axes = [
            [me[i] if d == 0 else lax.rem(me[i] + d, sizes[i]) for d in range(sizes[i])]
            for i in range(3)
        ]
        return list(itertools.product(*axes))[1:]

    def finish_tile(slot, t, chunk, row, column):
        landed = land.at[slot, chunk]
        pltpu.make_async_copy(landed, landed, arecv.at[slot, chunk]).wait()
        rounded = (pack[slot, t] + jnp.sum(land[slot, chunk], axis=0)).astype(part.dtype)
        part[slot, chunk] = rounded
        full[slot, row, column] = rounded

        def tell(spot):
            pltpu.make_async_remote_copy(
                src_ref=part.at[slot, chunk],
                dst_ref=full.at[slot, row, column],
                send_sem=bsend.at[slot],
                recv_sem=brecv.at[slot],
                device_id=spot,
                device_id_type=MESH,
            ).start()

        if total <= 64:
            for spot in others():
                tell(spot)
        else:

            @pl.loop(1, total)
            def _(i):
                tell(place(lax.rem(line + i, total)))

    def gather(slot):
        @pl.when(is_base)
        def _():
            for kx in range(3):
                finish_tile(slot, kx * batch + base_at, kx, base_at, kx)

        @pl.when(is_extra)
        def _():
            finish_tile(slot, extra_at * batch + len(base), 0, len(base), extra_at)

    def drain(slot, out, direction):
        none = jnp.logical_not(jnp.logical_or(is_base, is_extra))
        for owned, here in ((3, is_base), (1, is_extra), (0, none)):

            @pl.when(here)
            def _():
                some = told.at[pl.ds(0, tiles - owned)]
                pltpu.make_async_copy(some, some, brecv.at[slot]).wait()
                sent_all = pack.at[slot, pl.ds(0, tiles - owned)]
                pltpu.make_async_copy(sent_all, sent_all, asend.at[slot]).wait()
                if owned:
                    gone = told.at[pl.ds(0, owned * (total - 1))]
                    pltpu.make_async_copy(gone, gone, bsend.at[slot]).wait()

        for kx in range(3):
            whole = full[slot, :, kx].astype(jnp.float32).reshape(step_rows, width)
            for j in range(lanes):
                at = slice(kx * slab + j * step_rows, kx * slab + (j + 1) * step_rows)
                damp = 0.1 * direction[at].astype(jnp.float32)
                mean = whole[:, j * chan : (j + 1) * chan] * (1.0 / cells_all)
                out[at] = factor * (mean + damp)

    def arrange():
        filt = 27 * chan
        for load in loads[1:]:
            load.wait()
        four = jnp.concatenate([wf[...], vf[...], vs[...], ws[...]], axis=1)
        rows = lax.broadcasted_iota(jnp.int32, (4 * chan, 4 * chan), 0)
        cols = lax.broadcasted_iota(jnp.int32, (4 * chan, 4 * chan), 1)
        eye = jnp.where(rows == cols, 1.0, 0.0).astype(four.dtype)
        turned = lax.dot_general(eye, four, NT, preferred_element_type=jnp.float32)
        turned = turned.astype(w1.dtype)
        w1[...] = turned[: 2 * chan]
        third = 3 * chan
        for k in range(9):
            part = slice(k * third, (k + 1) * third)
            w2[:, 2 * k * third : (2 * k + 1) * third] = turned[2 * chan : 3 * chan, part]
            w2[:, (2 * k + 1) * third : (2 * k + 2) * third] = turned[3 * chan :, part]
        for k in range(27):
            at = filt - (k + 1) * chan
            w3[:, k * chan : (k + 1) * chan] = ws[at : at + chan]

    inner = (slice(1, depth + 1), slice(1, height + 1))
    loads[0].wait()
    for x in range(depth):
        rv[x + 1, 1 : height + 1] = jnp.swapaxes(volume[:, x], 0, 1)
    cells0, cells1, cells2 = (rv, zv, ev, 0), (rp, zp, ep, 1), (rj, zj, ej, 2)
    pl.semaphore_wait(barrier, greeted)
    send_faces(cells0, 0)
    send_rest(cells0, False)
    edges(rv, ev)
    send_rest(cells0, True)
    send_faces(cells0, 1)
    send_faces(cells0, 2)
    build1[...] = jnp.zeros_like(build1)
    build2[...] = jnp.zeros_like(build2)
    for rows, zbuf in ((rv, zv), (rp, zp), (rj, zj)):
        clear(rows, zbuf)
    shifter()
    arrange()
    band(w1, t1, 2)
    band(w2, t2, 4)
    band(w3, t3, 4)

    def first(x, y, out):
        hidden, slope = gelu_pair(out[:chan])
        slope_ref[x, y] = slope
        tangent = slope * out[chan:]
        rp[x + 1, y + 1, :chan] = hidden.astype(jnp.bfloat16)
        rp[x + 1, y + 1, chan:] = tangent.astype(jnp.bfloat16)
        if folds == 2:
            collect(build1, (hidden, tangent), x * height + y)

    def launch():
        sent(cells0)
        send_faces(cells1, 0)

    def launch_rest():
        if folds == 2:
            ep[...] = build1[...].astype(ep.dtype)
        else:
            edges(rp, ep)
        send_rest(cells1, False)
        send_rest(cells1, True)
        send_faces(cells1, 2)

    stage(
        cells0,
        sv,
        t1,
        2,
        first,
        (
            ((0,), 1, launch),
            ((1,), 2, lambda: None),
            ((2,), early // 4, lambda: send_faces(cells1, 1)),
            ((), height // 4, launch_rest),
        ),
    )

    def second(x, y, out):
        rj[x + 1, y + 1] = out.astype(jnp.bfloat16)
        if folds == 2:
            half = chan // 2
            collect(build2, (out[:half], out[half:]), x * height + y)

    def pass_on():
        sent(cells1)
        send_faces(cells2, 0)

    def pass_rest():
        if folds == 2:
            ej[...] = build2[...].astype(ej.dtype)
        else:
            edges(rj, ej)
        send_rest(cells2, False)
        send_rest(cells2, True)
        send_faces(cells2, 1)

    stage(
        cells1,
        sp,
        t2,
        4,
        second,
        (((0, 1), bands, pass_on), ((2,), height // 8, pass_rest)),
    )
    for x in range(depth):
        jv_out[:, x] = jnp.swapaxes(rj[x + 1, 1 : height + 1], 0, 1)
    correlate(sp, rj, 1, 0)

    def third(x, y, out):
        back_ref[x, y] = (slope_ref[x, y] * out).astype(jnp.bfloat16)

    stage(cells2, sj, t3, 4, third, (((0, 1), height // 8, lambda: None),))
    correlate(sv, back_ref, 0, 1)
    gather(0)
    gather(1)
    drain(0, gv2, vs)
    drain(1, gv1, vf)
    sent(cells2)


def place_out(*refs):
    count = len(refs) // 2
    sems = refs[-1]
    copies = [
        pltpu.make_async_copy(refs[i], refs[count + i], sems.at[i]) for i in range(count)
    ]
    for copy in copies:
        copy.start()
    for copy in copies:
        copy.wait()


def body(volume, w_first, w_second, v_first, v_second):
    chan, depth, height, width = volume.shape
    sizes = tuple(lax.axis_size(a) for a in AXES)
    total = sizes[0] * sizes[1] * sizes[2]
    filt = 27 * chan
    tiles = filt * chan // (8 * width)
    _, ways = codes(sizes)
    folds = 2 if 4 * depth * height <= width else 1
    bf, f32 = jnp.bfloat16, jnp.float32
    pads = (depth + 2, height + 2)
    vmem = pl.BlockSpec(memory_space=pltpu.VMEM)
    jv, corr1, corr2 = pl.pallas_call(
        functools.partial(kernel, sizes),
        out_shape=(
            jax.ShapeDtypeStruct(volume.shape, bf),
            jax.ShapeDtypeStruct((filt, chan), f32),
            jax.ShapeDtypeStruct((filt, chan), f32),
        ),
        in_specs=[pl.BlockSpec(memory_space=pltpu.HBM)] * 5,
        out_specs=(vmem,) * 3,
        scratch_shapes=[
            pltpu.VMEM(pads + (chan, width), bf),
            pltpu.VMEM(pads + (2 * chan, width), bf),
            pltpu.VMEM(pads + (chan, width), bf),
            pltpu.VMEM((2, 3, 3, chan // folds, width), bf),
            pltpu.VMEM((2, 3, 3, 2 * chan // folds, width), bf),
            pltpu.VMEM((2, 3, 3, chan // folds, width), bf),
            pltpu.VMEM((chan // folds, width), bf),
            pltpu.VMEM((2 * chan // folds, width), bf),
            pltpu.VMEM((chan // folds, width), bf),
            pltpu.VMEM(pads + (3 * chan, width), bf),
            pltpu.VMEM(pads + (6 * chan, width), bf),
            pltpu.VMEM(pads + (3 * chan, width), bf),
            pltpu.VMEM((depth, height, chan, width), f32),
            pltpu.VMEM((depth, height, chan, width), bf),
            pltpu.VMEM((2, depth * 2 * 2 * chan, depth * 4 * 3 * chan), bf),
            pltpu.VMEM((2, depth * 4 * chan, depth * 6 * 6 * chan), bf),
            pltpu.VMEM((2, depth * 4 * chan, depth * 6 * 3 * chan), bf),
            pltpu.VMEM((2 * width, 2 * width), bf),
            pltpu.VMEM((height // 4, depth * 4 * chan, 2 * width), f32),
            pltpu.VMEM((depth + 2, 6, 3 * chan, depth * 4 * chan), f32),
            pltpu.VMEM((9 * chan, width), f32),
            pltpu.VMEM((2, tiles, 8, width), f32),
            pltpu.VMEM((2, 3, total - 1, 8, width), f32),
            pltpu.VMEM((2, 3, 8, width), bf),
            pltpu.VMEM((2, 9, 3, 8, width), bf),
            pltpu.VMEM(((total - 1) * 3, 8, width), bf),
            pltpu.SemaphoreType.DMA((ways + 4,)),
            pltpu.SemaphoreType.DMA((2, ways + 4)),
            pltpu.SemaphoreType.DMA((2,)),
            pltpu.SemaphoreType.DMA((2, 3)),
            pltpu.SemaphoreType.DMA((2,)),
            pltpu.SemaphoreType.DMA((2,)),
            pltpu.VMEM(volume.shape, bf),
            pltpu.VMEM((filt, chan), bf),
            pltpu.VMEM((filt, chan), bf),
            pltpu.VMEM((filt, chan), bf),
            pltpu.VMEM((filt, chan), bf),
            pltpu.VMEM((2 * chan, filt), bf),
            pltpu.VMEM((chan, 2 * filt), bf),
            pltpu.VMEM((chan, filt), bf),
            pltpu.VMEM((2 * chan // folds, width), f32),
            pltpu.VMEM((chan // folds, width), f32),
            pltpu.SemaphoreType.DMA((5,)),
        ],
        compiler_params=pltpu.CompilerParams(
            collective_id=0, has_side_effects=True, vmem_limit_bytes=48 * 1024 * 1024
        ),
    )(*(pltpu.with_memory_space_constraint(w, pltpu.HBM) for w in (volume, *(w.reshape(filt, chan) for w in (w_first, w_second, v_first, v_second)))))
    jv, corr1, corr2 = pl.pallas_call(
        place_out,
        out_shape=(
            jax.ShapeDtypeStruct(volume.shape, bf),
            jax.ShapeDtypeStruct((filt, chan), f32),
            jax.ShapeDtypeStruct((filt, chan), f32),
        ),
        in_specs=[vmem] * 3,
        out_specs=(pl.BlockSpec(memory_space=pltpu.HBM),) * 3,
        scratch_shapes=[pltpu.SemaphoreType.DMA((3,))],
        compiler_params=pltpu.CompilerParams(vmem_limit_bytes=4 * 1024 * 1024),
    )(jv, corr1, corr2)
    return jv, corr1.reshape(v_first.shape), corr2.reshape(v_second.shape)


def solution(mesh):
    in_specs = (P(None, "gx", "gy", "gz"), P(), P(), P(), P())
    out_specs = (P(None, "gx", "gy", "gz"), P(), P())
    return jax.shard_map(body, mesh=mesh, in_specs=in_specs, out_specs=out_specs, check_vma=False)
```

```python
import functools
import itertools
import math

import jax
import jax.numpy as jnp
from jax import lax
from jax.experimental import pallas as pl
from jax.experimental.pallas import tpu as pltpu
from jax.sharding import PartitionSpec as P

MESH = pl.DeviceIdType.MESH
AXES = ("gx", "gy", "gz")
STEPS = [d for d in itertools.product((-1, 0, 1), repeat=3) if d != (0, 0, 0)]
STEPS.sort(key=lambda d: (d[2] != 0, d[0] == 0, abs(d[0]) + abs(d[1])))
NT = (((1,), (1,)), ((), ()))


def gelu_pair(pre):
    inner = 0.7978845608 * (pre + 0.044715 * pre * pre * pre)
    hyper = jnp.tanh(inner)
    hidden = 0.5 * pre * (1.0 + hyper)
    slope = 0.5 * (1.0 + hyper) + 0.5 * pre * (1.0 - hyper * hyper) * 0.7978845608 * (
        1.0 + 0.134145 * pre * pre
    )
    return hidden, slope


def codes(sizes):
    spans = [3 if size > 2 else 2 for size in sizes]

    def code(step):
        total = 0
        for delta, span in zip(step, spans):
            total = total * span + (delta + 1 if span == 3 else abs(delta))
        return total

    return code, math.prod(spans)


def owners(sizes):
    mids = min(2, sizes[0])
    start = (sizes[0] - mids) // 2
    spots = [
        (x, y, z)
        for z in range(sizes[2])
        for y in range(sizes[1])
        for x in range(start, start + mids)
    ]
    base = [spot for spot in spots if spot[2] % 2 == 1][:8]
    rest = [spot for spot in spots if spot not in base]
    return base, [rest[0], rest[-1], rest[len(rest) // 2 - 1]]


def kernel(
    sizes,
    volume_hbm,
    wf_hbm,
    ws_hbm,
    vf_hbm,
    vs_hbm,
    jv_out,
    gv1,
    gv2,
    *scratch,
):
    (rv, rp, rj, zv, zp, zj, ev, ep, ej, sv, sp, sj, slope_ref, back_ref,
     t1, t2, t3, shift, keep, prod, diag, pack, land, part, full, told,
     hsend, hrecv, asend, arecv, bsend, brecv,
     volume, wf, ws, vf, vs, w1, w2, w3, build1, build2, isem) = scratch
    chan, depth, height, width = volume.shape
    code, ways = codes(sizes)
    early = height - 4
    bands = (early - 1) // 8
    cuts = ((5, 9, height), (4, 8 * bands + 1, height), (8 * bands, height))
    loads = [
        pltpu.make_async_copy(src, dst, isem.at[i])
        for i, (src, dst) in enumerate(
            (
                (volume_hbm, volume),
                (wf_hbm, wf),
                (ws_hbm, ws),
                (vf_hbm, vf),
                (vs_hbm, vs),
            )
        )
    ]
    for load in loads:
        load.start()
    me = tuple(lax.axis_index(a) for a in AXES)
    total = sizes[0] * sizes[1] * sizes[2]
    line = (me[0] * sizes[1] + me[1]) * sizes[2] + me[2]

    def place(index):
        return (
            index // (sizes[1] * sizes[2]),
            index // sizes[2] % sizes[1],
            index % sizes[2],
        )

    def there(step):
        ok = None
        for pos, size, delta in zip(me, sizes, step):
            if delta == -1:
                term = pos > 0
            elif delta == 1:
                term = pos < size - 1
            else:
                continue
            ok = term if ok is None else jnp.logical_and(ok, term)
        return ok

    barrier = pltpu.get_barrier_semaphore()
    near_only = max(sizes) <= 4

    if near_only:
        greeted = 0
        for step in STEPS:
            ok = there(step)
            greeted = greeted + jnp.where(ok, 1, 0)

            @pl.when(ok)
            def _():
                pl.semaphore_signal(
                    barrier,
                    inc=1,
                    device_id=tuple(p + d for p, d in zip(me, step)),
                    device_id_type=MESH,
                )
    else:
        greeted = total - 1

        @pl.loop(1, total)
        def _(i):
            pl.semaphore_signal(
                barrier, inc=1, device_id=place(lax.rem(line + i, total)), device_id_type=MESH
            )

    def source(delta, extent):
        return {-1: pl.ds(1, 1), 1: pl.ds(extent, 1), 0: pl.ds(1, extent)}[delta]

    def target(delta, extent):
        return {-1: pl.ds(extent + 1, 1), 1: pl.ds(0, 1), 0: pl.ds(1, extent)}[delta]

    def pieces(step, slot):
        if step[1] or step[2]:
            return [None]
        ends = cuts[slot]
        return [(p, lo, hi) for p, (lo, hi) in enumerate(zip((0,) + ends, ends))]

    def landing(step, rows, zbuf, piece=None):
        if step[2] == 0:
            if piece is None:
                return rows.at[target(step[0], depth), target(step[1], height)]
            _, lo, hi = piece
            return rows.at[target(step[0], depth), pl.ds(1 + lo, hi - lo)]
        return zbuf.at[0 if step[2] == 1 else 1, 1 - step[0], 1 - step[1]]

    def message(step, rows, zbuf, edge, slot, piece=None):
        lane = code(step)
        if step[2] != 0:
            src = edge
        elif piece is None:
            src = rows.at[source(step[0], depth), source(step[1], height)]
        else:
            part, lo, hi = piece
            src = rows.at[source(step[0], depth), pl.ds(1 + lo, hi - lo)]
            if part:
                lane = ways + 2 * (part - 1) + (step[0] > 0)
        return pltpu.make_async_remote_copy(
            src_ref=src,
            dst_ref=landing(step, rows, zbuf, piece),
            send_sem=hsend.at[lane],
            recv_sem=hrecv.at[slot % 2, lane],
            device_id=tuple(p + d for p, d in zip(me, step)),
            device_id_type=MESH,
        )

    def send_faces(halo, part):
        for step in STEPS:
            found = pieces(step, halo[3])
            if found == [None] or part >= len(found):
                continue

            @pl.when(there(step))
            def _():
                message(step, *halo, found[part]).start()

    def send_rest(halo, cross):
        for step in STEPS:
            if (step[2] != 0) == cross and pieces(step, halo[3]) == [None]:

                @pl.when(there(step))
                def _():
                    message(step, *halo).start()

    def clear(rows, zbuf):
        for step in STEPS:
            back = tuple(-d for d in step)

            @pl.when(jnp.logical_not(there(back)))
            def _():
                ref = landing(step, rows, zbuf)
                ref[...] = jnp.zeros(ref.shape, ref.dtype)

    def receive(halo, kind, parts):
        for step in STEPS:
            if (step[0] != 0) != (kind == 1):
                continue
            found = pieces(step, halo[3])
            if found == [None]:
                found = found if 0 in parts else []
            else:
                found = [piece for piece in found if piece[0] in parts]
            if not found:
                continue
            back = tuple(-d for d in step)

            @pl.when(there(back))
            def _():
                for piece in found:
                    message(step, *halo, piece).wait_recv()

    def stage(halo, out, table, group, finish, plan):
        rows, zbuf, _, slot = halo
        receive(halo, 0, (0,))
        spread(rows, zbuf, out, near, 0, height + 2)
        convolve(table, out, group, 0, finish, 0, height // (2 * group))
        done = 0
        for parts, upto, hook in plan:
            if parts:
                receive(halo, 1, parts)
                last = cuts[slot][parts[-1]]
                end = height + 2 if last == height else last + 1
                start = 0 if parts[0] == 0 else cuts[slot][parts[0] - 1] + 1
                spread(rows, zbuf, out, far, start, end)
            convolve(table, out, group, 1, finish, done, upto)
            done = upto
            hook()

    def sent(halo):
        for step in STEPS:

            @pl.when(there(step))
            def _():
                for piece in pieces(step, halo[3]):
                    message(step, *halo, piece).wait_send()

    cells = depth * height
    folds = 2 if 4 * cells <= width else 1
    pitch = width // folds

    def collect(build, bits, at):
        count = bits[0].shape[0]
        pair = lax.broadcasted_iota(jnp.int32, (count, width), 1) // 2
        built = build[...]
        for f, bit in enumerate(bits):
            spot = f * (pitch // 2) + at
            built = jnp.where(pair == spot, pltpu.roll(bit, 2 * spot + 1, 1), built)
        build[...] = built

    def edges(rows, edge):
        count = edge.shape[0]
        lane = lax.broadcasted_iota(jnp.int32, (count, width), 1)
        pair = lane // 2
        whole = jnp.zeros((count, width), jnp.float32)
        for f in range(folds):
            part_rows = slice(f * count, (f + 1) * count)
            built = jnp.zeros((count, width), jnp.float32)
            for x in range(depth):
                for y in range(height):
                    row = rows[x + 1, y + 1, part_rows].astype(jnp.float32)
                    spot = f * (pitch // 2) + x * height + y
                    shift_by = (2 * spot + 1) % width
                    built = jnp.where(pair == spot, pltpu.roll(row, shift_by, 1), built)
            whole = jnp.where(lane < f * pitch, whole, built)
        edge[...] = whole.astype(edge.dtype)

    def shifter():
        src = lax.broadcasted_iota(jnp.int32, (2 * width, 2 * width), 0)
        dst = lax.broadcasted_iota(jnp.int32, (2 * width, 2 * width), 1)
        spot = src % pitch
        used = jnp.logical_and(src >= width, spot < 2 * cells)
        right = jnp.logical_and(used, spot % 2 == 1)
        left = jnp.logical_and(used, spot % 2 == 0)
        low = jnp.logical_or(
            jnp.logical_and(src == dst - 1, src < width - 1),
            jnp.logical_and(dst == 0, left),
        )
        high = jnp.logical_or(
            jnp.logical_and(src == dst - width + 1, src < width),
            jnp.logical_and(dst == 2 * width - 1, right),
        )
        pick = jnp.logical_or(
            jnp.logical_and(dst < width, low), jnp.logical_and(dst >= width, high)
        )
        shift[...] = jnp.where(pick, 1.0, 0.0).astype(shift.dtype)

    near = tuple(range(1, depth + 1))
    far = (0, depth + 1)

    def spread(rows, zbuf, out, planes, start, end):
        count = rows.shape[2]
        part = zbuf.shape[3]
        groups = count // chan
        span = end - start
        lane = lax.broadcasted_iota(jnp.int32, (part, width), 1)

        for xp in planes:
            dx = 0 if xp == 0 else (2 if xp == depth + 1 else 1)
            halo = []
            for yp in range(start, end):
                dy = 0 if yp == 0 else (2 if yp == height + 1 else 1)
                left = zbuf[0, dx, dy].astype(jnp.float32)
                right = zbuf[1, dx, dy].astype(jnp.float32)
                for f in range(folds):
                    at = f * pitch + 2 * ((xp - 1) % depth * height + (yp - 1) % height)
                    both = jnp.where(
                        lane == at + 1, right, jnp.where(lane == at, left, 0.0)
                    )
                    halo.append(both.astype(rows.dtype))
            wide = rows[xp, start:end].reshape(span * count, width)
            lhs = jnp.concatenate([wide, jnp.concatenate(halo, axis=0)], axis=1)
            moved = jnp.dot(lhs, shift[...], preferred_element_type=jnp.float32)
            moved = moved.astype(rows.dtype).reshape(span, count, 2 * width)
            kept = wide.reshape(span, count, width)
            for g in range(groups):
                at = slice(g * chan, (g + 1) * chan)
                base = g * 3 * chan
                out[xp, start:end, base : base + chan] = moved[:, at, :width]
                out[xp, start:end, base + chan : base + 2 * chan] = kept[:, at]
                out[xp, start:end, base + 2 * chan : base + 3 * chan] = moved[:, at, width:]

    def band(weights, table, group):
        outs = weights.shape[0]
        third = weights.shape[1] // 3
        step = third // 3
        table[...] = jnp.zeros_like(table)
        for kx in range(3):
            piece = weights[:, kx * third : (kx + 1) * third]
            for ox in range(depth):
                xp = ox + kx
                kind, pos = (0, near.index(xp)) if xp in near else (1, far.index(xp))
                for oy in range(group):
                    row = (ox * group + oy) * outs
                    at = (pos * (group + 2) + oy) * step
                    table[kind, row : row + outs, at : at + third] = piece

    def convolve(table, ref, group, kind, finish, lo, hi):
        outs = table.shape[1] // (depth * group)
        planes = (near, far)[kind]

        @pl.loop(lo, hi, unroll=hi - lo if kind == 0 and table is not t3 else 1)
        def _(j):
            halves = []
            for half in range(2):
                y = (2 * j + half) * group
                halves.append(
                    jnp.concatenate(
                        [
                            ref[xp, pl.ds(y, group + 2)].reshape(
                                (group + 2) * ref.shape[2], width
                            )
                            for xp in planes
                        ],
                        axis=0,
                    )
                )
            rhs = jnp.concatenate(halves, axis=1)
            out = jnp.dot(
                table[kind, :, : rhs.shape[0]], rhs, preferred_element_type=jnp.float32
            )
            if kind == 0:
                keep[j] = out
                return
            out = out + keep[j]
            for half in range(2):
                for ox in range(depth):
                    for oy in range(group):
                        row = (ox * group + oy) * outs
                        finish(
                            ox,
                            (2 * j + half) * group + oy,
                            out[row : row + outs, half * width : (half + 1) * width],
                        )

    tiles = pack.shape[1]
    cells_all = float(depth * height * width * total)
    factor = math.sqrt(27.0 * chan)
    lanes = width // chan
    trio = 3 * chan

    def correlate(ref, rows, offset, slot):
        starts_y = range(0, height, 4)
        inner = slice(offset, offset + depth)
        rhs = jnp.concatenate(
            [
                rows[inner, y + offset : y + offset + 4].reshape(depth * 4 * chan, width)
                for y in starts_y
            ],
            axis=1,
        )

        def multiply(planes):
            lhs = jnp.concatenate(
                [ref[planes, y : y + 6, :trio].reshape(-1, width) for y in starts_y], axis=1
            )
            prod[planes] = lax.dot_general(
                lhs, rhs, NT, preferred_element_type=jnp.float32
            ).reshape((-1,) + prod.shape[1:])

        multiply(slice(0, depth + 2))
        for kx in range(3):
            fold(kx, slot)
            scatter(kx, slot)

    slab = 9 * chan
    step_rows = slab // lanes
    batch = step_rows // 8

    def fold(kx, slot):
        group = lax.broadcasted_iota(jnp.int32, (8, width), 1) // chan
        for r in range(0, trio, 8):
            sums = []
            for y in range(6):
                part_sum = prod[kx, y, r : r + 8, :width]
                for x in range(1, depth):
                    part_sum = part_sum + prod[
                        kx + x, y, r : r + 8, x * width : (x + 1) * width
                    ]
                sums.append(part_sum)
            for ky in range(3):
                at = ky * trio + r
                keep_y = sums[ky + 3]
                for y in (2, 1, 0):
                    keep_y = jnp.where(group == y, sums[ky + y], keep_y)
                diag[at : at + 8] = keep_y
        low = group < 2
        even = group % 2 == 0
        for i in range(batch):
            rows = [diag[j * step_rows + 8 * i : j * step_rows + 8 * i + 8] for j in range(4)]
            pairs = []
            for j in range(2):
                one, two = rows[j], rows[j + 2]
                pairs.append(
                    jnp.where(low, one, two)
                    + pltpu.roll(jnp.where(low, two, one), 2 * chan, 1)
                )
            one, two = pairs
            cross = jnp.where(even, two, one)
            pack[slot, kx * batch + i] = jnp.where(even, one, two) + jnp.where(
                even, pltpu.roll(cross, width - chan, 1), pltpu.roll(cross, chan, 1)
            )

    base, extra = owners(sizes)

    def at_spot(spot):
        return jnp.logical_and(
            me[0] == spot[0], jnp.logical_and(me[1] == spot[1], me[2] == spot[2])
        )

    def which(spots):
        found, index = False, 0
        for i, spot in enumerate(spots):
            here = at_spot(spot)
            found = jnp.logical_or(found, here)
            index = index + jnp.where(here, i, 0)
        return found, index

    is_base, base_at = which(base)
    is_extra, extra_at = which(extra)

    def give(slot, t, chunk, spot):
        at = (spot[0] * sizes[1] + spot[1]) * sizes[2] + spot[2]

        @pl.when(line != at)
        def _():
            pltpu.make_async_remote_copy(
                src_ref=pack.at[slot, t],
                dst_ref=land.at[slot, chunk, lax.rem(line - at + total, total) - 1],
                send_sem=asend.at[slot],
                recv_sem=arecv.at[slot, chunk],
                device_id=spot,
                device_id_type=MESH,
            ).start()

    def scatter(kx, slot):
        for w, spot in enumerate(base):
            give(slot, kx * batch + w, kx, spot)
        give(slot, kx * batch + len(base), 0, extra[kx])

    def others():
        axes = [
            [me[i] if d == 0 else lax.rem(me[i] + d, sizes[i]) for d in range(sizes[i])]
            for i in range(3)
        ]
        return list(itertools.product(*axes))[1:]

    def finish_tile(slot, t, chunk, row, column):
        landed = land.at[slot, chunk]
        pltpu.make_async_copy(landed, landed, arecv.at[slot, chunk]).wait()
        rounded = (pack[slot, t] + jnp.sum(land[slot, chunk], axis=0)).astype(part.dtype)
        part[slot, chunk] = rounded
        full[slot, row, column] = rounded

        def tell(spot):
            pltpu.make_async_remote_copy(
                src_ref=part.at[slot, chunk],
                dst_ref=full.at[slot, row, column],
                send_sem=bsend.at[slot],
                recv_sem=brecv.at[slot],
                device_id=spot,
                device_id_type=MESH,
            ).start()

        if total <= 64:
            for spot in others():
                tell(spot)
        else:

            @pl.loop(1, total)
            def _(i):
                tell(place(lax.rem(line + i, total)))

    def gather(slot):
        @pl.when(is_base)
        def _():
            for kx in range(3):
                finish_tile(slot, kx * batch + base_at, kx, base_at, kx)

        @pl.when(is_extra)
        def _():
            finish_tile(slot, extra_at * batch + len(base), 0, len(base), extra_at)

    def drain(slot, out, direction):
        none = jnp.logical_not(jnp.logical_or(is_base, is_extra))
        for owned, here in ((3, is_base), (1, is_extra), (0, none)):

            @pl.when(here)
            def _():
                some = told.at[pl.ds(0, tiles - owned)]
                pltpu.make_async_copy(some, some, brecv.at[slot]).wait()
                sent_all = pack.at[slot, pl.ds(0, tiles - owned)]
                pltpu.make_async_copy(sent_all, sent_all, asend.at[slot]).wait()
                if owned:
                    gone = told.at[pl.ds(0, owned * (total - 1))]
                    pltpu.make_async_copy(gone, gone, bsend.at[slot]).wait()

        for kx in range(3):
            whole = full[slot, :, kx].astype(jnp.float32).reshape(step_rows, width)
            for j in range(lanes):
                at = slice(kx * slab + j * step_rows, kx * slab + (j + 1) * step_rows)
                damp = 0.1 * direction[at].astype(jnp.float32)
                mean = whole[:, j * chan : (j + 1) * chan] * (1.0 / cells_all)
                out[at] = factor * (mean + damp)

    def arrange():
        filt = 27 * chan
        for load in loads[1:]:
            load.wait()
        four = jnp.concatenate([wf[...], vf[...], vs[...], ws[...]], axis=1)
        rows = lax.broadcasted_iota(jnp.int32, (4 * chan, 4 * chan), 0)
        cols = lax.broadcasted_iota(jnp.int32, (4 * chan, 4 * chan), 1)
        eye = jnp.where(rows == cols, 1.0, 0.0).astype(four.dtype)
        turned = lax.dot_general(eye, four, NT, preferred_element_type=jnp.float32)
        turned = turned.astype(w1.dtype)
        w1[...] = turned[: 2 * chan]
        third = 3 * chan
        for k in range(9):
            part = slice(k * third, (k + 1) * third)
            w2[:, 2 * k * third : (2 * k + 1) * third] = turned[2 * chan : 3 * chan, part]
            w2[:, (2 * k + 1) * third : (2 * k + 2) * third] = turned[3 * chan :, part]
        for k in range(27):
            at = filt - (k + 1) * chan
            w3[:, k * chan : (k + 1) * chan] = ws[at : at + chan]

    inner = (slice(1, depth + 1), slice(1, height + 1))
    loads[0].wait()
    for x in range(depth):
        rv[x + 1, 1 : height + 1] = jnp.swapaxes(volume[:, x], 0, 1)
    cells0, cells1, cells2 = (rv, zv, ev, 0), (rp, zp, ep, 1), (rj, zj, ej, 2)
    edges(rv, ev)
    pl.semaphore_wait(barrier, greeted)
    send_rest(cells0, True)
    send_rest(cells0, False)
    send_faces(cells0, 0)
    send_faces(cells0, 1)
    send_faces(cells0, 2)
    build1[...] = jnp.zeros_like(build1)
    build2[...] = jnp.zeros_like(build2)
    for rows, zbuf in ((rv, zv), (rp, zp), (rj, zj)):
        clear(rows, zbuf)
    shifter()
    arrange()
    band(w1, t1, 2)
    band(w2, t2, 4)
    band(w3, t3, 4)

    def first(x, y, out):
        hidden, slope = gelu_pair(out[:chan])
        slope_ref[x, y] = slope
        tangent = slope * out[chan:]
        rp[x + 1, y + 1, :chan] = hidden.astype(jnp.bfloat16)
        rp[x + 1, y + 1, chan:] = tangent.astype(jnp.bfloat16)
        if folds == 2:
            collect(build1, (hidden, tangent), x * height + y)

    def launch():
        sent(cells0)
        send_faces(cells1, 0)

    def launch_rest():
        if folds == 2:
            ep[...] = build1[...].astype(ep.dtype)
        else:
            edges(rp, ep)
        send_rest(cells1, True)
        send_rest(cells1, False)
        send_faces(cells1, 2)

    stage(
        cells0,
        sv,
        t1,
        2,
        first,
        (
            ((0,), 1, launch),
            ((1,), 2, lambda: None),
            ((2,), early // 4, lambda: send_faces(cells1, 1)),
            ((), height // 4, launch_rest),
        ),
    )

    def second(x, y, out):
        rj[x + 1, y + 1] = out.astype(jnp.bfloat16)
        if folds == 2:
            half = chan // 2
            collect(build2, (out[:half], out[half:]), x * height + y)

    def pass_on():
        sent(cells1)
        send_faces(cells2, 0)

    def pass_rest():
        if folds == 2:
            ej[...] = build2[...].astype(ej.dtype)
        else:
            edges(rj, ej)
        send_rest(cells2, True)
        send_rest(cells2, False)
        send_faces(cells2, 1)

    stage(
        cells1,
        sp,
        t2,
        4,
        second,
        (((0, 1), bands, pass_on), ((2,), height // 8, pass_rest)),
    )
    for x in range(depth):
        jv_out[:, x] = jnp.swapaxes(rj[x + 1, 1 : height + 1], 0, 1)
    correlate(sp, rj, 1, 0)

    def third(x, y, out):
        back_ref[x, y] = (slope_ref[x, y] * out).astype(jnp.bfloat16)

    stage(cells2, sj, t3, 4, third, (((0, 1), height // 8, lambda: None),))
    correlate(sv, back_ref, 0, 1)
    gather(0)
    gather(1)
    sent(cells2)
    drain(0, gv2, vs)
    drain(1, gv1, vf)


def place_out(*refs):
    count = len(refs) // 2
    sems = refs[-1]
    copies = [
        pltpu.make_async_copy(refs[i], refs[count + i], sems.at[i]) for i in range(count)
    ]
    for copy in copies:
        copy.start()
    for copy in copies:
        copy.wait()


def body(volume, w_first, w_second, v_first, v_second):
    chan, depth, height, width = volume.shape
    sizes = tuple(lax.axis_size(a) for a in AXES)
    total = sizes[0] * sizes[1] * sizes[2]
    filt = 27 * chan
    tiles = filt * chan // (8 * width)
    _, ways = codes(sizes)
    folds = 2 if 4 * depth * height <= width else 1
    bf, f32 = jnp.bfloat16, jnp.float32
    pads = (depth + 2, height + 2)
    vmem = pl.BlockSpec(memory_space=pltpu.VMEM)
    jv, corr1, corr2 = pl.pallas_call(
        functools.partial(kernel, sizes),
        out_shape=(
            jax.ShapeDtypeStruct(volume.shape, bf),
            jax.ShapeDtypeStruct((filt, chan), f32),
            jax.ShapeDtypeStruct((filt, chan), f32),
        ),
        in_specs=[pl.BlockSpec(memory_space=pltpu.HBM)] * 5,
        out_specs=(vmem,) * 3,
        scratch_shapes=[
            pltpu.VMEM(pads + (chan, width), bf),
            pltpu.VMEM(pads + (2 * chan, width), bf),
            pltpu.VMEM(pads + (chan, width), bf),
            pltpu.VMEM((2, 3, 3, chan // folds, width), bf),
            pltpu.VMEM((2, 3, 3, 2 * chan // folds, width), bf),
            pltpu.VMEM((2, 3, 3, chan // folds, width), bf),
            pltpu.VMEM((chan // folds, width), bf),
            pltpu.VMEM((2 * chan // folds, width), bf),
            pltpu.VMEM((chan // folds, width), bf),
            pltpu.VMEM(pads + (3 * chan, width), bf),
            pltpu.VMEM(pads + (6 * chan, width), bf),
            pltpu.VMEM(pads + (3 * chan, width), bf),
            pltpu.VMEM((depth, height, chan, width), f32),
            pltpu.VMEM((depth, height, chan, width), bf),
            pltpu.VMEM((2, depth * 2 * 2 * chan, depth * 4 * 3 * chan), bf),
            pltpu.VMEM((2, depth * 4 * chan, depth * 6 * 6 * chan), bf),
            pltpu.VMEM((2, depth * 4 * chan, depth * 6 * 3 * chan), bf),
            pltpu.VMEM((2 * width, 2 * width), bf),
            pltpu.VMEM((height // 4, depth * 4 * chan, 2 * width), f32),
            pltpu.VMEM((depth + 2, 6, 3 * chan, depth * 4 * chan), f32),
            pltpu.VMEM((9 * chan, width), f32),
            pltpu.VMEM((2, tiles, 8, width), f32),
            pltpu.VMEM((2, 3, total - 1, 8, width), f32),
            pltpu.VMEM((2, 3, 8, width), bf),
            pltpu.VMEM((2, 9, 3, 8, width), bf),
            pltpu.VMEM(((total - 1) * 3, 8, width), bf),
            pltpu.SemaphoreType.DMA((ways + 4,)),
            pltpu.SemaphoreType.DMA((2, ways + 4)),
            pltpu.SemaphoreType.DMA((2,)),
            pltpu.SemaphoreType.DMA((2, 3)),
            pltpu.SemaphoreType.DMA((2,)),
            pltpu.SemaphoreType.DMA((2,)),
            pltpu.VMEM(volume.shape, bf),
            pltpu.VMEM((filt, chan), bf),
            pltpu.VMEM((filt, chan), bf),
            pltpu.VMEM((filt, chan), bf),
            pltpu.VMEM((filt, chan), bf),
            pltpu.VMEM((2 * chan, filt), bf),
            pltpu.VMEM((chan, 2 * filt), bf),
            pltpu.VMEM((chan, filt), bf),
            pltpu.VMEM((2 * chan // folds, width), f32),
            pltpu.VMEM((chan // folds, width), f32),
            pltpu.SemaphoreType.DMA((5,)),
        ],
        compiler_params=pltpu.CompilerParams(
            collective_id=0, has_side_effects=True, vmem_limit_bytes=48 * 1024 * 1024
        ),
    )(*(pltpu.with_memory_space_constraint(w, pltpu.HBM) for w in (volume, *(w.reshape(filt, chan) for w in (w_first, w_second, v_first, v_second)))))
    jv, corr1, corr2 = pl.pallas_call(
        place_out,
        out_shape=(
            jax.ShapeDtypeStruct(volume.shape, bf),
            jax.ShapeDtypeStruct((filt, chan), f32),
            jax.ShapeDtypeStruct((filt, chan), f32),
        ),
        in_specs=[vmem] * 3,
        out_specs=(pl.BlockSpec(memory_space=pltpu.HBM),) * 3,
        scratch_shapes=[pltpu.SemaphoreType.DMA((3,))],
        compiler_params=pltpu.CompilerParams(vmem_limit_bytes=4 * 1024 * 1024),
    )(jv, corr1, corr2)
    return jv, corr1.reshape(v_first.shape), corr2.reshape(v_second.shape)


def solution(mesh):
    in_specs = (P(None, "gx", "gy", "gz"), P(), P(), P(), P())
    out_specs = (P(None, "gx", "gy", "gz"), P(), P())
    return jax.shard_map(body, mesh=mesh, in_specs=in_specs, out_specs=out_specs, check_vma=False)
```

```python
import functools
import itertools
import math

import jax
import jax.numpy as jnp
from jax import lax
from jax.experimental import pallas as pl
from jax.experimental.pallas import tpu as pltpu
from jax.sharding import PartitionSpec as P

MESH = pl.DeviceIdType.MESH
AXES = ("gx", "gy", "gz")
STEPS = [d for d in itertools.product((-1, 0, 1), repeat=3) if d != (0, 0, 0)]
STEPS.sort(key=lambda d: (d[2] != 0, d[0] == 0, abs(d[0]) + abs(d[1])))
NT = (((1,), (1,)), ((), ()))


def gelu_pair(pre):
    inner = 0.7978845608 * (pre + 0.044715 * pre * pre * pre)
    hyper = jnp.tanh(inner)
    hidden = 0.5 * pre * (1.0 + hyper)
    slope = 0.5 * (1.0 + hyper) + 0.5 * pre * (1.0 - hyper * hyper) * 0.7978845608 * (
        1.0 + 0.134145 * pre * pre
    )
    return hidden, slope


def codes(sizes):
    spans = [3 if size > 2 else 2 for size in sizes]

    def code(step):
        total = 0
        for delta, span in zip(step, spans):
            total = total * span + (delta + 1 if span == 3 else abs(delta))
        return total

    return code, math.prod(spans)


def owners(sizes):
    mids = min(2, sizes[0])
    start = (sizes[0] - mids) // 2
    spots = [
        (x, y, z)
        for z in range(sizes[2])
        for y in range(sizes[1])
        for x in range(start, start + mids)
    ]
    base = [spot for spot in spots if spot[2] % 2 == 1][:8]
    rest = [spot for spot in spots if spot not in base]
    return base, [rest[0], rest[-1], rest[len(rest) // 2 - 1]]


def kernel(
    sizes,
    volume_hbm,
    wf_hbm,
    ws_hbm,
    vf_hbm,
    vs_hbm,
    jv_out,
    gv1,
    gv2,
    *scratch,
):
    (rv, rp, rj, zv, zp, zj, ev, ep, ej, sv, sp, sj, slope_ref, back_ref,
     t1, t2, t3, shift, keep, prod, diag, pack, land, part, full, told,
     hsend, hrecv, asend, arecv, bsend, brecv,
     volume, wf, ws, vf, vs, w1, w2, w3, build1, build2, isem) = scratch
    chan, depth, height, width = volume.shape
    code, ways = codes(sizes)
    early = height - 4
    bands = (early - 1) // 8
    cuts = ((5, 9, height), (4, 8 * bands + 1, height), (8 * bands, height))
    loads = [
        pltpu.make_async_copy(src, dst, isem.at[i])
        for i, (src, dst) in enumerate(
            (
                (volume_hbm, volume),
                (wf_hbm, wf),
                (ws_hbm, ws),
                (vf_hbm, vf),
                (vs_hbm, vs),
            )
        )
    ]
    for load in loads:
        load.start()
    me = tuple(lax.axis_index(a) for a in AXES)
    total = sizes[0] * sizes[1] * sizes[2]
    line = (me[0] * sizes[1] + me[1]) * sizes[2] + me[2]

    def place(index):
        return (
            index // (sizes[1] * sizes[2]),
            index // sizes[2] % sizes[1],
            index % sizes[2],
        )

    def there(step):
        ok = None
        for pos, size, delta in zip(me, sizes, step):
            if delta == -1:
                term = pos > 0
            elif delta == 1:
                term = pos < size - 1
            else:
                continue
            ok = term if ok is None else jnp.logical_and(ok, term)
        return ok

    barrier = pltpu.get_barrier_semaphore()
    near_only = max(sizes) <= 4

    if near_only:
        greeted = 0
        for step in STEPS:
            ok = there(step)
            greeted = greeted + jnp.where(ok, 1, 0)

            @pl.when(ok)
            def _():
                pl.semaphore_signal(
                    barrier,
                    inc=1,
                    device_id=tuple(p + d for p, d in zip(me, step)),
                    device_id_type=MESH,
                )
    else:
        greeted = total - 1

        @pl.loop(1, total)
        def _(i):
            pl.semaphore_signal(
                barrier, inc=1, device_id=place(lax.rem(line + i, total)), device_id_type=MESH
            )

    def source(delta, extent):
        return {-1: pl.ds(1, 1), 1: pl.ds(extent, 1), 0: pl.ds(1, extent)}[delta]

    def target(delta, extent):
        return {-1: pl.ds(extent + 1, 1), 1: pl.ds(0, 1), 0: pl.ds(1, extent)}[delta]

    def pieces(step, slot):
        if step[1] or step[2]:
            return [None]
        ends = cuts[slot]
        return [(p, lo, hi) for p, (lo, hi) in enumerate(zip((0,) + ends, ends))]

    def landing(step, rows, zbuf, piece=None):
        if step[2] == 0:
            if piece is None:
                return rows.at[target(step[0], depth), target(step[1], height)]
            _, lo, hi = piece
            return rows.at[target(step[0], depth), pl.ds(1 + lo, hi - lo)]
        return zbuf.at[0 if step[2] == 1 else 1, 1 - step[0], 1 - step[1]]

    def message(step, rows, zbuf, edge, slot, piece=None):
        lane = code(step)
        if step[2] != 0:
            src = edge
        elif piece is None:
            src = rows.at[source(step[0], depth), source(step[1], height)]
        else:
            part, lo, hi = piece
            src = rows.at[source(step[0], depth), pl.ds(1 + lo, hi - lo)]
            if part:
                lane = ways + 2 * (part - 1) + (step[0] > 0)
        return pltpu.make_async_remote_copy(
            src_ref=src,
            dst_ref=landing(step, rows, zbuf, piece),
            send_sem=hsend.at[lane],
            recv_sem=hrecv.at[slot % 2, lane],
            device_id=tuple(p + d for p, d in zip(me, step)),
            device_id_type=MESH,
        )

    def send_faces(halo, part):
        for step in STEPS:
            found = pieces(step, halo[3])
            if found == [None] or part >= len(found):
                continue

            @pl.when(there(step))
            def _():
                message(step, *halo, found[part]).start()

    def send_rest(halo, cross):
        for step in STEPS:
            if (step[2] != 0) == cross and pieces(step, halo[3]) == [None]:

                @pl.when(there(step))
                def _():
                    message(step, *halo).start()

    def clear(rows, zbuf):
        for step in STEPS:
            back = tuple(-d for d in step)

            @pl.when(jnp.logical_not(there(back)))
            def _():
                ref = landing(step, rows, zbuf)
                ref[...] = jnp.zeros(ref.shape, ref.dtype)

    def receive(halo, kind, parts):
        for step in STEPS:
            if (step[0] != 0) != (kind == 1):
                continue
            found = pieces(step, halo[3])
            if found == [None]:
                found = found if 0 in parts else []
            else:
                found = [piece for piece in found if piece[0] in parts]
            if not found:
                continue
            back = tuple(-d for d in step)

            @pl.when(there(back))
            def _():
                for piece in found:
                    message(step, *halo, piece).wait_recv()

    def stage(halo, out, table, group, finish, plan):
        rows, zbuf, _, slot = halo
        receive(halo, 0, (0,))
        spread(rows, zbuf, out, near, 0, height + 2)
        if len(plan) > 1:
            convolve(table, out, group, 0, finish, 0, height // (2 * group))
        done = 0
        for parts, upto, hook in plan:
            if parts:
                receive(halo, 1, parts)
                last = cuts[slot][parts[-1]]
                end = height + 2 if last == height else last + 1
                start = 0 if parts[0] == 0 else cuts[slot][parts[0] - 1] + 1
                spread(rows, zbuf, out, far, start, end)
            convolve(table, out, group, 1 if len(plan) > 1 else 2, finish, done, upto)
            done = upto
            hook()

    def sent(halo):
        for step in STEPS:

            @pl.when(there(step))
            def _():
                for piece in pieces(step, halo[3]):
                    message(step, *halo, piece).wait_send()

    cells = depth * height
    folds = 2 if 4 * cells <= width else 1
    pitch = width // folds

    def collect(build, bits, at):
        count = bits[0].shape[0]
        pair = lax.broadcasted_iota(jnp.int32, (count, width), 1) // 2
        built = build[...]
        for f, bit in enumerate(bits):
            spot = f * (pitch // 2) + at
            built = jnp.where(pair == spot, pltpu.roll(bit, 2 * spot + 1, 1), built)
        build[...] = built

    def edges(rows, edge):
        count = edge.shape[0]
        lane = lax.broadcasted_iota(jnp.int32, (count, width), 1)
        pair = lane // 2
        whole = jnp.zeros((count, width), jnp.float32)
        for f in range(folds):
            part_rows = slice(f * count, (f + 1) * count)
            built = jnp.zeros((count, width), jnp.float32)
            for x in range(depth):
                for y in range(height):
                    row = rows[x + 1, y + 1, part_rows].astype(jnp.float32)
                    spot = f * (pitch // 2) + x * height + y
                    shift_by = (2 * spot + 1) % width
                    built = jnp.where(pair == spot, pltpu.roll(row, shift_by, 1), built)
            whole = jnp.where(lane < f * pitch, whole, built)
        edge[...] = whole.astype(edge.dtype)

    def shifter():
        src = lax.broadcasted_iota(jnp.int32, (2 * width, 2 * width), 0)
        dst = lax.broadcasted_iota(jnp.int32, (2 * width, 2 * width), 1)
        spot = src % pitch
        used = jnp.logical_and(src >= width, spot < 2 * cells)
        right = jnp.logical_and(used, spot % 2 == 1)
        left = jnp.logical_and(used, spot % 2 == 0)
        low = jnp.logical_or(
            jnp.logical_and(src == dst - 1, src < width - 1),
            jnp.logical_and(dst == 0, left),
        )
        high = jnp.logical_or(
            jnp.logical_and(src == dst - width + 1, src < width),
            jnp.logical_and(dst == 2 * width - 1, right),
        )
        pick = jnp.logical_or(
            jnp.logical_and(dst < width, low), jnp.logical_and(dst >= width, high)
        )
        shift[...] = jnp.where(pick, 1.0, 0.0).astype(shift.dtype)

    near = tuple(range(1, depth + 1))
    far = (0, depth + 1)

    def spread(rows, zbuf, out, planes, start, end):
        count = rows.shape[2]
        part = zbuf.shape[3]
        groups = count // chan
        span = end - start
        lane = lax.broadcasted_iota(jnp.int32, (part, width), 1)

        for xp in planes:
            dx = 0 if xp == 0 else (2 if xp == depth + 1 else 1)
            halo = []
            for yp in range(start, end):
                dy = 0 if yp == 0 else (2 if yp == height + 1 else 1)
                left = zbuf[0, dx, dy].astype(jnp.float32)
                right = zbuf[1, dx, dy].astype(jnp.float32)
                for f in range(folds):
                    at = f * pitch + 2 * ((xp - 1) % depth * height + (yp - 1) % height)
                    both = jnp.where(
                        lane == at + 1, right, jnp.where(lane == at, left, 0.0)
                    )
                    halo.append(both.astype(rows.dtype))
            wide = rows[xp, start:end].reshape(span * count, width)
            lhs = jnp.concatenate([wide, jnp.concatenate(halo, axis=0)], axis=1)
            moved = jnp.dot(lhs, shift[...], preferred_element_type=jnp.float32)
            moved = moved.astype(rows.dtype).reshape(span, count, 2 * width)
            kept = wide.reshape(span, count, width)
            for g in range(groups):
                at = slice(g * chan, (g + 1) * chan)
                base = g * 3 * chan
                out[xp, start:end, base : base + chan] = moved[:, at, :width]
                out[xp, start:end, base + chan : base + 2 * chan] = kept[:, at]
                out[xp, start:end, base + 2 * chan : base + 3 * chan] = moved[:, at, width:]

    def band(weights, table, group):
        outs = weights.shape[0]
        third = weights.shape[1] // 3
        step = third // 3
        table[...] = jnp.zeros_like(table)
        for kx in range(3):
            piece = weights[:, kx * third : (kx + 1) * third]
            for ox in range(depth):
                xp = ox + kx
                kind, pos = (0, near.index(xp)) if xp in near else (1, far.index(xp))
                for oy in range(group):
                    row = (ox * group + oy) * outs
                    at = (pos * (group + 2) + oy) * step
                    table[kind, row : row + outs, at : at + third] = piece

    def convolve(table, ref, group, kind, finish, lo, hi):
        outs = table.shape[1] // (depth * group)
        planes = (near, far, near + far)[kind]

        @pl.loop(lo, hi, unroll=1 if kind == 1 else hi - lo)
        def _(j):
            halves = []
            for half in range(2):
                y = (2 * j + half) * group
                halves.append(
                    jnp.concatenate(
                        [
                            ref[xp, pl.ds(y, group + 2)].reshape(
                                (group + 2) * ref.shape[2], width
                            )
                            for xp in planes
                        ],
                        axis=0,
                    )
                )
            rhs = jnp.concatenate(halves, axis=1)
            if kind == 2:
                weights = jnp.concatenate([table[0], table[1]], axis=1)
            else:
                weights = table[kind, :, : rhs.shape[0]]
            out = jnp.dot(weights, rhs, preferred_element_type=jnp.float32)
            if kind == 0:
                keep[j] = out
                return
            if kind == 1:
                out = out + keep[j]
            for half in range(2):
                for ox in range(depth):
                    for oy in range(group):
                        row = (ox * group + oy) * outs
                        finish(
                            ox,
                            (2 * j + half) * group + oy,
                            out[row : row + outs, half * width : (half + 1) * width],
                        )

    tiles = pack.shape[1]
    cells_all = float(depth * height * width * total)
    factor = math.sqrt(27.0 * chan)
    lanes = width // chan
    trio = 3 * chan

    def correlate(ref, rows, offset, slot):
        starts_y = range(0, height, 4)
        inner = slice(offset, offset + depth)
        rhs = jnp.concatenate(
            [
                rows[inner, y + offset : y + offset + 4].reshape(depth * 4 * chan, width)
                for y in starts_y
            ],
            axis=1,
        )

        def multiply(planes):
            lhs = jnp.concatenate(
                [ref[planes, y : y + 6, :trio].reshape(-1, width) for y in starts_y], axis=1
            )
            prod[planes] = lax.dot_general(
                lhs, rhs, NT, preferred_element_type=jnp.float32
            ).reshape((-1,) + prod.shape[1:])

        multiply(slice(0, depth + 2))
        for kx in range(3):
            fold(kx, slot)
            scatter(kx, slot)

    slab = 9 * chan
    step_rows = slab // lanes
    batch = step_rows // 8

    def fold(kx, slot):
        group = lax.broadcasted_iota(jnp.int32, (8, width), 1) // chan
        for r in range(0, trio, 8):
            sums = []
            for y in range(6):
                part_sum = prod[kx, y, r : r + 8, :width]
                for x in range(1, depth):
                    part_sum = part_sum + prod[
                        kx + x, y, r : r + 8, x * width : (x + 1) * width
                    ]
                sums.append(part_sum)
            for ky in range(3):
                at = ky * trio + r
                keep_y = sums[ky + 3]
                for y in (2, 1, 0):
                    keep_y = jnp.where(group == y, sums[ky + y], keep_y)
                diag[at : at + 8] = keep_y
        low = group < 2
        even = group % 2 == 0
        for i in range(batch):
            rows = [diag[j * step_rows + 8 * i : j * step_rows + 8 * i + 8] for j in range(4)]
            pairs = []
            for j in range(2):
                one, two = rows[j], rows[j + 2]
                pairs.append(
                    jnp.where(low, one, two)
                    + pltpu.roll(jnp.where(low, two, one), 2 * chan, 1)
                )
            one, two = pairs
            cross = jnp.where(even, two, one)
            pack[slot, kx * batch + i] = jnp.where(even, one, two) + jnp.where(
                even, pltpu.roll(cross, width - chan, 1), pltpu.roll(cross, chan, 1)
            )

    base, extra = owners(sizes)

    def at_spot(spot):
        return jnp.logical_and(
            me[0] == spot[0], jnp.logical_and(me[1] == spot[1], me[2] == spot[2])
        )

    def which(spots):
        found, index = False, 0
        for i, spot in enumerate(spots):
            here = at_spot(spot)
            found = jnp.logical_or(found, here)
            index = index + jnp.where(here, i, 0)
        return found, index

    is_base, base_at = which(base)
    is_extra, extra_at = which(extra)

    def give(slot, t, chunk, spot):
        at = (spot[0] * sizes[1] + spot[1]) * sizes[2] + spot[2]

        @pl.when(line != at)
        def _():
            pltpu.make_async_remote_copy(
                src_ref=pack.at[slot, t],
                dst_ref=land.at[slot, chunk, lax.rem(line - at + total, total) - 1],
                send_sem=asend.at[slot],
                recv_sem=arecv.at[slot, chunk],
                device_id=spot,
                device_id_type=MESH,
            ).start()

    def scatter(kx, slot):
        for w, spot in enumerate(base):
            give(slot, kx * batch + w, kx, spot)
        give(slot, kx * batch + len(base), 0, extra[kx])

    def others():
        axes = [
            [me[i] if d == 0 else lax.rem(me[i] + d, sizes[i]) for d in range(sizes[i])]
            for i in range(3)
        ]
        return list(itertools.product(*axes))[1:]

    def finish_tile(slot, t, chunk, row, column):
        landed = land.at[slot, chunk]
        pltpu.make_async_copy(landed, landed, arecv.at[slot, chunk]).wait()
        rounded = (pack[slot, t] + jnp.sum(land[slot, chunk], axis=0)).astype(part.dtype)
        part[slot, chunk] = rounded
        full[slot, row, column] = rounded

        def tell(spot):
            pltpu.make_async_remote_copy(
                src_ref=part.at[slot, chunk],
                dst_ref=full.at[slot, row, column],
                send_sem=bsend.at[slot],
                recv_sem=brecv.at[slot],
                device_id=spot,
                device_id_type=MESH,
            ).start()

        if total <= 64:
            for spot in others():
                tell(spot)
        else:

            @pl.loop(1, total)
            def _(i):
                tell(place(lax.rem(line + i, total)))

    def gather(slot):
        @pl.when(is_base)
        def _():
            for kx in range(3):
                finish_tile(slot, kx * batch + base_at, kx, base_at, kx)

        @pl.when(is_extra)
        def _():
            finish_tile(slot, extra_at * batch + len(base), 0, len(base), extra_at)

    def drain(slot, out, direction):
        none = jnp.logical_not(jnp.logical_or(is_base, is_extra))
        for owned, here in ((3, is_base), (1, is_extra), (0, none)):

            @pl.when(here)
            def _():
                some = told.at[pl.ds(0, tiles - owned)]
                pltpu.make_async_copy(some, some, brecv.at[slot]).wait()
                sent_all = pack.at[slot, pl.ds(0, tiles - owned)]
                pltpu.make_async_copy(sent_all, sent_all, asend.at[slot]).wait()
                if owned:
                    gone = told.at[pl.ds(0, owned * (total - 1))]
                    pltpu.make_async_copy(gone, gone, bsend.at[slot]).wait()

        for kx in range(3):
            whole = full[slot, :, kx].astype(jnp.float32).reshape(step_rows, width)
            for j in range(lanes):
                at = slice(kx * slab + j * step_rows, kx * slab + (j + 1) * step_rows)
                damp = 0.1 * direction[at].astype(jnp.float32)
                mean = whole[:, j * chan : (j + 1) * chan] * (1.0 / cells_all)
                out[at] = factor * (mean + damp)

    def arrange():
        filt = 27 * chan
        for load in loads[1:]:
            load.wait()
        four = jnp.concatenate([wf[...], vf[...], vs[...], ws[...]], axis=1)
        rows = lax.broadcasted_iota(jnp.int32, (4 * chan, 4 * chan), 0)
        cols = lax.broadcasted_iota(jnp.int32, (4 * chan, 4 * chan), 1)
        eye = jnp.where(rows == cols, 1.0, 0.0).astype(four.dtype)
        turned = lax.dot_general(eye, four, NT, preferred_element_type=jnp.float32)
        turned = turned.astype(w1.dtype)
        w1[...] = turned[: 2 * chan]
        third = 3 * chan
        for k in range(9):
            part = slice(k * third, (k + 1) * third)
            w2[:, 2 * k * third : (2 * k + 1) * third] = turned[2 * chan : 3 * chan, part]
            w2[:, (2 * k + 1) * third : (2 * k + 2) * third] = turned[3 * chan :, part]
        for k in range(27):
            at = filt - (k + 1) * chan
            w3[:, k * chan : (k + 1) * chan] = ws[at : at + chan]

    inner = (slice(1, depth + 1), slice(1, height + 1))
    loads[0].wait()
    for x in range(depth):
        rv[x + 1, 1 : height + 1] = jnp.swapaxes(volume[:, x], 0, 1)
    cells0, cells1, cells2 = (rv, zv, ev, 0), (rp, zp, ep, 1), (rj, zj, ej, 2)
    edges(rv, ev)
    pl.semaphore_wait(barrier, greeted)
    send_rest(cells0, True)
    send_rest(cells0, False)
    send_faces(cells0, 0)
    send_faces(cells0, 1)
    send_faces(cells0, 2)
    build1[...] = jnp.zeros_like(build1)
    build2[...] = jnp.zeros_like(build2)
    for rows, zbuf in ((rv, zv), (rp, zp), (rj, zj)):
        clear(rows, zbuf)
    shifter()
    arrange()
    band(w1, t1, 2)
    band(w2, t2, 4)
    band(w3, t3, 4)

    def first(x, y, out):
        hidden, slope = gelu_pair(out[:chan])
        slope_ref[x, y] = slope
        tangent = slope * out[chan:]
        rp[x + 1, y + 1, :chan] = hidden.astype(jnp.bfloat16)
        rp[x + 1, y + 1, chan:] = tangent.astype(jnp.bfloat16)
        if folds == 2:
            collect(build1, (hidden, tangent), x * height + y)

    def launch():
        sent(cells0)
        send_faces(cells1, 0)

    def launch_rest():
        if folds == 2:
            ep[...] = build1[...].astype(ep.dtype)
        else:
            edges(rp, ep)
        send_rest(cells1, True)
        send_rest(cells1, False)
        send_faces(cells1, 2)

    stage(
        cells0,
        sv,
        t1,
        2,
        first,
        (
            ((0,), 1, launch),
            ((1,), 2, lambda: None),
            ((2,), early // 4, lambda: send_faces(cells1, 1)),
            ((), height // 4, launch_rest),
        ),
    )

    def second(x, y, out):
        rj[x + 1, y + 1] = out.astype(jnp.bfloat16)
        if folds == 2:
            half = chan // 2
            collect(build2, (out[:half], out[half:]), x * height + y)

    def pass_on():
        sent(cells1)
        send_faces(cells2, 0)

    def pass_rest():
        if folds == 2:
            ej[...] = build2[...].astype(ej.dtype)
        else:
            edges(rj, ej)
        send_rest(cells2, True)
        send_rest(cells2, False)
        send_faces(cells2, 1)

    stage(
        cells1,
        sp,
        t2,
        4,
        second,
        (((0, 1), bands, pass_on), ((2,), height // 8, pass_rest)),
    )
    for x in range(depth):
        jv_out[:, x] = jnp.swapaxes(rj[x + 1, 1 : height + 1], 0, 1)
    correlate(sp, rj, 1, 0)

    def third(x, y, out):
        back_ref[x, y] = (slope_ref[x, y] * out).astype(jnp.bfloat16)

    stage(cells2, sj, t3, 4, third, (((0, 1), height // 8, lambda: None),))
    correlate(sv, back_ref, 0, 1)
    gather(0)
    gather(1)
    sent(cells2)
    drain(0, gv2, vs)
    drain(1, gv1, vf)


def place_out(*refs):
    count = len(refs) // 2
    sems = refs[-1]
    copies = [
        pltpu.make_async_copy(refs[i], refs[count + i], sems.at[i]) for i in range(count)
    ]
    for copy in copies:
        copy.start()
    for copy in copies:
        copy.wait()


def body(volume, w_first, w_second, v_first, v_second):
    chan, depth, height, width = volume.shape
    sizes = tuple(lax.axis_size(a) for a in AXES)
    total = sizes[0] * sizes[1] * sizes[2]
    filt = 27 * chan
    tiles = filt * chan // (8 * width)
    _, ways = codes(sizes)
    folds = 2 if 4 * depth * height <= width else 1
    bf, f32 = jnp.bfloat16, jnp.float32
    pads = (depth + 2, height + 2)
    vmem = pl.BlockSpec(memory_space=pltpu.VMEM)
    jv, corr1, corr2 = pl.pallas_call(
        functools.partial(kernel, sizes),
        out_shape=(
            jax.ShapeDtypeStruct(volume.shape, bf),
            jax.ShapeDtypeStruct((filt, chan), f32),
            jax.ShapeDtypeStruct((filt, chan), f32),
        ),
        in_specs=[pl.BlockSpec(memory_space=pltpu.HBM)] * 5,
        out_specs=(vmem,) * 3,
        scratch_shapes=[
            pltpu.VMEM(pads + (chan, width), bf),
            pltpu.VMEM(pads + (2 * chan, width), bf),
            pltpu.VMEM(pads + (chan, width), bf),
            pltpu.VMEM((2, 3, 3, chan // folds, width), bf),
            pltpu.VMEM((2, 3, 3, 2 * chan // folds, width), bf),
            pltpu.VMEM((2, 3, 3, chan // folds, width), bf),
            pltpu.VMEM((chan // folds, width), bf),
            pltpu.VMEM((2 * chan // folds, width), bf),
            pltpu.VMEM((chan // folds, width), bf),
            pltpu.VMEM(pads + (3 * chan, width), bf),
            pltpu.VMEM(pads + (6 * chan, width), bf),
            pltpu.VMEM(pads + (3 * chan, width), bf),
            pltpu.VMEM((depth, height, chan, width), f32),
            pltpu.VMEM((depth, height, chan, width), bf),
            pltpu.VMEM((2, depth * 2 * 2 * chan, depth * 4 * 3 * chan), bf),
            pltpu.VMEM((2, depth * 4 * chan, depth * 6 * 6 * chan), bf),
            pltpu.VMEM((2, depth * 4 * chan, depth * 6 * 3 * chan), bf),
            pltpu.VMEM((2 * width, 2 * width), bf),
            pltpu.VMEM((height // 4, depth * 4 * chan, 2 * width), f32),
            pltpu.VMEM((depth + 2, 6, 3 * chan, depth * 4 * chan), f32),
            pltpu.VMEM((9 * chan, width), f32),
            pltpu.VMEM((2, tiles, 8, width), f32),
            pltpu.VMEM((2, 3, total - 1, 8, width), f32),
            pltpu.VMEM((2, 3, 8, width), bf),
            pltpu.VMEM((2, 9, 3, 8, width), bf),
            pltpu.VMEM(((total - 1) * 3, 8, width), bf),
            pltpu.SemaphoreType.DMA((ways + 4,)),
            pltpu.SemaphoreType.DMA((2, ways + 4)),
            pltpu.SemaphoreType.DMA((2,)),
            pltpu.SemaphoreType.DMA((2, 3)),
            pltpu.SemaphoreType.DMA((2,)),
            pltpu.SemaphoreType.DMA((2,)),
            pltpu.VMEM(volume.shape, bf),
            pltpu.VMEM((filt, chan), bf),
            pltpu.VMEM((filt, chan), bf),
            pltpu.VMEM((filt, chan), bf),
            pltpu.VMEM((filt, chan), bf),
            pltpu.VMEM((2 * chan, filt), bf),
            pltpu.VMEM((chan, 2 * filt), bf),
            pltpu.VMEM((chan, filt), bf),
            pltpu.VMEM((2 * chan // folds, width), f32),
            pltpu.VMEM((chan // folds, width), f32),
            pltpu.SemaphoreType.DMA((5,)),
        ],
        compiler_params=pltpu.CompilerParams(
            collective_id=0, has_side_effects=True, vmem_limit_bytes=48 * 1024 * 1024
        ),
    )(*(pltpu.with_memory_space_constraint(w, pltpu.HBM) for w in (volume, *(w.reshape(filt, chan) for w in (w_first, w_second, v_first, v_second)))))
    jv, corr1, corr2 = pl.pallas_call(
        place_out,
        out_shape=(
            jax.ShapeDtypeStruct(volume.shape, bf),
            jax.ShapeDtypeStruct((filt, chan), f32),
            jax.ShapeDtypeStruct((filt, chan), f32),
        ),
        in_specs=[vmem] * 3,
        out_specs=(pl.BlockSpec(memory_space=pltpu.HBM),) * 3,
        scratch_shapes=[pltpu.SemaphoreType.DMA((3,))],
        compiler_params=pltpu.CompilerParams(vmem_limit_bytes=4 * 1024 * 1024),
    )(jv, corr1, corr2)
    return jv, corr1.reshape(v_first.shape), corr2.reshape(v_second.shape)


def solution(mesh):
    in_specs = (P(None, "gx", "gy", "gz"), P(), P(), P(), P())
    out_specs = (P(None, "gx", "gy", "gz"), P(), P())
    return jax.shard_map(body, mesh=mesh, in_specs=in_specs, out_specs=out_specs, check_vma=False)
```

```python
import functools
import itertools
import math

import jax
import jax.numpy as jnp
from jax import lax
from jax.experimental import pallas as pl
from jax.experimental.pallas import tpu as pltpu
from jax.sharding import PartitionSpec as P

MESH = pl.DeviceIdType.MESH
AXES = ("gx", "gy", "gz")
STEPS = [d for d in itertools.product((-1, 0, 1), repeat=3) if d != (0, 0, 0)]
STEPS.sort(key=lambda d: (d[2] != 0, d[0] == 0, abs(d[0]) + abs(d[1])))
NT = (((1,), (1,)), ((), ()))


def gelu_pair(pre):
    inner = 0.7978845608 * (pre + 0.044715 * pre * pre * pre)
    hyper = jnp.tanh(inner)
    hidden = 0.5 * pre * (1.0 + hyper)
    slope = 0.5 * (1.0 + hyper) + 0.5 * pre * (1.0 - hyper * hyper) * 0.7978845608 * (
        1.0 + 0.134145 * pre * pre
    )
    return hidden, slope


def codes(sizes):
    spans = [3 if size > 2 else 2 for size in sizes[:2]]

    def code(step):
        total = 0
        for delta, span in zip(step, spans):
            total = total * span + (delta + 1 if span == 3 else abs(delta))
        return total

    return code, math.prod(spans)


def owners(sizes):
    mids = min(2, sizes[0])
    start = (sizes[0] - mids) // 2
    spots = [
        (x, y, z)
        for z in range(sizes[2])
        for y in range(sizes[1])
        for x in range(start, start + mids)
    ]
    base = [spot for spot in spots if spot[2] % 2 == 1][:8]
    rest = [spot for spot in spots if spot not in base]
    return base, [rest[0], rest[-1], rest[len(rest) // 2 - 1]]


def kernel(
    sizes,
    volume_hbm,
    wf_hbm,
    ws_hbm,
    vf_hbm,
    vs_hbm,
    jv_out,
    gv1,
    gv2,
    *scratch,
):
    (rv, rp, rj, zv, zp, zj, ev, ep, ej, sv, sp, sj, slope_ref, back_ref,
     t1, t2, t3, shift, keep, prod, diag, pack, land, part, full, told,
     hsend, hrecv, asend, arecv, bsend, brecv,
     volume, wf, ws, vf, vs, w1, w2, w3, build1, build2, blank, isem) = scratch
    chan, depth, height, width = volume.shape
    code, ways = codes(sizes)
    early = height - 4
    bands = (early - 1) // 8
    cuts = ((5, 9, height), (4, 8 * bands + 1, height), (8 * bands, height))
    loads = [
        pltpu.make_async_copy(src, dst, isem.at[i])
        for i, (src, dst) in enumerate(
            (
                (volume_hbm, volume),
                (wf_hbm, wf),
                (ws_hbm, ws),
                (vf_hbm, vf),
                (vs_hbm, vs),
            )
        )
    ]
    for load in loads:
        load.start()
    me = tuple(lax.axis_index(a) for a in AXES)
    total = sizes[0] * sizes[1] * sizes[2]
    line = (me[0] * sizes[1] + me[1]) * sizes[2] + me[2]

    def place(index):
        return (
            index // (sizes[1] * sizes[2]),
            index // sizes[2] % sizes[1],
            index % sizes[2],
        )

    def there(step):
        ok = None
        for pos, size, delta in zip(me, sizes, step):
            if delta == -1:
                term = pos > 0
            elif delta == 1:
                term = pos < size - 1
            else:
                continue
            ok = term if ok is None else jnp.logical_and(ok, term)
        return ok

    barrier = pltpu.get_barrier_semaphore()
    near_only = max(sizes) <= 4

    if near_only:
        greeted = 0
        for step in STEPS:
            ok = there(step)
            greeted = greeted + jnp.where(ok, 1, 0)

            @pl.when(ok)
            def _():
                pl.semaphore_signal(
                    barrier,
                    inc=1,
                    device_id=tuple(p + d for p, d in zip(me, step)),
                    device_id_type=MESH,
                )
    else:
        greeted = total - 1

        @pl.loop(1, total)
        def _(i):
            pl.semaphore_signal(
                barrier, inc=1, device_id=place(lax.rem(line + i, total)), device_id_type=MESH
            )

    def source(delta, extent):
        return {-1: pl.ds(1, 1), 1: pl.ds(extent, 1), 0: pl.ds(1, extent)}[delta]

    def target(delta, extent):
        return {-1: pl.ds(extent + 1, 1), 1: pl.ds(0, 1), 0: pl.ds(1, extent)}[delta]

    def pieces(step, slot):
        if step[1] or step[2]:
            return [None]
        ends = cuts[slot]
        return [(p, lo, hi) for p, (lo, hi) in enumerate(zip((0,) + ends, ends))]

    def landing(step, rows, zbuf, piece=None):
        if step[2] == 0:
            if piece is None:
                return rows.at[target(step[0], depth), target(step[1], height)]
            _, lo, hi = piece
            return rows.at[target(step[0], depth), pl.ds(1 + lo, hi - lo)]
        return zbuf.at[0 if step[2] == 1 else 1, 1 - step[0], 1 - step[1]]

    def message(step, rows, zbuf, edge, slot, piece=None):
        lane = take = code(step)
        if step[2] != 0:
            src = edge
            lane = ways + 4
            take = lane + (step[0] != 0)
        elif piece is None:
            src = rows.at[source(step[0], depth), source(step[1], height)]
        else:
            part, lo, hi = piece
            src = rows.at[source(step[0], depth), pl.ds(1 + lo, hi - lo)]
            if part:
                lane = take = ways + 2 * (part - 1) + (step[0] > 0)
        return pltpu.make_async_remote_copy(
            src_ref=src,
            dst_ref=landing(step, rows, zbuf, piece),
            send_sem=hsend.at[lane],
            recv_sem=hrecv.at[slot % 2, take],
            device_id=tuple(p + d for p, d in zip(me, step)),
            device_id_type=MESH,
        )

    def send_faces(halo, part):
        for step in STEPS:
            found = pieces(step, halo[3])
            if found == [None] or part >= len(found):
                continue

            @pl.when(there(step))
            def _():
                message(step, *halo, found[part]).start()

    def send_rest(halo, cross):
        for step in STEPS:
            if (step[2] != 0) == cross and pieces(step, halo[3]) == [None]:

                @pl.when(there(step))
                def _():
                    message(step, *halo).start()

    def clear(rows, zbuf):
        for step in STEPS:
            back = tuple(-d for d in step)

            @pl.when(jnp.logical_not(there(back)))
            def _():
                ref = landing(step, rows, zbuf)
                ref[...] = jnp.zeros(ref.shape, ref.dtype)

    def crosswise(halo, sem, kinds):
        rows_each = halo[2].shape[0] // (chan // folds)
        beside = [jnp.where(p > 0, 1, 0) + jnp.where(p < n - 1, 1, 0) for p, n in zip(me, sizes)]
        options = [(0,) if n == 1 else (1,) if n == 2 else (1, 2) for n in sizes]
        for nx, ny, nz in itertools.product(*options):
            count = nz * (1 + ny) * sum(nx if kind else 1 for kind in kinds) * rows_each
            if not count:
                continue
            fits = jnp.logical_and(
                beside[0] == nx, jnp.logical_and(beside[1] == ny, beside[2] == nz)
            )

            @pl.when(fits)
            def _():
                gone = blank.at[pl.ds(0, count)]
                pltpu.make_async_copy(gone, gone, sem).wait()

    def receive(halo, kind, parts):
        if 0 in parts:
            crosswise(halo, hrecv.at[halo[3] % 2, ways + 4 + kind], (kind,))
        for step in STEPS:
            if (step[0] != 0) != (kind == 1):
                continue
            found = pieces(step, halo[3])
            if step[2] != 0:
                continue
            if found == [None]:
                found = found if 0 in parts else []
            else:
                found = [piece for piece in found if piece[0] in parts]
            if not found:
                continue
            back = tuple(-d for d in step)

            @pl.when(there(back))
            def _():
                for piece in found:
                    message(step, *halo, piece).wait_recv()

    def stage(halo, out, table, group, finish, plan):
        rows, zbuf, _, slot = halo
        receive(halo, 0, (0,))
        spread(rows, zbuf, out, near, 0, height + 2)
        if len(plan) > 1:
            convolve(table, out, group, 0, finish, 0, height // (2 * group))
        done = 0
        for parts, upto, hook in plan:
            if parts:
                receive(halo, 1, parts)
                last = cuts[slot][parts[-1]]
                end = height + 2 if last == height else last + 1
                start = 0 if parts[0] == 0 else cuts[slot][parts[0] - 1] + 1
                spread(rows, zbuf, out, far, start, end)
            convolve(table, out, group, 1 if len(plan) > 1 else 2, finish, done, upto)
            done = upto
            hook()

    def sent(halo):
        crosswise(halo, hsend.at[ways + 4], (0, 1))
        for step in STEPS:
            if step[2] != 0:
                continue

            @pl.when(there(step))
            def _():
                for piece in pieces(step, halo[3]):
                    message(step, *halo, piece).wait_send()

    cells = depth * height
    folds = 2 if 4 * cells <= width else 1
    pitch = width // folds

    def collect(build, bits, at):
        count = bits[0].shape[0]
        pair = lax.broadcasted_iota(jnp.int32, (count, width), 1) // 2
        built = build[...]
        for f, bit in enumerate(bits):
            spot = f * (pitch // 2) + at
            built = jnp.where(pair == spot, pltpu.roll(bit, 2 * spot + 1, 1), built)
        build[...] = built

    def edges(rows, edge):
        count = edge.shape[0]
        lane = lax.broadcasted_iota(jnp.int32, (count, width), 1)
        pair = lane // 2
        whole = jnp.zeros((count, width), jnp.float32)
        for f in range(folds):
            part_rows = slice(f * count, (f + 1) * count)
            built = jnp.zeros((count, width), jnp.float32)
            for x in range(depth):
                for y in range(height):
                    row = rows[x + 1, y + 1, part_rows].astype(jnp.float32)
                    spot = f * (pitch // 2) + x * height + y
                    shift_by = (2 * spot + 1) % width
                    built = jnp.where(pair == spot, pltpu.roll(row, shift_by, 1), built)
            whole = jnp.where(lane < f * pitch, whole, built)
        edge[...] = whole.astype(edge.dtype)

    def shifter():
        src = lax.broadcasted_iota(jnp.int32, (2 * width, 2 * width), 0)
        dst = lax.broadcasted_iota(jnp.int32, (2 * width, 2 * width), 1)
        spot = src % pitch
        used = jnp.logical_and(src >= width, spot < 2 * cells)
        right = jnp.logical_and(used, spot % 2 == 1)
        left = jnp.logical_and(used, spot % 2 == 0)
        low = jnp.logical_or(
            jnp.logical_and(src == dst - 1, src < width - 1),
            jnp.logical_and(dst == 0, left),
        )
        high = jnp.logical_or(
            jnp.logical_and(src == dst - width + 1, src < width),
            jnp.logical_and(dst == 2 * width - 1, right),
        )
        pick = jnp.logical_or(
            jnp.logical_and(dst < width, low), jnp.logical_and(dst >= width, high)
        )
        shift[...] = jnp.where(pick, 1.0, 0.0).astype(shift.dtype)

    near = tuple(range(1, depth + 1))
    far = (0, depth + 1)

    def spread(rows, zbuf, out, planes, start, end):
        count = rows.shape[2]
        part = zbuf.shape[3]
        groups = count // chan
        span = end - start
        lane = lax.broadcasted_iota(jnp.int32, (part, width), 1)

        for xp in planes:
            dx = 0 if xp == 0 else (2 if xp == depth + 1 else 1)
            halo = []
            for yp in range(start, end):
                dy = 0 if yp == 0 else (2 if yp == height + 1 else 1)
                left = zbuf[0, dx, dy].astype(jnp.float32)
                right = zbuf[1, dx, dy].astype(jnp.float32)
                for f in range(folds):
                    at = f * pitch + 2 * ((xp - 1) % depth * height + (yp - 1) % height)
                    both = jnp.where(
                        lane == at + 1, right, jnp.where(lane == at, left, 0.0)
                    )
                    halo.append(both.astype(rows.dtype))
            wide = rows[xp, start:end].reshape(span * count, width)
            lhs = jnp.concatenate([wide, jnp.concatenate(halo, axis=0)], axis=1)
            moved = jnp.dot(lhs, shift[...], preferred_element_type=jnp.float32)
            moved = moved.astype(rows.dtype).reshape(span, count, 2 * width)
            kept = wide.reshape(span, count, width)
            for g in range(groups):
                at = slice(g * chan, (g + 1) * chan)
                base = g * 3 * chan
                out[xp, start:end, base : base + chan] = moved[:, at, :width]
                out[xp, start:end, base + chan : base + 2 * chan] = kept[:, at]
                out[xp, start:end, base + 2 * chan : base + 3 * chan] = moved[:, at, width:]

    def band(weights, table, group):
        outs = weights.shape[0]
        third = weights.shape[1] // 3
        step = third // 3
        table[...] = jnp.zeros_like(table)
        for kx in range(3):
            piece = weights[:, kx * third : (kx + 1) * third]
            for ox in range(depth):
                xp = ox + kx
                kind, pos = (0, near.index(xp)) if xp in near else (1, far.index(xp))
                for oy in range(group):
                    row = (ox * group + oy) * outs
                    at = (pos * (group + 2) + oy) * step
                    table[kind, row : row + outs, at : at + third] = piece

    def convolve(table, ref, group, kind, finish, lo, hi):
        outs = table.shape[1] // (depth * group)
        planes = (near, far, near + far)[kind]

        @pl.loop(lo, hi, unroll=1 if kind == 1 else hi - lo)
        def _(j):
            halves = []
            for half in range(2):
                y = (2 * j + half) * group
                halves.append(
                    jnp.concatenate(
                        [
                            ref[xp, pl.ds(y, group + 2)].reshape(
                                (group + 2) * ref.shape[2], width
                            )
                            for xp in planes
                        ],
                        axis=0,
                    )
                )
            rhs = jnp.concatenate(halves, axis=1)
            if kind == 2:
                weights = jnp.concatenate([table[0], table[1]], axis=1)
            else:
                weights = table[kind, :, : rhs.shape[0]]
            out = jnp.dot(weights, rhs, preferred_element_type=jnp.float32)
            if kind == 0:
                keep[j] = out
                return
            if kind == 1:
                out = out + keep[j]
            for half in range(2):
                for ox in range(depth):
                    for oy in range(group):
                        row = (ox * group + oy) * outs
                        finish(
                            ox,
                            (2 * j + half) * group + oy,
                            out[row : row + outs, half * width : (half + 1) * width],
                        )

    tiles = pack.shape[1]
    cells_all = float(depth * height * width * total)
    factor = math.sqrt(27.0 * chan)
    lanes = width // chan
    trio = 3 * chan

    def correlate(ref, rows, offset, slot):
        starts_y = range(0, height, 4)
        inner = slice(offset, offset + depth)
        rhs = jnp.concatenate(
            [
                rows[inner, y + offset : y + offset + 4].reshape(depth * 4 * chan, width)
                for y in starts_y
            ],
            axis=1,
        )

        def multiply(planes):
            lhs = jnp.concatenate(
                [ref[planes, y : y + 6, :trio].reshape(-1, width) for y in starts_y], axis=1
            )
            prod[planes] = lax.dot_general(
                lhs, rhs, NT, preferred_element_type=jnp.float32
            ).reshape((-1,) + prod.shape[1:])

        multiply(slice(0, depth + 2))
        for kx in range(3):
            fold(kx, slot)
            scatter(kx, slot)

    slab = 9 * chan
    step_rows = slab // lanes
    batch = step_rows // 8

    def fold(kx, slot):
        group = lax.broadcasted_iota(jnp.int32, (8, width), 1) // chan
        for r in range(0, trio, 8):
            sums = []
            for y in range(6):
                part_sum = prod[kx, y, r : r + 8, :width]
                for x in range(1, depth):
                    part_sum = part_sum + prod[
                        kx + x, y, r : r + 8, x * width : (x + 1) * width
                    ]
                sums.append(part_sum)
            for ky in range(3):
                at = ky * trio + r
                keep_y = sums[ky + 3]
                for y in (2, 1, 0):
                    keep_y = jnp.where(group == y, sums[ky + y], keep_y)
                diag[at : at + 8] = keep_y
        low = group < 2
        even = group % 2 == 0
        for i in range(batch):
            rows = [diag[j * step_rows + 8 * i : j * step_rows + 8 * i + 8] for j in range(4)]
            pairs = []
            for j in range(2):
                one, two = rows[j], rows[j + 2]
                pairs.append(
                    jnp.where(low, one, two)
                    + pltpu.roll(jnp.where(low, two, one), 2 * chan, 1)
                )
            one, two = pairs
            cross = jnp.where(even, two, one)
            pack[slot, kx * batch + i] = jnp.where(even, one, two) + jnp.where(
                even, pltpu.roll(cross, width - chan, 1), pltpu.roll(cross, chan, 1)
            )

    base, extra = owners(sizes)

    def at_spot(spot):
        return jnp.logical_and(
            me[0] == spot[0], jnp.logical_and(me[1] == spot[1], me[2] == spot[2])
        )

    def which(spots):
        found, index = False, 0
        for i, spot in enumerate(spots):
            here = at_spot(spot)
            found = jnp.logical_or(found, here)
            index = index + jnp.where(here, i, 0)
        return found, index

    is_base, base_at = which(base)
    is_extra, extra_at = which(extra)

    def give(slot, t, chunk, spot):
        at = (spot[0] * sizes[1] + spot[1]) * sizes[2] + spot[2]

        @pl.when(line != at)
        def _():
            pltpu.make_async_remote_copy(
                src_ref=pack.at[slot, t],
                dst_ref=land.at[slot, chunk, lax.rem(line - at + total, total) - 1],
                send_sem=asend.at[slot],
                recv_sem=arecv.at[slot, chunk],
                device_id=spot,
                device_id_type=MESH,
            ).start()

    def scatter(kx, slot):
        for w, spot in enumerate(base):
            give(slot, kx * batch + w, kx, spot)
        give(slot, kx * batch + len(base), 0, extra[kx])

    def others():
        axes = [
            [me[i] if d == 0 else lax.rem(me[i] + d, sizes[i]) for d in range(sizes[i])]
            for i in range(3)
        ]
        return list(itertools.product(*axes))[1:]

    def finish_tile(slot, t, chunk, row, column):
        landed = land.at[slot, chunk]
        pltpu.make_async_copy(landed, landed, arecv.at[slot, chunk]).wait()
        rounded = (pack[slot, t] + jnp.sum(land[slot, chunk], axis=0)).astype(part.dtype)
        part[slot, chunk] = rounded
        full[slot, row, column] = rounded

        def tell(spot):
            pltpu.make_async_remote_copy(
                src_ref=part.at[slot, chunk],
                dst_ref=full.at[slot, row, column],
                send_sem=bsend.at[slot],
                recv_sem=brecv.at[slot],
                device_id=spot,
                device_id_type=MESH,
            ).start()

        if total <= 64:
            for spot in others():
                tell(spot)
        else:

            @pl.loop(1, total)
            def _(i):
                tell(place(lax.rem(line + i, total)))

    def gather(slot):
        @pl.when(is_base)
        def _():
            for kx in range(3):
                finish_tile(slot, kx * batch + base_at, kx, base_at, kx)

        @pl.when(is_extra)
        def _():
            finish_tile(slot, extra_at * batch + len(base), 0, len(base), extra_at)

    def drain(slot, out, direction):
        none = jnp.logical_not(jnp.logical_or(is_base, is_extra))
        for owned, here in ((3, is_base), (1, is_extra), (0, none)):

            @pl.when(here)
            def _():
                some = told.at[pl.ds(0, tiles - owned)]
                pltpu.make_async_copy(some, some, brecv.at[slot]).wait()
                sent_all = pack.at[slot, pl.ds(0, tiles - owned)]
                pltpu.make_async_copy(sent_all, sent_all, asend.at[slot]).wait()
                if owned:
                    gone = told.at[pl.ds(0, owned * (total - 1))]
                    pltpu.make_async_copy(gone, gone, bsend.at[slot]).wait()

        for kx in range(3):
            whole = full[slot, :, kx].astype(jnp.float32).reshape(step_rows, width)
            for j in range(lanes):
                at = slice(kx * slab + j * step_rows, kx * slab + (j + 1) * step_rows)
                damp = 0.1 * direction[at].astype(jnp.float32)
                mean = whole[:, j * chan : (j + 1) * chan] * (1.0 / cells_all)
                out[at] = factor * (mean + damp)

    def arrange():
        filt = 27 * chan
        for load in loads[1:]:
            load.wait()
        four = jnp.concatenate([wf[...], vf[...], vs[...], ws[...]], axis=1)
        rows = lax.broadcasted_iota(jnp.int32, (4 * chan, 4 * chan), 0)
        cols = lax.broadcasted_iota(jnp.int32, (4 * chan, 4 * chan), 1)
        eye = jnp.where(rows == cols, 1.0, 0.0).astype(four.dtype)
        turned = lax.dot_general(eye, four, NT, preferred_element_type=jnp.float32)
        turned = turned.astype(w1.dtype)
        w1[...] = turned[: 2 * chan]
        third = 3 * chan
        for k in range(9):
            part = slice(k * third, (k + 1) * third)
            w2[:, 2 * k * third : (2 * k + 1) * third] = turned[2 * chan : 3 * chan, part]
            w2[:, (2 * k + 1) * third : (2 * k + 2) * third] = turned[3 * chan :, part]
        for k in range(27):
            at = filt - (k + 1) * chan
            w3[:, k * chan : (k + 1) * chan] = ws[at : at + chan]

    inner = (slice(1, depth + 1), slice(1, height + 1))
    loads[0].wait()
    for x in range(depth):
        rv[x + 1, 1 : height + 1] = jnp.swapaxes(volume[:, x], 0, 1)
    cells0, cells1, cells2 = (rv, zv, ev, 0), (rp, zp, ep, 1), (rj, zj, ej, 2)
    edges(rv, ev)
    pl.semaphore_wait(barrier, greeted)
    send_rest(cells0, True)
    send_rest(cells0, False)
    send_faces(cells0, 0)
    send_faces(cells0, 1)
    send_faces(cells0, 2)
    build1[...] = jnp.zeros_like(build1)
    build2[...] = jnp.zeros_like(build2)
    for rows, zbuf in ((rv, zv), (rp, zp), (rj, zj)):
        clear(rows, zbuf)
    shifter()
    arrange()
    band(w1, t1, 2)
    band(w2, t2, 4)
    band(w3, t3, 4)

    def first(x, y, out):
        hidden, slope = gelu_pair(out[:chan])
        slope_ref[x, y] = slope
        tangent = slope * out[chan:]
        rp[x + 1, y + 1, :chan] = hidden.astype(jnp.bfloat16)
        rp[x + 1, y + 1, chan:] = tangent.astype(jnp.bfloat16)
        if folds == 2:
            collect(build1, (hidden, tangent), x * height + y)

    def launch():
        sent(cells0)
        send_faces(cells1, 0)

    def launch_rest():
        if folds == 2:
            ep[...] = build1[...].astype(ep.dtype)
        else:
            edges(rp, ep)
        send_rest(cells1, True)
        send_rest(cells1, False)
        send_faces(cells1, 2)

    stage(
        cells0,
        sv,
        t1,
        2,
        first,
        (
            ((0,), 1, launch),
            ((1,), 2, lambda: None),
            ((2,), early // 4, lambda: send_faces(cells1, 1)),
            ((), height // 4, launch_rest),
        ),
    )

    def second(x, y, out):
        rj[x + 1, y + 1] = out.astype(jnp.bfloat16)
        if folds == 2:
            half = chan // 2
            collect(build2, (out[:half], out[half:]), x * height + y)

    def pass_on():
        sent(cells1)
        send_faces(cells2, 0)

    def pass_rest():
        if folds == 2:
            ej[...] = build2[...].astype(ej.dtype)
        else:
            edges(rj, ej)
        send_rest(cells2, True)
        send_rest(cells2, False)
        send_faces(cells2, 1)

    stage(
        cells1,
        sp,
        t2,
        4,
        second,
        (((0, 1), bands, pass_on), ((2,), height // 8, pass_rest)),
    )
    for x in range(depth):
        jv_out[:, x] = jnp.swapaxes(rj[x + 1, 1 : height + 1], 0, 1)
    correlate(sp, rj, 1, 0)

    def third(x, y, out):
        back_ref[x, y] = (slope_ref[x, y] * out).astype(jnp.bfloat16)

    stage(cells2, sj, t3, 4, third, (((0, 1), height // 8, lambda: None),))
    correlate(sv, back_ref, 0, 1)
    gather(0)
    gather(1)
    sent(cells2)
    drain(0, gv2, vs)
    drain(1, gv1, vf)


def place_out(*refs):
    count = len(refs) // 2
    sems = refs[-1]
    copies = [
        pltpu.make_async_copy(refs[i], refs[count + i], sems.at[i]) for i in range(count)
    ]
    for copy in copies:
        copy.start()
    for copy in copies:
        copy.wait()


def body(volume, w_first, w_second, v_first, v_second):
    chan, depth, height, width = volume.shape
    sizes = tuple(lax.axis_size(a) for a in AXES)
    total = sizes[0] * sizes[1] * sizes[2]
    filt = 27 * chan
    tiles = filt * chan // (8 * width)
    _, ways = codes(sizes)
    folds = 2 if 4 * depth * height <= width else 1
    bf, f32 = jnp.bfloat16, jnp.float32
    pads = (depth + 2, height + 2)
    vmem = pl.BlockSpec(memory_space=pltpu.VMEM)
    jv, corr1, corr2 = pl.pallas_call(
        functools.partial(kernel, sizes),
        out_shape=(
            jax.ShapeDtypeStruct(volume.shape, bf),
            jax.ShapeDtypeStruct((filt, chan), f32),
            jax.ShapeDtypeStruct((filt, chan), f32),
        ),
        in_specs=[pl.BlockSpec(memory_space=pltpu.HBM)] * 5,
        out_specs=(vmem,) * 3,
        scratch_shapes=[
            pltpu.VMEM(pads + (chan, width), bf),
            pltpu.VMEM(pads + (2 * chan, width), bf),
            pltpu.VMEM(pads + (chan, width), bf),
            pltpu.VMEM((2, 3, 3, chan // folds, width), bf),
            pltpu.VMEM((2, 3, 3, 2 * chan // folds, width), bf),
            pltpu.VMEM((2, 3, 3, chan // folds, width), bf),
            pltpu.VMEM((chan // folds, width), bf),
            pltpu.VMEM((2 * chan // folds, width), bf),
            pltpu.VMEM((chan // folds, width), bf),
            pltpu.VMEM(pads + (3 * chan, width), bf),
            pltpu.VMEM(pads + (6 * chan, width), bf),
            pltpu.VMEM(pads + (3 * chan, width), bf),
            pltpu.VMEM((depth, height, chan, width), f32),
            pltpu.VMEM((depth, height, chan, width), bf),
            pltpu.VMEM((2, depth * 2 * 2 * chan, depth * 4 * 3 * chan), bf),
            pltpu.VMEM((2, depth * 4 * chan, depth * 6 * 6 * chan), bf),
            pltpu.VMEM((2, depth * 4 * chan, depth * 6 * 3 * chan), bf),
            pltpu.VMEM((2 * width, 2 * width), bf),
            pltpu.VMEM((height // 4, depth * 4 * chan, 2 * width), f32),
            pltpu.VMEM((depth + 2, 6, 3 * chan, depth * 4 * chan), f32),
            pltpu.VMEM((9 * chan, width), f32),
            pltpu.VMEM((2, tiles, 8, width), f32),
            pltpu.VMEM((2, 3, total - 1, 8, width), f32),
            pltpu.VMEM((2, 3, 8, width), bf),
            pltpu.VMEM((2, 9, 3, 8, width), bf),
            pltpu.VMEM(((total - 1) * 3, 8, width), bf),
            pltpu.SemaphoreType.DMA((ways + 5,)),
            pltpu.SemaphoreType.DMA((2, ways + 6)),
            pltpu.SemaphoreType.DMA((2,)),
            pltpu.SemaphoreType.DMA((2, 3)),
            pltpu.SemaphoreType.DMA((2,)),
            pltpu.SemaphoreType.DMA((2,)),
            pltpu.VMEM(volume.shape, bf),
            pltpu.VMEM((filt, chan), bf),
            pltpu.VMEM((filt, chan), bf),
            pltpu.VMEM((filt, chan), bf),
            pltpu.VMEM((filt, chan), bf),
            pltpu.VMEM((2 * chan, filt), bf),
            pltpu.VMEM((chan, 2 * filt), bf),
            pltpu.VMEM((chan, filt), bf),
            pltpu.VMEM((2 * chan // folds, width), f32),
            pltpu.VMEM((chan // folds, width), f32),
            pltpu.VMEM((36, chan // folds, width), bf),
            pltpu.SemaphoreType.DMA((5,)),
        ],
        compiler_params=pltpu.CompilerParams(
            collective_id=0, has_side_effects=True, vmem_limit_bytes=48 * 1024 * 1024
        ),
    )(*(pltpu.with_memory_space_constraint(w, pltpu.HBM) for w in (volume, *(w.reshape(filt, chan) for w in (w_first, w_second, v_first, v_second)))))
    jv, corr1, corr2 = pl.pallas_call(
        place_out,
        out_shape=(
            jax.ShapeDtypeStruct(volume.shape, bf),
            jax.ShapeDtypeStruct((filt, chan), f32),
            jax.ShapeDtypeStruct((filt, chan), f32),
        ),
        in_specs=[vmem] * 3,
        out_specs=(pl.BlockSpec(memory_space=pltpu.HBM),) * 3,
        scratch_shapes=[pltpu.SemaphoreType.DMA((3,))],
        compiler_params=pltpu.CompilerParams(vmem_limit_bytes=4 * 1024 * 1024),
    )(jv, corr1, corr2)
    return jv, corr1.reshape(v_first.shape), corr2.reshape(v_second.shape)


def solution(mesh):
    in_specs = (P(None, "gx", "gy", "gz"), P(), P(), P(), P())
    out_specs = (P(None, "gx", "gy", "gz"), P(), P())
    return jax.shard_map(body, mesh=mesh, in_specs=in_specs, out_specs=out_specs, check_vma=False)
```

```python
import functools
import itertools
import math

import jax
import jax.numpy as jnp
from jax import lax
from jax.experimental import pallas as pl
from jax.experimental.pallas import tpu as pltpu
from jax.sharding import PartitionSpec as P

MESH = pl.DeviceIdType.MESH
AXES = ("gx", "gy", "gz")
STEPS = [d for d in itertools.product((-1, 0, 1), repeat=3) if d != (0, 0, 0)]
STEPS.sort(key=lambda d: (d[2] != 0, d[0] == 0, abs(d[0]) + abs(d[1])))
NT = (((1,), (1,)), ((), ()))


def gelu_pair(pre):
    inner = 0.7978845608 * (pre + 0.044715 * pre * pre * pre)
    hyper = jnp.tanh(inner)
    hidden = 0.5 * pre * (1.0 + hyper)
    slope = 0.5 * (1.0 + hyper) + 0.5 * pre * (1.0 - hyper * hyper) * 0.7978845608 * (
        1.0 + 0.134145 * pre * pre
    )
    return hidden, slope


def codes(sizes):
    spans = [3 if size > 2 else 2 for size in sizes[:2]]

    def code(step):
        total = 0
        for delta, span in zip(step, spans):
            total = total * span + (delta + 1 if span == 3 else abs(delta))
        return total

    return code, math.prod(spans)


def owners(sizes):
    mids = min(2, sizes[0])
    start = (sizes[0] - mids) // 2
    spots = [
        (x, y, z)
        for z in range(sizes[2])
        for y in range(sizes[1])
        for x in range(start, start + mids)
    ]
    base = [spot for spot in spots if spot[2] % 2 == 1][:8]
    rest = [spot for spot in spots if spot not in base]
    return base, [rest[0], rest[-1], rest[len(rest) // 2 - 1]]


def kernel(
    sizes,
    volume_hbm,
    wf_hbm,
    ws_hbm,
    vf_hbm,
    vs_hbm,
    jv_out,
    gv1,
    gv2,
    *scratch,
):
    (rv, rp, rj, zv, zp, zj, ev, ep, ej, sv, sp, sj, slope_ref, back_ref,
     t1, t2, t3, shift, keep, prod, diag, pack, land, part, full, told,
     hsend, hrecv, asend, arecv, bsend, brecv,
     volume, wf, ws, vf, vs, w1, w2, w3, build1, build2, blank, isem) = scratch
    chan, depth, height, width = volume.shape
    code, ways = codes(sizes)
    early = height - 4
    bands = (early - 1) // 8
    cuts = ((5, 9, height), (4, 8 * bands + 1, height), (8 * bands, height))
    loads = [
        pltpu.make_async_copy(src, dst, isem.at[i])
        for i, (src, dst) in enumerate(
            (
                (volume_hbm, volume),
                (wf_hbm, wf),
                (ws_hbm, ws),
                (vf_hbm, vf),
                (vs_hbm, vs),
            )
        )
    ]
    for load in loads:
        load.start()
    me = tuple(lax.axis_index(a) for a in AXES)
    total = sizes[0] * sizes[1] * sizes[2]
    line = (me[0] * sizes[1] + me[1]) * sizes[2] + me[2]

    def place(index):
        return (
            index // (sizes[1] * sizes[2]),
            index // sizes[2] % sizes[1],
            index % sizes[2],
        )

    def there(step):
        ok = None
        for pos, size, delta in zip(me, sizes, step):
            if delta == -1:
                term = pos > 0
            elif delta == 1:
                term = pos < size - 1
            else:
                continue
            ok = term if ok is None else jnp.logical_and(ok, term)
        return ok

    barrier = pltpu.get_barrier_semaphore()
    near_only = max(sizes) <= 4

    if near_only:
        greeted = 0
        for step in STEPS:
            ok = there(step)
            greeted = greeted + jnp.where(ok, 1, 0)

            @pl.when(ok)
            def _():
                pl.semaphore_signal(
                    barrier,
                    inc=1,
                    device_id=tuple(p + d for p, d in zip(me, step)),
                    device_id_type=MESH,
                )
    else:
        greeted = total - 1

        @pl.loop(1, total)
        def _(i):
            pl.semaphore_signal(
                barrier, inc=1, device_id=place(lax.rem(line + i, total)), device_id_type=MESH
            )

    def source(delta, extent):
        return {-1: pl.ds(1, 1), 1: pl.ds(extent, 1), 0: pl.ds(1, extent)}[delta]

    def target(delta, extent):
        return {-1: pl.ds(extent + 1, 1), 1: pl.ds(0, 1), 0: pl.ds(1, extent)}[delta]

    def pieces(step, slot):
        if step[1] or step[2]:
            return [None]
        ends = cuts[slot]
        return [(p, lo, hi) for p, (lo, hi) in enumerate(zip((0,) + ends, ends))]

    def landing(step, rows, zbuf, piece=None):
        if step[2] == 0:
            if piece is None:
                return rows.at[target(step[0], depth), target(step[1], height)]
            _, lo, hi = piece
            return rows.at[target(step[0], depth), pl.ds(1 + lo, hi - lo)]
        return zbuf.at[0 if step[2] == 1 else 1, 1 - step[0], 1 - step[1]]

    def message(step, rows, zbuf, edge, slot, piece=None):
        lane = take = code(step)
        if step[2] != 0:
            src = edge
            lane = ways + 4
            take = lane + (step[0] != 0)
        elif piece is None:
            src = rows.at[source(step[0], depth), source(step[1], height)]
        else:
            part, lo, hi = piece
            src = rows.at[source(step[0], depth), pl.ds(1 + lo, hi - lo)]
            if part:
                lane = take = ways + 2 * (part - 1) + (step[0] > 0)
        return pltpu.make_async_remote_copy(
            src_ref=src,
            dst_ref=landing(step, rows, zbuf, piece),
            send_sem=hsend.at[lane],
            recv_sem=hrecv.at[slot % 2, take],
            device_id=tuple(p + d for p, d in zip(me, step)),
            device_id_type=MESH,
        )

    def send_faces(halo, part):
        for step in STEPS:
            found = pieces(step, halo[3])
            if found == [None] or part >= len(found):
                continue

            @pl.when(there(step))
            def _():
                message(step, *halo, found[part]).start()

    def send_rest(halo, cross):
        for step in STEPS:
            if (step[2] != 0) == cross and pieces(step, halo[3]) == [None]:

                @pl.when(there(step))
                def _():
                    message(step, *halo).start()

    def clear(rows, zbuf):
        for step in STEPS:
            back = tuple(-d for d in step)

            @pl.when(jnp.logical_not(there(back)))
            def _():
                ref = landing(step, rows, zbuf)
                ref[...] = jnp.zeros(ref.shape, ref.dtype)

    def crosswise(halo, sem, kinds):
        rows_each = halo[2].shape[0] // (chan // folds)
        beside = [jnp.where(p > 0, 1, 0) + jnp.where(p < n - 1, 1, 0) for p, n in zip(me, sizes)]
        options = [(0,) if n == 1 else (1,) if n == 2 else (1, 2) for n in sizes]
        for nx, ny, nz in itertools.product(*options):
            count = nz * (1 + ny) * sum(nx if kind else 1 for kind in kinds) * rows_each
            if not count:
                continue
            fits = jnp.logical_and(
                beside[0] == nx, jnp.logical_and(beside[1] == ny, beside[2] == nz)
            )

            @pl.when(fits)
            def _():
                gone = blank.at[pl.ds(0, count)]
                pltpu.make_async_copy(gone, gone, sem).wait()

    def receive(halo, kind, parts):
        if 0 in parts:
            crosswise(halo, hrecv.at[halo[3] % 2, ways + 4 + kind], (kind,))
        for step in STEPS:
            if (step[0] != 0) != (kind == 1):
                continue
            found = pieces(step, halo[3])
            if step[2] != 0:
                continue
            if found == [None]:
                found = found if 0 in parts else []
            else:
                found = [piece for piece in found if piece[0] in parts]
            if not found:
                continue
            back = tuple(-d for d in step)

            @pl.when(there(back))
            def _():
                for piece in found:
                    message(step, *halo, piece).wait_recv()

    def stage(halo, out, table, group, finish, plan):
        rows, zbuf, _, slot = halo
        receive(halo, 0, (0,))
        spread(rows, zbuf, out, near, 0, height + 2)
        if len(plan) > 1:
            convolve(table, out, group, 0, finish, 0, height // (2 * group))
        done = 0
        for parts, upto, hook in plan:
            if parts:
                receive(halo, 1, parts)
                last = cuts[slot][parts[-1]]
                end = height + 2 if last == height else last + 1
                start = 0 if parts[0] == 0 else cuts[slot][parts[0] - 1] + 1
                spread(rows, zbuf, out, far, start, end)
            convolve(table, out, group, 1 if len(plan) > 1 else 2, finish, done, upto)
            done = upto
            hook()

    def sent(halo):
        crosswise(halo, hsend.at[ways + 4], (0, 1))
        for step in STEPS:
            if step[2] != 0:
                continue

            @pl.when(there(step))
            def _():
                for piece in pieces(step, halo[3]):
                    message(step, *halo, piece).wait_send()

    cells = depth * height
    folds = 2 if 4 * cells <= width else 1
    pitch = width // folds

    def collect(build, bits, at):
        count = bits[0].shape[0]
        pair = lax.broadcasted_iota(jnp.int32, (count, width), 1) // 2
        built = build[...]
        for f, bit in enumerate(bits):
            spot = f * (pitch // 2) + at
            built = jnp.where(pair == spot, pltpu.roll(bit, 2 * spot + 1, 1), built)
        build[...] = built

    def edges(rows, edge):
        count = edge.shape[0]
        lane = lax.broadcasted_iota(jnp.int32, (count, width), 1)
        pair = lane // 2
        whole = jnp.zeros((count, width), jnp.float32)
        for f in range(folds):
            part_rows = slice(f * count, (f + 1) * count)
            built = jnp.zeros((count, width), jnp.float32)
            for x in range(depth):
                for y in range(height):
                    row = rows[x + 1, y + 1, part_rows].astype(jnp.float32)
                    spot = f * (pitch // 2) + x * height + y
                    shift_by = (2 * spot + 1) % width
                    built = jnp.where(pair == spot, pltpu.roll(row, shift_by, 1), built)
            whole = jnp.where(lane < f * pitch, whole, built)
        edge[...] = whole.astype(edge.dtype)

    def shifter():
        src = lax.broadcasted_iota(jnp.int32, (2 * width, 2 * width), 0)
        dst = lax.broadcasted_iota(jnp.int32, (2 * width, 2 * width), 1)
        spot = src % pitch
        used = jnp.logical_and(src >= width, spot < 2 * cells)
        right = jnp.logical_and(used, spot % 2 == 1)
        left = jnp.logical_and(used, spot % 2 == 0)
        low = jnp.logical_or(
            jnp.logical_and(src == dst - 1, src < width - 1),
            jnp.logical_and(dst == 0, left),
        )
        high = jnp.logical_or(
            jnp.logical_and(src == dst - width + 1, src < width),
            jnp.logical_and(dst == 2 * width - 1, right),
        )
        pick = jnp.logical_or(
            jnp.logical_and(dst < width, low), jnp.logical_and(dst >= width, high)
        )
        shift[...] = jnp.where(pick, 1.0, 0.0).astype(shift.dtype)

    near = tuple(range(1, depth + 1))
    far = (0, depth + 1)

    def spread(rows, zbuf, out, planes, start, end):
        count = rows.shape[2]
        part = zbuf.shape[3]
        groups = count // chan
        span = end - start
        lane = lax.broadcasted_iota(jnp.int32, (part, width), 1)

        for xp in planes:
            dx = 0 if xp == 0 else (2 if xp == depth + 1 else 1)
            halo = []
            for yp in range(start, end):
                dy = 0 if yp == 0 else (2 if yp == height + 1 else 1)
                left = zbuf[0, dx, dy].astype(jnp.float32)
                right = zbuf[1, dx, dy].astype(jnp.float32)
                for f in range(folds):
                    at = f * pitch + 2 * ((xp - 1) % depth * height + (yp - 1) % height)
                    both = jnp.where(
                        lane == at + 1, right, jnp.where(lane == at, left, 0.0)
                    )
                    halo.append(both.astype(rows.dtype))
            wide = rows[xp, start:end].reshape(span * count, width)
            lhs = jnp.concatenate([wide, jnp.concatenate(halo, axis=0)], axis=1)
            moved = jnp.dot(lhs, shift[...], preferred_element_type=jnp.float32)
            moved = moved.astype(rows.dtype).reshape(span, count, 2 * width)
            kept = wide.reshape(span, count, width)
            for g in range(groups):
                at = slice(g * chan, (g + 1) * chan)
                base = g * 3 * chan
                out[xp, start:end, base : base + chan] = moved[:, at, :width]
                out[xp, start:end, base + chan : base + 2 * chan] = kept[:, at]
                out[xp, start:end, base + 2 * chan : base + 3 * chan] = moved[:, at, width:]

    def band(weights, table, group):
        outs = weights.shape[0]
        third = weights.shape[1] // 3
        step = third // 3
        table[...] = jnp.zeros_like(table)
        for kx in range(3):
            piece = weights[:, kx * third : (kx + 1) * third]
            for ox in range(depth):
                xp = ox + kx
                kind, pos = (0, near.index(xp)) if xp in near else (1, far.index(xp))
                for oy in range(group):
                    row = (ox * group + oy) * outs
                    at = (pos * (group + 2) + oy) * step
                    table[kind, row : row + outs, at : at + third] = piece

    def convolve(table, ref, group, kind, finish, lo, hi):
        outs = table.shape[1] // (depth * group)
        planes = (near, far, near + far)[kind]

        @pl.loop(lo, hi, unroll=1 if kind == 1 else hi - lo)
        def _(j):
            halves = []
            for half in range(2):
                y = (2 * j + half) * group
                halves.append(
                    jnp.concatenate(
                        [
                            ref[xp, pl.ds(y, group + 2)].reshape(
                                (group + 2) * ref.shape[2], width
                            )
                            for xp in planes
                        ],
                        axis=0,
                    )
                )
            rhs = jnp.concatenate(halves, axis=1)
            if kind == 2:
                weights = jnp.concatenate([table[0], table[1]], axis=1)
            else:
                weights = table[kind, :, : rhs.shape[0]]
            out = jnp.dot(weights, rhs, preferred_element_type=jnp.float32)
            if kind == 0:
                keep[j] = out
                return
            if kind == 1:
                out = out + keep[j]
            for half in range(2):
                for ox in range(depth):
                    for oy in range(group):
                        row = (ox * group + oy) * outs
                        finish(
                            ox,
                            (2 * j + half) * group + oy,
                            out[row : row + outs, half * width : (half + 1) * width],
                        )

    tiles = pack.shape[1]
    cells_all = float(depth * height * width * total)
    factor = math.sqrt(27.0 * chan)
    lanes = width // chan
    trio = 3 * chan

    def correlate(ref, rows, offset, slot):
        starts_y = range(0, height, 4)
        inner = slice(offset, offset + depth)
        rhs = jnp.concatenate(
            [
                rows[inner, y + offset : y + offset + 4].reshape(depth * 4 * chan, width)
                for y in starts_y
            ],
            axis=1,
        )

        def multiply(planes):
            lhs = jnp.concatenate(
                [ref[planes, y : y + 6, :trio].reshape(-1, width) for y in starts_y], axis=1
            )
            prod[planes] = lax.dot_general(
                lhs, rhs, NT, preferred_element_type=jnp.float32
            ).reshape((-1,) + prod.shape[1:])

        multiply(slice(0, depth + 2))
        for kx in range(3):
            fold(kx, slot)
            scatter(kx, slot)

    slab = 9 * chan
    step_rows = slab // lanes
    batch = step_rows // 8

    def fold(kx, slot):
        group = lax.broadcasted_iota(jnp.int32, (8, width), 1) // chan
        for r in range(0, trio, 8):
            sums = []
            for y in range(6):
                part_sum = prod[kx, y, r : r + 8, :width]
                for x in range(1, depth):
                    part_sum = part_sum + prod[
                        kx + x, y, r : r + 8, x * width : (x + 1) * width
                    ]
                sums.append(part_sum)
            for ky in range(3):
                at = ky * trio + r
                keep_y = sums[ky + 3]
                for y in (2, 1, 0):
                    keep_y = jnp.where(group == y, sums[ky + y], keep_y)
                diag[at : at + 8] = keep_y
        low = group < 2
        even = group % 2 == 0
        for i in range(batch):
            rows = [diag[j * step_rows + 8 * i : j * step_rows + 8 * i + 8] for j in range(4)]
            pairs = []
            for j in range(2):
                one, two = rows[j], rows[j + 2]
                pairs.append(
                    jnp.where(low, one, two)
                    + pltpu.roll(jnp.where(low, two, one), 2 * chan, 1)
                )
            one, two = pairs
            cross = jnp.where(even, two, one)
            pack[slot, kx * batch + i] = jnp.where(even, one, two) + jnp.where(
                even, pltpu.roll(cross, width - chan, 1), pltpu.roll(cross, chan, 1)
            )

    base, extra = owners(sizes)

    def at_spot(spot):
        return jnp.logical_and(
            me[0] == spot[0], jnp.logical_and(me[1] == spot[1], me[2] == spot[2])
        )

    def which(spots):
        found, index = False, 0
        for i, spot in enumerate(spots):
            here = at_spot(spot)
            found = jnp.logical_or(found, here)
            index = index + jnp.where(here, i, 0)
        return found, index

    is_base, base_at = which(base)
    is_extra, extra_at = which(extra)

    def give(slot, t, chunk, spot):
        at = (spot[0] * sizes[1] + spot[1]) * sizes[2] + spot[2]

        @pl.when(line != at)
        def _():
            pltpu.make_async_remote_copy(
                src_ref=pack.at[slot, t],
                dst_ref=land.at[slot, chunk, lax.rem(line - at + total, total) - 1],
                send_sem=asend.at[slot],
                recv_sem=arecv.at[slot, chunk],
                device_id=spot,
                device_id_type=MESH,
            ).start()

    def scatter(kx, slot):
        for w, spot in enumerate(base):
            give(slot, kx * batch + w, kx, spot)
        give(slot, kx * batch + len(base), 0, extra[kx])

    def others():
        axes = [
            [me[i] if d == 0 else lax.rem(me[i] + d, sizes[i]) for d in range(sizes[i])]
            for i in range(3)
        ]
        return list(itertools.product(*axes))[1:]

    def finish_tile(slot, t, chunk, row, column):
        landed = land.at[slot, chunk]
        pltpu.make_async_copy(landed, landed, arecv.at[slot, chunk]).wait()
        rounded = (pack[slot, t] + jnp.sum(land[slot, chunk], axis=0)).astype(part.dtype)
        part[slot, chunk] = rounded
        full[slot, row, column] = rounded

        def tell(spot):
            pltpu.make_async_remote_copy(
                src_ref=part.at[slot, chunk],
                dst_ref=full.at[slot, row, column],
                send_sem=bsend.at[slot],
                recv_sem=brecv.at[slot],
                device_id=spot,
                device_id_type=MESH,
            ).start()

        if total <= 64:
            for spot in others():
                tell(spot)
        else:

            @pl.loop(1, total)
            def _(i):
                tell(place(lax.rem(line + i, total)))

    def gather(slot):
        @pl.when(is_base)
        def _():
            for kx in range(3):
                finish_tile(slot, kx * batch + base_at, kx, base_at, kx)

        @pl.when(is_extra)
        def _():
            finish_tile(slot, extra_at * batch + len(base), 0, len(base), extra_at)

    def drain(slot, out, direction):
        out[...] = (0.1 * factor) * direction[...].astype(jnp.float32)
        none = jnp.logical_not(jnp.logical_or(is_base, is_extra))
        for owned, here in ((3, is_base), (1, is_extra), (0, none)):

            @pl.when(here)
            def _():
                some = told.at[pl.ds(0, tiles - owned)]
                pltpu.make_async_copy(some, some, brecv.at[slot]).wait()
                sent_all = pack.at[slot, pl.ds(0, tiles - owned)]
                pltpu.make_async_copy(sent_all, sent_all, asend.at[slot]).wait()
                if owned:
                    gone = told.at[pl.ds(0, owned * (total - 1))]
                    pltpu.make_async_copy(gone, gone, bsend.at[slot]).wait()

        for kx in range(3):
            whole = full[slot, :, kx].astype(jnp.float32).reshape(step_rows, width)
            for j in range(lanes):
                at = slice(kx * slab + j * step_rows, kx * slab + (j + 1) * step_rows)
                out[at] += whole[:, j * chan : (j + 1) * chan] * (factor / cells_all)

    def arrange():
        filt = 27 * chan
        for load in loads[1:]:
            load.wait()
        four = jnp.concatenate([wf[...], vf[...], vs[...], ws[...]], axis=1)
        rows = lax.broadcasted_iota(jnp.int32, (4 * chan, 4 * chan), 0)
        cols = lax.broadcasted_iota(jnp.int32, (4 * chan, 4 * chan), 1)
        eye = jnp.where(rows == cols, 1.0, 0.0).astype(four.dtype)
        turned = lax.dot_general(eye, four, NT, preferred_element_type=jnp.float32)
        turned = turned.astype(w1.dtype)
        w1[...] = turned[: 2 * chan]
        third = 3 * chan
        for k in range(9):
            part = slice(k * third, (k + 1) * third)
            w2[:, 2 * k * third : (2 * k + 1) * third] = turned[2 * chan : 3 * chan, part]
            w2[:, (2 * k + 1) * third : (2 * k + 2) * third] = turned[3 * chan :, part]
        for k in range(27):
            at = filt - (k + 1) * chan
            w3[:, k * chan : (k + 1) * chan] = ws[at : at + chan]

    inner = (slice(1, depth + 1), slice(1, height + 1))
    loads[0].wait()
    for x in range(depth):
        rv[x + 1, 1 : height + 1] = jnp.swapaxes(volume[:, x], 0, 1)
    cells0, cells1, cells2 = (rv, zv, ev, 0), (rp, zp, ep, 1), (rj, zj, ej, 2)
    edges(rv, ev)
    pl.semaphore_wait(barrier, greeted)
    send_rest(cells0, True)
    send_rest(cells0, False)
    send_faces(cells0, 0)
    send_faces(cells0, 1)
    send_faces(cells0, 2)
    build1[...] = jnp.zeros_like(build1)
    build2[...] = jnp.zeros_like(build2)
    for rows, zbuf in ((rv, zv), (rp, zp), (rj, zj)):
        clear(rows, zbuf)
    shifter()
    arrange()
    band(w1, t1, 2)
    band(w2, t2, 4)
    band(w3, t3, 4)

    def first(x, y, out):
        hidden, slope = gelu_pair(out[:chan])
        slope_ref[x, y] = slope
        tangent = slope * out[chan:]
        rp[x + 1, y + 1, :chan] = hidden.astype(jnp.bfloat16)
        rp[x + 1, y + 1, chan:] = tangent.astype(jnp.bfloat16)
        if folds == 2:
            collect(build1, (hidden, tangent), x * height + y)

    def launch():
        sent(cells0)
        send_faces(cells1, 0)

    def launch_rest():
        if folds == 2:
            ep[...] = build1[...].astype(ep.dtype)
        else:
            edges(rp, ep)
        send_rest(cells1, True)
        send_rest(cells1, False)
        send_faces(cells1, 2)

    stage(
        cells0,
        sv,
        t1,
        2,
        first,
        (
            ((0,), 1, launch),
            ((1,), 2, lambda: None),
            ((2,), early // 4, lambda: send_faces(cells1, 1)),
            ((), height // 4, launch_rest),
        ),
    )

    def second(x, y, out):
        rj[x + 1, y + 1] = out.astype(jnp.bfloat16)
        if folds == 2:
            half = chan // 2
            collect(build2, (out[:half], out[half:]), x * height + y)

    def pass_on():
        sent(cells1)
        send_faces(cells2, 0)

    def pass_rest():
        if folds == 2:
            ej[...] = build2[...].astype(ej.dtype)
        else:
            edges(rj, ej)
        send_rest(cells2, True)
        send_rest(cells2, False)
        send_faces(cells2, 1)

    stage(
        cells1,
        sp,
        t2,
        4,
        second,
        (((0, 1), bands, pass_on), ((2,), height // 8, pass_rest)),
    )
    for x in range(depth):
        jv_out[:, x] = jnp.swapaxes(rj[x + 1, 1 : height + 1], 0, 1)
    correlate(sp, rj, 1, 0)

    def third(x, y, out):
        back_ref[x, y] = (slope_ref[x, y] * out).astype(jnp.bfloat16)

    stage(cells2, sj, t3, 4, third, (((0, 1), height // 8, lambda: None),))
    correlate(sv, back_ref, 0, 1)
    gather(0)
    gather(1)
    sent(cells2)
    drain(0, gv2, vs)
    drain(1, gv1, vf)


def place_out(*refs):
    count = len(refs) // 2
    sems = refs[-1]
    copies = [
        pltpu.make_async_copy(refs[i], refs[count + i], sems.at[i]) for i in range(count)
    ]
    for copy in copies:
        copy.start()
    for copy in copies:
        copy.wait()


def body(volume, w_first, w_second, v_first, v_second):
    chan, depth, height, width = volume.shape
    sizes = tuple(lax.axis_size(a) for a in AXES)
    total = sizes[0] * sizes[1] * sizes[2]
    filt = 27 * chan
    tiles = filt * chan // (8 * width)
    _, ways = codes(sizes)
    folds = 2 if 4 * depth * height <= width else 1
    bf, f32 = jnp.bfloat16, jnp.float32
    pads = (depth + 2, height + 2)
    vmem = pl.BlockSpec(memory_space=pltpu.VMEM)
    jv, corr1, corr2 = pl.pallas_call(
        functools.partial(kernel, sizes),
        out_shape=(
            jax.ShapeDtypeStruct(volume.shape, bf),
            jax.ShapeDtypeStruct((filt, chan), f32),
            jax.ShapeDtypeStruct((filt, chan), f32),
        ),
        in_specs=[pl.BlockSpec(memory_space=pltpu.HBM)] * 5,
        out_specs=(vmem,) * 3,
        scratch_shapes=[
            pltpu.VMEM(pads + (chan, width), bf),
            pltpu.VMEM(pads + (2 * chan, width), bf),
            pltpu.VMEM(pads + (chan, width), bf),
            pltpu.VMEM((2, 3, 3, chan // folds, width), bf),
            pltpu.VMEM((2, 3, 3, 2 * chan // folds, width), bf),
            pltpu.VMEM((2, 3, 3, chan // folds, width), bf),
            pltpu.VMEM((chan // folds, width), bf),
            pltpu.VMEM((2 * chan // folds, width), bf),
            pltpu.VMEM((chan // folds, width), bf),
            pltpu.VMEM(pads + (3 * chan, width), bf),
            pltpu.VMEM(pads + (6 * chan, width), bf),
            pltpu.VMEM(pads + (3 * chan, width), bf),
            pltpu.VMEM((depth, height, chan, width), f32),
            pltpu.VMEM((depth, height, chan, width), bf),
            pltpu.VMEM((2, depth * 2 * 2 * chan, depth * 4 * 3 * chan), bf),
            pltpu.VMEM((2, depth * 4 * chan, depth * 6 * 6 * chan), bf),
            pltpu.VMEM((2, depth * 4 * chan, depth * 6 * 3 * chan), bf),
            pltpu.VMEM((2 * width, 2 * width), bf),
            pltpu.VMEM((height // 4, depth * 4 * chan, 2 * width), f32),
            pltpu.VMEM((depth + 2, 6, 3 * chan, depth * 4 * chan), f32),
            pltpu.VMEM((9 * chan, width), f32),
            pltpu.VMEM((2, tiles, 8, width), f32),
            pltpu.VMEM((2, 3, total - 1, 8, width), f32),
            pltpu.VMEM((2, 3, 8, width), bf),
            pltpu.VMEM((2, 9, 3, 8, width), bf),
            pltpu.VMEM(((total - 1) * 3, 8, width), bf),
            pltpu.SemaphoreType.DMA((ways + 5,)),
            pltpu.SemaphoreType.DMA((2, ways + 6)),
            pltpu.SemaphoreType.DMA((2,)),
            pltpu.SemaphoreType.DMA((2, 3)),
            pltpu.SemaphoreType.DMA((2,)),
            pltpu.SemaphoreType.DMA((2,)),
            pltpu.VMEM(volume.shape, bf),
            pltpu.VMEM((filt, chan), bf),
            pltpu.VMEM((filt, chan), bf),
            pltpu.VMEM((filt, chan), bf),
            pltpu.VMEM((filt, chan), bf),
            pltpu.VMEM((2 * chan, filt), bf),
            pltpu.VMEM((chan, 2 * filt), bf),
            pltpu.VMEM((chan, filt), bf),
            pltpu.VMEM((2 * chan // folds, width), f32),
            pltpu.VMEM((chan // folds, width), f32),
            pltpu.VMEM((36, chan // folds, width), bf),
            pltpu.SemaphoreType.DMA((5,)),
        ],
        compiler_params=pltpu.CompilerParams(
            collective_id=0, has_side_effects=True, vmem_limit_bytes=48 * 1024 * 1024
        ),
    )(*(pltpu.with_memory_space_constraint(w, pltpu.HBM) for w in (volume, *(w.reshape(filt, chan) for w in (w_first, w_second, v_first, v_second)))))
    jv, corr1, corr2 = pl.pallas_call(
        place_out,
        out_shape=(
            jax.ShapeDtypeStruct(volume.shape, bf),
            jax.ShapeDtypeStruct((filt, chan), f32),
            jax.ShapeDtypeStruct((filt, chan), f32),
        ),
        in_specs=[vmem] * 3,
        out_specs=(pl.BlockSpec(memory_space=pltpu.HBM),) * 3,
        scratch_shapes=[pltpu.SemaphoreType.DMA((3,))],
        compiler_params=pltpu.CompilerParams(vmem_limit_bytes=4 * 1024 * 1024),
    )(jv, corr1, corr2)
    return jv, corr1.reshape(v_first.shape), corr2.reshape(v_second.shape)


def solution(mesh):
    in_specs = (P(None, "gx", "gy", "gz"), P(), P(), P(), P())
    out_specs = (P(None, "gx", "gy", "gz"), P(), P())
    return jax.shard_map(body, mesh=mesh, in_specs=in_specs, out_specs=out_specs, check_vma=False)
```
